512 devices in a mesh: crop: 8 (over z_lo, core), axial: 64 (over x, y, z_hi).
Axes of the slice: x: 4, y: 4, z: 16 (z_hi: 4, z_lo: 4; z = z_hi * 4 + z_lo), core: 2. Of those that a mesh axis runs over, the one named last changes fastest.
Arguments:
- pair: bfloat16 [8, 256, 256, 128], P('crop', 'axial'), may hold values from -6 to 6
- crop_mask: int32 [8, 256], P('crop'), may hold values 0 or 1
- weights: bfloat16 [128, 768], replicated, may hold values from -0.5 to 0.5
- probe_signs: int32 [128, 768], replicated, may hold values from 0 to 1
Outputs:
- pair_out: bfloat16 [8, 256, 256, 128], P('crop', 'axial')
- curvature: float32 [128, 768], replicated
The draws below stay inside these ranges and needn't reach their ends.
All inputs are finite; a program needn't handle non-finite values. No bound on the sum of `crop_mask` on one device may be relied on, other than what follows from the above.
Results may differ from the reference program's by a relative error of at most 0.006.
Values may be sent and summed in bfloat16 or wider, within the bound.
A program may use at most 64 MiB of HBM per device.

```python
import jax
import jax.numpy as jnp
from jax import lax

C = 128
N = 256
CROPS = 8
WCOLS = 768


def place_ends(entries, own_key, smallest, top_value):
    spot = [jax.random.randint(jax.random.fold_in(own_key, axis), (), 0, length) for axis, length in enumerate(entries.shape)]
    longest = entries.shape.index(max(entries.shape))
    next_to = spot[:longest] + [(spot[longest] + 1) % entries.shape[longest]] + spot[longest + 1:]
    return entries.at[tuple(spot)].set(smallest).at[tuple(next_to)].set(top_value)


def level_of(stream_key, extent, cuts, low, top_value):
    level, own = 1.0, jax.random.fold_in(stream_key, 6)
    for position, blocks in cuts:
        heights = jnp.exp(jax.random.uniform(jax.random.fold_in(own, position), (blocks,), jnp.float32, low / len(cuts), top_value / len(cuts)))
        level = level * jnp.repeat(heights, extent[position] // blocks).reshape([-1 if axis == position else 1 for axis in range(len(extent))])
    return level


def normal_values(key, dims, spread, most, cuts=(), kind=jnp.bfloat16):
    factor_of = level_of(key, dims, cuts, -0.22, 0.18) if cuts else 1.0
    result = jax.random.normal(key, dims, jnp.float32) * spread * factor_of
    return jnp.minimum(jnp.maximum(result, -most), most).astype(kind)


def setup_inputs(seed: int = 0) -> dict:
    arg_keys = jax.random.split(jax.random.key(seed), 5)
    pair = normal_values(arg_keys[0], (CROPS, N, N, C), 1.0, 6.0, ((0, 8), (1, 64)))
    crop_mask = place_ends((jax.random.randint(arg_keys[1], (CROPS, N), 0, 8) < 7).astype(jnp.int32), jax.random.fold_in(arg_keys[1], 1), 0, 1)
    weights = normal_values(arg_keys[2], (C, WCOLS), C ** -0.5, 0.5)
    probe_signs = place_ends(jax.random.randint(arg_keys[3], (C, WCOLS), 0, 2), jax.random.fold_in(arg_keys[3], 1), 0, 1).astype(jnp.int32)
    return dict(pair=pair, crop_mask=crop_mask, weights=weights, probe_signs=probe_signs)


def norm_axis(value, axis):
    mean = lax.optimization_barrier(jnp.mean(value, axis=axis, keepdims=True))
    centered = value - mean
    var = lax.optimization_barrier(jnp.mean(centered * centered, axis=axis, keepdims=True))
    return centered * lax.rsqrt(var + 1e-05)

def project_in(w_in, zn_bf, mask_pair):
    proj = jnp.einsum('rnc,cd->drn', zn_bf.astype(jnp.float32), w_in.astype(jnp.bfloat16).astype(jnp.float32))
    hid = proj.shape[0] // 4
    a_full = jax.nn.sigmoid(proj[hid:2 * hid]) * proj[:hid] * mask_pair
    b_full = jax.nn.sigmoid(proj[3 * hid:]) * proj[2 * hid:3 * hid] * mask_pair
    return (a_full, b_full)

def head(w_head, x_full, zn_bf):
    chans = zn_bf.shape[2]
    w_gate = w_head[:, :chans].astype(jnp.bfloat16).astype(jnp.float32)
    w_out = w_head[:, chans:].astype(jnp.bfloat16).astype(jnp.float32)
    x_norm = norm_axis(x_full, 0).astype(jnp.bfloat16).astype(jnp.float32)
    out_proj = jnp.einsum('hrn,hc->rnc', x_norm, w_out)
    gating = jax.nn.sigmoid(jnp.einsum('rnc,cd->rnd', zn_bf.astype(jnp.float32), w_gate))
    return gating * out_proj

def tri_out(left, right):
    return jnp.einsum('cik,cjk->cij', left.astype(jnp.float32), right.astype(jnp.float32))

def one_crop(pair_crop, mask_crop, weights, probe_signs):
    chans = weights.shape[0]
    h4 = weights.shape[1] - 2 * chans
    zn = norm_axis(pair_crop.astype(jnp.float32), 2).astype(jnp.bfloat16)
    mask = mask_crop.astype(jnp.float32)
    mask_pair = mask[:, None] * mask[None, :]
    w_all = weights.astype(jnp.float32)
    probe = (2 * probe_signs - 1).astype(jnp.float32) * (1.0 / jnp.sqrt(jnp.float32(chans)))
    w_in, w_head = (w_all[:, :h4], w_all[:, h4:])
    v_in, v_head = (probe[:, :h4], probe[:, h4:])
    fin = lambda w: project_in(w, zn, mask_pair)
    (a_f, b_f), pull_in = jax.vjp(fin, w_in)
    _, (ta_f, tb_f) = jax.jvp(fin, (w_in,), (v_in,))
    a_bf, b_bf = (a_f.astype(jnp.bfloat16), b_f.astype(jnp.bfloat16))
    ta_bf, tb_bf = (ta_f.astype(jnp.bfloat16), tb_f.astype(jnp.bfloat16))
    x_bf = tri_out(a_bf, b_bf).astype(jnp.bfloat16)
    tx_bf = (tri_out(ta_bf, b_bf) + tri_out(a_bf, tb_bf)).astype(jnp.bfloat16)
    fhead = lambda w, xx: head(w, xx, zn)
    out, pull_head = jax.vjp(fhead, w_head, x_bf.astype(jnp.float32))
    _, t_out = jax.jvp(fhead, (w_head, x_bf.astype(jnp.float32)), (v_head, tx_bf.astype(jnp.float32)))
    total = CROPS * N * N
    cot = t_out * (1.0 / total)
    g_head, x_bar = pull_head(cot)
    xb_bf = x_bar.astype(jnp.bfloat16).astype(jnp.float32)
    a_bar = jnp.einsum('cij,cjk->cik', xb_bf, b_bf.astype(jnp.float32)).astype(jnp.bfloat16)
    b_bar = jnp.einsum('cij,cik->cjk', xb_bf, a_bf.astype(jnp.float32)).astype(jnp.bfloat16)
    g_in = pull_in((a_bar.astype(jnp.float32), b_bar.astype(jnp.float32)))[0]
    new_pair = (pair_crop.astype(jnp.float32) + out).astype(jnp.bfloat16)
    return (new_pair, jnp.concatenate([g_in, g_head], axis=1))

def reference(pair, crop_mask, weights, probe_signs):

    def step(items):
        return one_crop(items[0], items[1], weights, probe_signs)
    new_pairs, grads = lax.map(step, (pair, crop_mask))
    return (new_pairs, lax.optimization_barrier(jnp.sum(grads, axis=0)))
```

```python
import jax
import jax.numpy as jnp
from jax import lax
from jax.experimental import pallas as pl
from jax.experimental.pallas import tpu as pltpu
from jax.sharding import PartitionSpec as P

MESH = pl.DeviceIdType.MESH
F32 = jnp.float32
BF16 = jnp.bfloat16
EPS = 1e-05
TOTAL = 8 * 256 * 256
NT = (((1,), (1,)), ((), ()))
NN = (((1,), (0,)), ((), ()))
TN = (((0,), (0,)), ((), ()))


def dot(a, b, dims):
    return lax.dot_general(a, b, dims, preferred_element_type=F32)


def mean0(value):
    return jnp.mean(value, axis=0, keepdims=True)


def loop(lo, hi, body):
    def step(i, carry):
        body(i)
        return carry

    lax.fori_loop(lo, hi, step, 0)


def kernel(
    pair_ref, cmask_ref, w_ref, s_ref,
    out_ref, curv_ref,
    wt, vt, wq, pg, mk, zn, fac, tmp,
    sf, rf, xs, xr, zs, zr, outs, xb4, xbr, xbs, rx, as_, ar,
    gg, hs, hr, gi, us, ur, vb, wb, ft,
    mv_s, mv_r, ag_s, ag_r, xs_s, xs_r, q_s, q_r, v_s, v_r, o_s, o_r, l_s,
):
    crop = lax.axis_index("crop")
    axial = lax.axis_index("axial")
    xy = lax.div(axial, 4)
    hi = lax.rem(axial, 4)
    half = lax.div(crop, 4)
    q = lax.rem(crop, 4)
    v = 2 * hi + half

    def dev(c, a):
        return {"crop": c, "axial": a}

    def xy_dev(p):
        return dev(crop, 4 * p + hi)

    def q_dev(p):
        return dev(4 * half + p, axial)

    def v_dev(p):
        return dev(4 * lax.rem(p, 2) + q, 4 * xy + lax.div(p, 2))

    dst_c = 4 * lax.rem(crop, 2) + hi
    dst_a = 4 * xy + lax.div(crop, 2)
    src_c = 2 * hi + half
    src_a = 4 * xy + q
    moved = jnp.logical_or(dst_c != crop, dst_a != axial)
    stays = jnp.logical_not(moved)

    def rcopy(src, dst, ssem, rsem, to):
        return pltpu.make_async_remote_copy(
            src_ref=src, dst_ref=dst, send_sem=ssem, recv_sem=rsem,
            device_id=to, device_id_type=MESH,
        )

    barrier = pltpu.get_barrier_semaphore()

    def greet(to):
        pl.semaphore_signal(barrier, inc=1, device_id=to, device_id_type=MESH)

    loop(1, 16, lambda d: greet(xy_dev(lax.rem(xy + d, 16))))
    loop(1, 8, lambda d: greet(v_dev(lax.rem(v + d, 8))))
    loop(1, 4, lambda d: greet(q_dev(lax.rem(q + d, 4))))

    @pl.when(moved)
    def _():
        greet(dev(dst_c, dst_a))
        greet(dev(src_c, src_a))

    for t in range(6):
        cols = slice(128 * t, 128 * t + 128)
        wt[cols, :] = w_ref[:, cols].astype(F32).T.astype(BF16)
        probe = (2 * s_ref[:, cols] - 1).astype(F32) * (1.0 / jnp.sqrt(F32(128)))
        vt[cols, :] = probe.T.astype(BF16)
    for t in range(4):
        rows = pl.ds(pl.multiple_of(128 * t + 32 * q, 32), 32)
        wq[32 * t : 32 * t + 32, :] = wt[rows, :]
        wq[128 + 32 * t : 160 + 32 * t, :] = vt[rows, :]

    @pl.when(moved)
    def _():
        pl.semaphore_wait(barrier, 27)

    @pl.when(stays)
    def _():
        pl.semaphore_wait(barrier, 25)

    def put(lo, val):
        for k in range(2):
            tmp[pl.ds(2048 * k + lo, 32, stride=16), :] = val[:, 128 * k : 128 * k + 128]

    def get(lo):
        parts = [tmp[pl.ds(2048 * k + lo, 32, stride=16), :] for k in range(2)]
        return jnp.concatenate(parts, axis=1)

    def put_flat(i, val):
        for k in range(2):
            rows = pl.ds(pl.multiple_of(2048 * k + 128 * i, 128), 128)
            tmp[rows, :] = val[:, 128 * k : 128 * k + 128]

    def get_flat(i):
        parts = [
            tmp[pl.ds(pl.multiple_of(2048 * k + 128 * i, 128), 128), :] for k in range(2)
        ]
        return jnp.concatenate(parts, axis=1).reshape(8, 16, 256)

    def mv_pair():
        return rcopy(
            pair_ref, pg.at[pl.ds(4 * hi, 4)], mv_s.at[0], mv_r.at[0], dev(dst_c, dst_a)
        )

    def mv_mask():
        return rcopy(cmask_ref, mk, mv_s.at[1], mv_r.at[1], dev(dst_c, dst_a))

    @pl.when(moved)
    def _():
        mv_pair().start()
        mv_mask().start()
        mv_pair().wait()
        mv_mask().wait()

    @pl.when(stays)
    def _():
        one = pltpu.make_async_copy(pair_ref, pg.at[pl.ds(4 * q, 4)], l_s.at[0])
        two = pltpu.make_async_copy(cmask_ref, mk, l_s.at[1])
        one.start()
        two.start()
        one.wait()
        two.wait()

    q1 = q + 1 - 2 * lax.rem(q, 2)
    q2 = lax.rem(q + 2, 4)
    q3 = lax.rem(q1 + 2, 4)

    def block(p):
        return pg.at[pl.ds(4 * p, 4)]

    near = rcopy(block(q), block(q), ag_s.at[0], ag_r.at[0], q_dev(q1))
    far = rcopy(block(q), block(q), ag_s.at[1], ag_r.at[1], q_dev(q2))
    pass_on = rcopy(block(q2), block(q2), ag_s.at[2], ag_r.at[2], q_dev(q1))
    far.start()
    near.start()

    lanes = lax.broadcasted_iota(jnp.int32, (1, 256), 1)

    def project(r):
        rows = pg[r].astype(F32)
        centered = rows - jnp.mean(rows, axis=1, keepdims=True)
        var = jnp.mean(centered * centered, axis=1, keepdims=True)
        znr = (centered * lax.rsqrt(var + EPS)).astype(BF16)
        zn[r] = znr
        proj = dot(wq[...], znr, NT)
        m = mk[...].astype(F32)
        mi = jnp.sum(jnp.where(lanes == 16 * xy + r, m, 0.0), axis=1, keepdims=True)
        mrow = m * mi
        for side in range(2):
            lo = 64 * side
            p, g = proj[lo : lo + 32], proj[lo + 32 : lo + 64]
            tp, tg = proj[128 + lo : 160 + lo], proj[160 + lo : 192 + lo]
            s = jax.nn.sigmoid(g)
            fp = s * mrow
            fg = p * (fp * (1.0 - s))
            fac[r, lo : lo + 32, :] = fp
            fac[r, lo + 32 : lo + 64, :] = fg
            put(512 * side + r, fp * p)
            put(1024 + 512 * side + r, fg * tg + fp * tp)

    loop(0, 4, lambda i: project(4 * q + i))
    far.wait_recv()
    pass_on.start()
    loop(0, 4, lambda i: project(4 * q2 + i))
    near.wait_recv()
    loop(0, 4, lambda i: project(4 * q1 + i))
    pass_on.wait_recv()
    loop(0, 4, lambda i: project(4 * q3 + i))
    near.wait_send()
    far.wait_send()
    pass_on.wait_send()

    def xy_start(n, src, dst):
        pltpu.make_async_copy(src(xy), dst(xy), l_s.at[0]).start()

        def send(d):
            p = lax.rem(xy + d, 16)
            rcopy(src(p), dst(xy), xs_s.at[n, p], xs_r.at[n, xy], xy_dev(p)).start()

        loop(1, 16, send)

    def xy_wait(n, src, dst):
        pltpu.make_async_copy(src(xy), dst(xy), l_s.at[0]).wait()

        def done(d):
            p = lax.rem(xy + d, 16)
            both = rcopy(src(p), dst(p), xs_s.at[n, p], xs_r.at[n, p], xy_dev(p))
            both.wait_send()
            both.wait_recv()

        loop(1, 16, done)

    def q_start(n, src, dst):
        pltpu.make_async_copy(src(q), dst(q), l_s.at[1 + n]).start()

        def send(d):
            p = lax.rem(q + d, 4)
            rcopy(src(p), dst(q), q_s.at[n, p], q_r.at[n, q], q_dev(p)).start()

        loop(1, 4, send)

    def q_wait(n, src, dst):
        pltpu.make_async_copy(src(q), dst(q), l_s.at[1 + n]).wait()

        def done(d):
            p = lax.rem(q + d, 4)
            both = rcopy(src(p), dst(p), q_s.at[n, p], q_r.at[n, p], q_dev(p))
            both.wait_send()
            both.wait_recv()

        loop(1, 4, done)

    def rows_of(p, n):
        return pl.ds(pl.multiple_of(n * p, n), n)

    def pack(i):
        sf[lax.div(i, 4), pl.ds(8 * lax.rem(i, 4), 8)] = get_flat(i).astype(BF16)

    loop(0, 16, pack)
    one = (0, lambda p: sf.at[:, pl.ds(2 * p, 2)], lambda p: rf.at[:, :, rows_of(p, 16), :])
    xy_start(*one)
    xy_wait(*one)

    for c in range(2):
        x = dot(rf[0, c], rf[1, c], NT)
        tx = dot(rf[2, c], rf[1, c], NT) + dot(rf[0, c], rf[3, c], NT)
        xs[0, c] = x.astype(BF16)
        xs[1, c] = tx.astype(BF16)

    two = (1, lambda p: xs.at[:, :, rows_of(p, 16), :], lambda p: xr.at[:, pl.ds(2 * p, 2)])
    xy_start(*two)
    xy_wait(*two)

    def spread(src):
        def body(i):
            val = src[lax.div(i, 4), pl.ds(8 * lax.rem(i, 4), 8)].astype(F32)
            put_flat(i, val.reshape(128, 256))

        loop(0, 8, body)

    spread(xr)

    def turn(r):
        zs[0, r] = get(r).astype(BF16)
        zs[1, r] = get(512 + r).astype(BF16)

    loop(0, 16, turn)
    three = (0, lambda p: zs.at[:, pl.ds(4 * p, 4)], lambda p: zr.at[:, :, rows_of(p, 32), :])
    q_start(*three)
    q_wait(*three)

    gg[...] = jnp.zeros_like(gg)
    hs[...] = jnp.zeros_like(hs)

    def head(r):
        znr = zn[4 * q + r]
        x = zr[0, r].astype(F32)
        tx = zr[1, r].astype(F32)
        c = x - mean0(x)
        rs = lax.rsqrt(mean0(c * c) + EPS)
        xnb = (c * rs).astype(BF16)
        tc = tx - mean0(tx)
        slope = -0.5 * (rs * rs * rs)
        drs = slope * mean0(2.0 * c * tc)
        dxnb = (tc * rs + c * drs).astype(BF16)
        g = dot(wt[512:640, :], znr, NT)
        dg = dot(vt[512:640, :], znr, NT)
        w_out = wt[640:768, :]
        out = dot(w_out, xnb, NN)
        dout = dot(w_out, dxnb, NN) + dot(vt[640:768, :], xnb, NN)
        s = jax.nn.sigmoid(g)
        sp = s * (1.0 - s)
        y = s * out
        ybar = (sp * dg * out + s * dout) * (1.0 / TOTAL)
        gbar = (ybar * out * sp).astype(BF16)
        obar = (ybar * s).astype(BF16)
        hs[0:128, :] += dot(gbar, znr, NN)
        hs[128:256, :] += dot(obar, xnb, NT)
        xnbar = dot(w_ref[:, 640:768], obar, NN).astype(BF16).astype(F32)
        rsbar = jnp.sum(xnbar * c, axis=0, keepdims=True)
        cbar = xnbar * rs + c * (rsbar * slope * (2.0 / 128))
        xb4[r] = (cbar - mean0(cbar)).astype(BF16)
        outs[r] = (pg[4 * q + r].astype(F32) + y.T).astype(BF16)

    loop(0, 4, head)

    four = (1, lambda p: xb4.at[:, rows_of(p, 32), :], lambda p: xbr.at[pl.ds(4 * p, 4)])
    five = (2, lambda p: hs.at[rows_of(p, 64), :], lambda p: hr.at[p])
    q_start(*four)

    def back():
        return rcopy(outs, out_ref, o_s, o_r, dev(src_c, src_a))

    def keep():
        return pltpu.make_async_copy(outs, out_ref, o_s)

    @pl.when(moved)
    def _():
        back().start()

    @pl.when(stays)
    def _():
        keep().start()

    q_wait(*four)
    q_start(*five)

    def turn_back(r):
        put(r, xbr[r].astype(F32))

    loop(0, 16, turn_back)

    def pack_back(i):
        xbs[pl.ds(8 * i, 8)] = get_flat(i).astype(BF16)

    loop(0, 4, pack_back)
    six = (2, lambda p: xbs.at[pl.ds(2 * p, 2)], lambda p: rx.at[:, rows_of(p, 16), :])
    xy_start(*six)
    xy_wait(*six)

    for c in range(2):
        as_[0, c] = dot(rx[c], rf[1, c], NN).astype(BF16)
        as_[1, c] = dot(rx[c], rf[0, c], TN).astype(BF16)

    seven = (3, lambda p: as_.at[:, :, rows_of(p, 16), :], lambda p: ar.at[:, pl.ds(2 * p, 2)])
    xy_start(*seven)
    q_wait(*five)
    xy_wait(*seven)
    spread(ar)
    gi[...] = jnp.zeros_like(gi)

    def grad(r):
        ab = get(r)
        bb = get(512 + r)
        d = (fac[r] * jnp.concatenate([ab, ab, bb, bb], axis=0)).astype(BF16)
        gi[...] += dot(d, zn[r], NN)

    loop(0, 16, grad)

    gg[...] = hr[0] + hr[1] + hr[2] + hr[3]
    for p in range(16):
        us[p, 0] = gi[8 * p : 8 * p + 4, :]
        us[p, 1] = gi[8 * p + 4 : 8 * p + 8, :]
        us[p, 2] = gg[4 * p : 4 * p + 4, :]
    eight = (4, lambda p: us.at[p], lambda p: ur.at[p])
    xy_start(*eight)
    xy_wait(*eight)
    total = ur[0]
    for p in range(1, 16):
        total = total + ur[p]
    vb[v] = total

    def v_copy(d, slot):
        p = lax.rem(v + d, 8)
        mine = v if slot else p
        return rcopy(vb.at[v], vb.at[mine], v_s.at[p], v_r.at[mine], v_dev(p))

    loop(1, 8, lambda d: v_copy(d, True).start())

    def v_done(d):
        both = v_copy(d, False)
        both.wait_send()
        both.wait_recv()

    loop(1, 8, v_done)
    total = vb[0]
    for p in range(1, 8):
        total = total + vb[p]
    wb[q, xy] = total

    def gather(d, mine):
        p = lax.rem(xy + d, 16)
        slot = xy if mine else p
        return rcopy(wb.at[q, xy], wb.at[q, slot], xs_s.at[5, p], xs_r.at[5, slot], xy_dev(p))

    loop(1, 16, lambda d: gather(d, True).start())

    def gathered(d):
        both = gather(d, False)
        both.wait_send()
        both.wait_recv()

    loop(1, 16, gathered)

    def column(d, mine):
        p = lax.rem(q + d, 4)
        slot = q if mine else p
        return rcopy(wb.at[q], wb.at[slot], q_s.at[3, p], q_r.at[3, slot], q_dev(p))

    loop(1, 4, lambda d: column(d, True).start())

    def columned(d):
        both = column(d, False)
        both.wait_send()
        both.wait_recv()

    loop(1, 4, columned)
    for p in range(4):
        for k in range(16):
            lo = 128 * (k // 4) + 32 * p + 8 * (k % 4)
            ft[lo : lo + 4, :] = wb[p, k, 0]
            ft[lo + 4 : lo + 8, :] = wb[p, k, 1]
            lo = 512 + 64 * p + 4 * k
            ft[lo : lo + 4, :] = wb[p, k, 2]
    for t in range(6):
        cols = slice(128 * t, 128 * t + 128)
        curv_ref[:, cols] = ft[cols, :].T

    @pl.when(moved)
    def _():
        back().wait()

    @pl.when(stays)
    def _():
        keep().wait()


def shards(pair, crop_mask, weights, probe_signs):
    vmem = pl.BlockSpec(memory_space=pltpu.VMEM)
    dma = pltpu.SemaphoreType.DMA
    out, curv = pl.pallas_call(
        kernel,
        out_shape=(
            jax.ShapeDtypeStruct((4, 256, 128), BF16),
            jax.ShapeDtypeStruct((128, 768), F32),
        ),
        in_specs=[vmem] * 4,
        out_specs=(pl.BlockSpec(memory_space=pl.ANY), vmem),
        scratch_shapes=[
            pltpu.VMEM((768, 128), BF16),
            pltpu.VMEM((768, 128), BF16),
            pltpu.VMEM((256, 128), BF16),
            pltpu.VMEM((16, 256, 128), BF16),
            pltpu.VMEM((1, 256), jnp.int32),
            pltpu.VMEM((16, 256, 128), BF16),
            pltpu.VMEM((16, 128, 256), F32),
            pltpu.VMEM((4096, 128), F32),
            pltpu.VMEM((4, 32, 16, 256), BF16),
            pltpu.VMEM((4, 2, 256, 256), BF16),
            pltpu.VMEM((2, 2, 256, 256), BF16),
            pltpu.VMEM((2, 32, 16, 256), BF16),
            pltpu.VMEM((2, 16, 32, 256), BF16),
            pltpu.VMEM((2, 4, 128, 256), BF16),
            pltpu.VMEM((4, 256, 128), BF16),
            pltpu.VMEM((4, 128, 256), BF16),
            pltpu.VMEM((16, 32, 256), BF16),
            pltpu.VMEM((32, 16, 256), BF16),
            pltpu.VMEM((2, 256, 256), BF16),
            pltpu.VMEM((2, 2, 256, 256), BF16),
            pltpu.VMEM((2, 32, 16, 256), BF16),
            pltpu.VMEM((64, 128), F32),
            pltpu.VMEM((256, 128), F32),
            pltpu.VMEM((4, 64, 128), F32),
            pltpu.VMEM((128, 128), F32),
            pltpu.VMEM((16, 3, 4, 128), F32),
            pltpu.VMEM((16, 3, 4, 128), F32),
            pltpu.VMEM((8, 3, 4, 128), F32),
            pltpu.VMEM((4, 16, 3, 4, 128), F32),
            pltpu.VMEM((768, 128), F32),
            dma((2,)), dma((2,)), dma((3,)), dma((3,)),
            dma((6, 16)), dma((6, 16)), dma((4, 4)), dma((4, 4)),
            dma((8,)), dma((8,)), dma, dma, dma((4,)),
        ],
        compiler_params=pltpu.CompilerParams(
            collective_id=0, has_side_effects=True, vmem_limit_bytes=48 * 2**20
        ),
    )(pair[0], crop_mask, weights, probe_signs)
    return out[None], curv


def solution(mesh):
    placed = (P("crop", "axial", None, None), P("crop", None), P(), P())
    return jax.shard_map(
        shards,
        mesh=mesh,
        in_specs=placed,
        out_specs=(P("crop", "axial", None, None), P()),
        check_vma=False,
    )
```

```python
import jax
import jax.numpy as jnp
from jax import lax
from jax.experimental import pallas as pl
from jax.experimental.pallas import tpu as pltpu
from jax.sharding import PartitionSpec as P

MESH = pl.DeviceIdType.MESH
F32 = jnp.float32
BF16 = jnp.bfloat16
EPS = 1e-05
TOTAL = 8 * 256 * 256
NT = (((1,), (1,)), ((), ()))
NN = (((1,), (0,)), ((), ()))
TN = (((0,), (0,)), ((), ()))


def dot(a, b, dims):
    return lax.dot_general(a, b, dims, preferred_element_type=F32)


def mean0(value):
    return jnp.mean(value, axis=0, keepdims=True)


BLOCK_OF = (6, 2, 1, 5, 0, 4, 3, 7)
PLACE_OF = (
    (2, 3, 0, 1), (0, 1, 3, 2), (1, 3, 2, 0), (2, 1, 0, 3),
    (3, 2, 0, 1), (0, 1, 3, 2), (1, 2, 3, 0), (3, 0, 1, 2),
)


def table(index, values):
    found = 0
    for k, value in enumerate(values):
        found = found + jnp.where(index == k, value, 0)
    return found


def loop(lo, hi, body):
    def step(i, carry):
        body(i)
        return carry

    lax.fori_loop(lo, hi, step, 0)


def kernel(
    pair_ref, cmask_ref, w_any, s_any,
    out_ref, curv_ref,
    pv, cm, w_ref, s_ref,
    wt, vt, wq, pg, mk, zn, fac, tmp,
    sf, rf, xs, xr, zs, zr, outs, xb4, xbr, xbs, rx, as_, ar,
    hsum, hs, hr, gi, us, ur, vb, wb, ft,
    in_s, mv_s, mv_r, ag_s, ag_r, xs_s, xs_r, q_s, q_r, v_s, v_r, o_s, o_r, lx_s, lq_s,
):
    crop = lax.axis_index("crop")
    axial = lax.axis_index("axial")
    xy = lax.div(axial, 4)
    hi = lax.rem(axial, 4)
    half = lax.div(crop, 4)
    q = lax.rem(crop, 4)
    v = 2 * hi + half

    def dev(c, a):
        return {"crop": c, "axial": a}

    def xy_dev(p):
        return dev(crop, 4 * p + hi)

    def q_dev(p):
        return dev(4 * half + p, axial)

    def v_dev(p):
        return dev(4 * lax.rem(p, 2) + q, 4 * xy + lax.div(p, 2))

    dst = table(
        4 * crop + hi, [4 * BLOCK_OF[c] + PLACE_OF[c][k] for c in range(8) for k in range(4)]
    )
    home = {4 * BLOCK_OF[c] + PLACE_OF[c][k]: 4 * c + k for c in range(8) for k in range(4)}
    homes = [home[k] for k in range(32)]
    src = table(4 * v + q, homes)
    slots = [table(v, [homes[4 * b + p] % 4 for b in range(8)]) for p in range(4)]

    def slot(p):
        return table(p, slots)

    dst_v, dst_q = lax.div(dst, 4), lax.rem(dst, 4)
    dst_c = 4 * lax.rem(dst_v, 2) + dst_q
    dst_a = 4 * xy + lax.div(dst_v, 2)
    src_c = lax.div(src, 4)
    src_a = 4 * xy + lax.rem(src, 4)
    moved = dst != 4 * v + q
    stays = jnp.logical_not(moved)

    def rcopy(src, dst, ssem, rsem, to):
        return pltpu.make_async_remote_copy(
            src_ref=src, dst_ref=dst, send_sem=ssem, recv_sem=rsem,
            device_id=to, device_id_type=MESH,
        )

    barrier = pltpu.get_barrier_semaphore()

    def greet(to):
        pl.semaphore_signal(barrier, inc=1, device_id=to, device_id_type=MESH)

    loop(1, 16, lambda d: greet(xy_dev(lax.rem(xy + d, 16))))
    loop(1, 8, lambda d: greet(v_dev(lax.rem(v + d, 8))))
    loop(1, 4, lambda d: greet(q_dev(lax.rem(q + d, 4))))

    @pl.when(moved)
    def _():
        greet(dev(dst_c, dst_a))
        greet(dev(src_c, src_a))

    loads = [
        pltpu.make_async_copy(a, b, in_s.at[k])
        for k, (a, b) in enumerate(
            ((w_any, w_ref), (s_any, s_ref), (cmask_ref, cm), (pair_ref, pv))
        )
    ]
    for load in loads:
        load.start()
    loads[0].wait()
    loads[1].wait()
    for t in range(6):
        cols = slice(128 * t, 128 * t + 128)
        wt[cols, :] = w_ref[:, cols].astype(F32).T.astype(BF16)
        probe = (2 * s_ref[:, cols] - 1).astype(F32) * (1.0 / jnp.sqrt(F32(128)))
        vt[cols, :] = probe.T.astype(BF16)
    for t in range(4):
        rows = pl.ds(pl.multiple_of(128 * t + 32 * q, 32), 32)
        wq[32 * t : 32 * t + 32, :] = wt[rows, :]
        wq[128 + 32 * t : 160 + 32 * t, :] = vt[rows, :]
    loads[2].wait()
    loads[3].wait()

    @pl.when(moved)
    def _():
        pl.semaphore_wait(barrier, 27)

    @pl.when(stays)
    def _():
        pl.semaphore_wait(barrier, 25)

    def put(k, lo, val):
        tmp[pl.ds(2048 * k + lo, 32, stride=16), :] = val

    def get(k, lo):
        return tmp[pl.ds(2048 * k + lo, 32, stride=16), :]

    def flat(k, i):
        return pl.ds(pl.multiple_of(2048 * k + 128 * i, 128), 128)

    def spread(k, src):
        def body(i):
            val = src[k, lax.div(i, 4), pl.ds(8 * lax.rem(i, 4), 8)].astype(F32)
            tmp[flat(k, i), :] = val.reshape(128, 128)

        loop(0, 8, body)

    own = slot(q)

    def lanes_of(k):
        return slice(128 * k, 128 * k + 128)

    def mv_pair(k):
        return rcopy(
            pv.at[:, lanes_of(k)], pg.at[pl.ds(4 * hi, 4), lanes_of(k)],
            mv_s.at[k], mv_r.at[k], dev(dst_c, dst_a),
        )

    def mv_mask():
        return rcopy(cm, mk, mv_s.at[2], mv_r.at[2], dev(dst_c, dst_a))

    def own_pair(k):
        return pltpu.make_async_copy(
            pv.at[:, lanes_of(k)], pg.at[pl.ds(4 * own, 4), lanes_of(k)], mv_r.at[k]
        )

    def own_mask():
        return pltpu.make_async_copy(cm, mk, mv_r.at[2])

    @pl.when(moved)
    def _():
        mv_mask().start()
        mv_pair(0).start()
        mv_pair(1).start()

    @pl.when(stays)
    def _():
        own_mask().start()
        own_pair(0).start()
        own_pair(1).start()

    q1 = q + 1 - 2 * lax.rem(q, 2)
    q2 = lax.rem(q + 2, 4)
    q3 = lax.rem(q1 + 2, 4)

    def block(k, p):
        return pg.at[pl.ds(4 * slot(p), 4), lanes_of(k)]

    def near(k):
        return rcopy(block(k, q), block(k, q), ag_s.at[k, 0], ag_r.at[k, 0], q_dev(q1))

    def far(k):
        return rcopy(block(k, q), block(k, q), ag_s.at[k, 1], ag_r.at[k, 1], q_dev(q2))

    def pass_on(k):
        return rcopy(block(k, q2), block(k, q2), ag_s.at[k, 2], ag_r.at[k, 2], q_dev(q1))

    def arrived(k):
        @pl.when(moved)
        def _():
            if k == 0:
                mv_mask().wait()
            mv_pair(k).wait()

        @pl.when(stays)
        def _():
            if k == 0:
                own_mask().wait()
            own_pair(k).wait()

    iota = lax.broadcasted_iota(jnp.int32, (1, 256), 1)

    def project(k, r):
        rows = pg[r, lanes_of(k), :].astype(F32)
        centered = rows - jnp.mean(rows, axis=1, keepdims=True)
        var = jnp.mean(centered * centered, axis=1, keepdims=True)
        znr = (centered * lax.rsqrt(var + EPS)).astype(BF16)
        zn[r, lanes_of(k), :] = znr
        proj = dot(wq[...], znr, NT)
        m = mk[...].astype(F32)
        mi = jnp.sum(jnp.where(iota == 16 * xy + r, m, 0.0), axis=1, keepdims=True)
        mrow = m[:, lanes_of(k)] * mi
        for side in range(2):
            lo = 64 * side
            p, g = proj[lo : lo + 32], proj[lo + 32 : lo + 64]
            tp, tg = proj[128 + lo : 160 + lo], proj[160 + lo : 192 + lo]
            s = jax.nn.sigmoid(g)
            fp = s * mrow
            fg = p * (fp * (1.0 - s))
            fac[k, r, lo : lo + 32, :] = fp
            fac[k, r, lo + 32 : lo + 64, :] = fg
            put(k, 512 * side + r, fp * p)
            put(k, 1024 + 512 * side + r, fg * tg + fp * tp)

    def project4(k, p):
        for i in range(4):
            project(k, 4 * p + i)

    def xy_start(n, src, dst):
        pltpu.make_async_copy(src(xy), dst(xy), lx_s.at[n]).start()

        def send(d):
            p = lax.rem(xy + d, 16)
            rcopy(src(p), dst(xy), xs_s.at[n, p], xs_r.at[n, xy], xy_dev(p)).start()

        loop(1, 16, send)

    def xy_wait(n, src, dst):
        pltpu.make_async_copy(src(xy), dst(xy), lx_s.at[n]).wait()

        def done(d):
            p = lax.rem(xy + d, 16)
            both = rcopy(src(p), dst(p), xs_s.at[n, p], xs_r.at[n, p], xy_dev(p))
            both.wait_send()
            both.wait_recv()

        loop(1, 16, done)

    def q_start(n, src, dst):
        pltpu.make_async_copy(src(q), dst(q), lq_s.at[n]).start()

        def send(d):
            p = lax.rem(q + d, 4)
            rcopy(src(p), dst(q), q_s.at[n, p], q_r.at[n, q], q_dev(p)).start()

        loop(1, 4, send)

    def q_wait(n, src, dst):
        pltpu.make_async_copy(src(q), dst(q), lq_s.at[n]).wait()

        def done(d):
            p = lax.rem(q + d, 4)
            both = rcopy(src(p), dst(p), q_s.at[n, p], q_r.at[n, p], q_dev(p))
            both.wait_send()
            both.wait_recv()

        loop(1, 4, done)

    def rows_of(p, n):
        return pl.ds(pl.multiple_of(n * p, n), n)

    def ab(k):
        return (
            k,
            lambda p: sf.at[k, :, pl.ds(2 * p, 2)],
            lambda p: rf.at[k, :, :, rows_of(p, 16), :],
        )

    for k in range(2):
        arrived(k)
        far(k).start()
        near(k).start()
        project4(k, slot(q))
        near(k).wait_recv()
        project4(k, slot(q1))
        far(k).wait_recv()
        pass_on(k).start()
        project4(k, slot(q2))
        pass_on(k).wait_recv()
        project4(k, slot(q3))

        def pack(i):
            val = tmp[flat(k, i), :].reshape(8, 16, 128)
            sf[k, lax.div(i, 4), pl.ds(8 * lax.rem(i, 4), 8)] = val.astype(BF16)

        loop(0, 16, pack)
        xy_start(*ab(k))
    for k in range(2):
        near(k).wait_send()
        far(k).wait_send()
        pass_on(k).wait_send()
    for k in range(2):
        xy_wait(*ab(k))

    def xx(k):
        return (
            2 + k,
            lambda p: xs.at[k, :, :, rows_of(p, 16), :],
            lambda p: xr.at[k, :, pl.ds(2 * p, 2)],
        )

    def both(ref, *at):
        return jnp.concatenate([ref[(0, *at)], ref[(1, *at)]], axis=1)

    for k in range(2):
        for c in range(2):
            a, b, ta, tb = [both(rf, n, c) for n in range(4)]
            b, tb = b[lanes_of(k)], tb[lanes_of(k)]
            x = dot(a, b, NT)
            tx = dot(jnp.concatenate([ta, a], axis=1), jnp.concatenate([b, tb], axis=1), NT)
            xs[k, 0, c] = x.astype(BF16)
            xs[k, 1, c] = tx.astype(BF16)
        xy_start(*xx(k))

    def zz(k):
        return (
            k,
            lambda p: zs.at[k, :, pl.ds(4 * slot(p), 4)],
            lambda p: zr.at[k, :, :, rows_of(p, 32), :],
        )

    for k in range(2):
        xy_wait(*xx(k))
        spread(k, xr)

        def turn(r):
            zs[k, 0, r] = get(k, r).astype(BF16)
            zs[k, 1, r] = get(k, 512 + r).astype(BF16)

        loop(0, 16, turn)
        q_start(*zz(k))

    hs[...] = jnp.zeros_like(hs)

    def head(k, r):
        znr = zn[4 * own + r, lanes_of(k), :]
        x = zr[k, 0, r].astype(F32)
        tx = zr[k, 1, r].astype(F32)
        c = x - mean0(x)
        rs = lax.rsqrt(mean0(c * c) + EPS)
        xnb = (c * rs).astype(BF16)
        tc = tx - mean0(tx)
        slope = -0.5 * (rs * rs * rs)
        drs = slope * mean0(2.0 * c * tc)
        dxnb = (tc * rs + c * drs).astype(BF16)
        g = dot(wt[512:640, :], znr, NT)
        dg = dot(vt[512:640, :], znr, NT)
        w_out = wt[640:768, :]
        out = dot(w_out, xnb, NN)
        dout = dot(w_out, dxnb, NN) + dot(vt[640:768, :], xnb, NN)
        s = jax.nn.sigmoid(g)
        sp = s * (1.0 - s)
        y = s * out
        ybar = (sp * dg * out + s * dout) * (1.0 / TOTAL)
        gbar = (ybar * out * sp).astype(BF16)
        obar = (ybar * s).astype(BF16)
        xnbar = dot(w_ref[:, 640:768], obar, NN).astype(BF16).astype(F32)
        rsbar = jnp.sum(xnbar * c, axis=0, keepdims=True)
        cbar = xnbar * rs + c * (rsbar * slope * (2.0 / 128))
        xb4[k, r] = (cbar - mean0(cbar)).astype(BF16)
        row = pg[4 * own + r, lanes_of(k), :].astype(F32)
        outs[r, lanes_of(k), :] = (row + y.T).astype(BF16)
        return dot(gbar, znr, NN), dot(obar, xnb, NT)

    def heads(k, i):
        first, second = head(k, 2 * i), head(k, 2 * i + 1)
        hs[0:128, :] += first[0] + second[0]
        hs[128:256, :] += first[1] + second[1]

    def xb(k):
        return (
            2 + k,
            lambda p: xb4.at[k, :, rows_of(p, 32), :],
            lambda p: xbr.at[k, pl.ds(4 * slot(p), 4)],
        )

    five = (4, lambda p: hs.at[rows_of(p, 64), :], lambda p: hr.at[p])
    for k in range(2):
        q_wait(*zz(k))
        loop(0, 2, lambda i: heads(k, i))
        q_start(*xb(k))

    def back():
        return rcopy(outs, out_ref, o_s, o_r, dev(src_c, src_a))

    def keep():
        return pltpu.make_async_copy(outs, out_ref, o_s)

    def rr(k):
        return (
            4 + k,
            lambda p: xbs.at[k, pl.ds(2 * p, 2)],
            lambda p: rx.at[k, :, rows_of(p, 16), :],
        )

    for k in range(2):
        q_wait(*xb(k))
        loop(0, 16, lambda r: put(k, r, xbr[k, r].astype(F32)))

        def pack_back(i):
            val = tmp[flat(k, i), :].reshape(8, 16, 128)
            xbs[k, pl.ds(8 * i, 8)] = val.astype(BF16)

        loop(0, 4, pack_back)
        xy_start(*rr(k))

    q_start(*five)

    @pl.when(moved)
    def _():
        back().start()

    @pl.when(stays)
    def _():
        keep().start()

    for k in range(2):
        xy_wait(*rr(k))

    def aa(k):
        return (
            6 + k,
            lambda p: as_.at[k, :, :, rows_of(p, 16), :],
            lambda p: ar.at[k, :, pl.ds(2 * p, 2)],
        )

    for c in range(2):
        xbar = both(rx, c)
        abar = dot(xbar, both(rf, 1, c), NN).astype(BF16)
        bbar = dot(xbar, both(rf, 0, c), TN).astype(BF16)
        for k in range(2):
            as_[k, 0, c] = abar[:, lanes_of(k)]
            as_[k, 1, c] = bbar[:, lanes_of(k)]
    for k in range(2):
        xy_start(*aa(k))

    gi[...] = jnp.zeros_like(gi)
    q_wait(*five)
    hsum[...] = hr[0] + hr[1] + hr[2] + hr[3]
    for k in range(2):
        xy_wait(*aa(k))
        spread(k, ar)

        def grad(r):
            ra = get(k, r)
            rb = get(k, 512 + r)
            d = (fac[k, r] * jnp.concatenate([ra, ra, rb, rb], axis=0)).astype(BF16)
            return dot(d, zn[r, lanes_of(k), :], NN)

        def grads(i):
            gi[...] += (grad(4 * i) + grad(4 * i + 1)) + (grad(4 * i + 2) + grad(4 * i + 3))

        loop(0, 4, grads)

    for p in range(16):
        us[p, 0] = gi[8 * p : 8 * p + 4, :]
        us[p, 1] = gi[8 * p + 4 : 8 * p + 8, :]
        us[p, 2] = hsum[4 * p : 4 * p + 4, :]
    eight = (8, lambda p: us.at[p], lambda p: ur.at[p])
    xy_start(*eight)
    xy_wait(*eight)
    total = ur[0]
    for p in range(1, 16):
        total = total + ur[p]
    vb[v] = total

    def v_copy(d, slot):
        p = lax.rem(v + d, 8)
        mine = v if slot else p
        return rcopy(vb.at[v], vb.at[mine], v_s.at[p], v_r.at[mine], v_dev(p))

    loop(1, 8, lambda d: v_copy(d, True).start())

    def v_done(d):
        both = v_copy(d, False)
        both.wait_send()
        both.wait_recv()

    loop(1, 8, v_done)
    total = vb[0]
    for p in range(1, 8):
        total = total + vb[p]
    wb[q, xy] = total

    def gather(d, mine):
        p = lax.rem(xy + d, 16)
        slot = xy if mine else p
        return rcopy(wb.at[q, xy], wb.at[q, slot], xs_s.at[9, p], xs_r.at[9, slot], xy_dev(p))

    loop(1, 16, lambda d: gather(d, True).start())

    def gathered(d):
        both = gather(d, False)
        both.wait_send()
        both.wait_recv()

    loop(1, 16, gathered)

    def col(p, n, to):
        return rcopy(wb.at[p], wb.at[p], ag_s.at[2, n], ag_r.at[2, n], q_dev(to))

    col(q, 1, q2).start()
    col(q, 0, q1).start()
    col(q, 1, q2).wait_recv()
    col(q2, 2, q1).start()
    col(q, 0, q1).wait()
    col(q2, 2, q1).wait()
    col(q, 1, q2).wait_send()
    for p in range(4):
        for k in range(16):
            lo = 128 * (k // 4) + 32 * p + 8 * (k % 4)
            ft[lo : lo + 4, :] = wb[p, k, 0]
            ft[lo + 4 : lo + 8, :] = wb[p, k, 1]
            lo = 512 + 64 * p + 4 * k
            ft[lo : lo + 4, :] = wb[p, k, 2]
    for t in range(6):
        cols = slice(128 * t, 128 * t + 128)
        curv_ref[:, cols] = ft[cols, :].T

    @pl.when(moved)
    def _():
        back().wait()

    @pl.when(stays)
    def _():
        keep().wait()


def shards(pair, crop_mask, weights, probe_signs):
    vmem = pl.BlockSpec(memory_space=pltpu.VMEM)
    dma = pltpu.SemaphoreType.DMA
    out, curv = pl.pallas_call(
        kernel,
        out_shape=(
            jax.ShapeDtypeStruct((4, 256, 128), BF16),
            jax.ShapeDtypeStruct((128, 768), F32),
        ),
        in_specs=[pl.BlockSpec(memory_space=pl.ANY)] * 4,
        out_specs=(pl.BlockSpec(memory_space=pl.ANY), vmem),
        scratch_shapes=[
            pltpu.VMEM((4, 256, 128), BF16),
            pltpu.VMEM((1, 256), jnp.int32),
            pltpu.VMEM((128, 768), BF16),
            pltpu.VMEM((128, 768), jnp.int32),
            pltpu.VMEM((768, 128), BF16),
            pltpu.VMEM((768, 128), BF16),
            pltpu.VMEM((256, 128), BF16),
            pltpu.VMEM((16, 256, 128), BF16),
            pltpu.VMEM((1, 256), jnp.int32),
            pltpu.VMEM((16, 256, 128), BF16),
            pltpu.VMEM((2, 16, 128, 128), F32),
            pltpu.VMEM((4096, 128), F32),
            pltpu.VMEM((2, 4, 32, 16, 128), BF16),
            pltpu.VMEM((2, 4, 2, 256, 128), BF16),
            pltpu.VMEM((2, 2, 2, 256, 128), BF16),
            pltpu.VMEM((2, 2, 32, 16, 128), BF16),
            pltpu.VMEM((2, 2, 16, 32, 128), BF16),
            pltpu.VMEM((2, 2, 4, 128, 128), BF16),
            pltpu.VMEM((4, 256, 128), BF16),
            pltpu.VMEM((2, 4, 128, 128), BF16),
            pltpu.VMEM((2, 16, 32, 128), BF16),
            pltpu.VMEM((2, 32, 16, 128), BF16),
            pltpu.VMEM((2, 2, 256, 128), BF16),
            pltpu.VMEM((2, 2, 2, 256, 128), BF16),
            pltpu.VMEM((2, 2, 32, 16, 128), BF16),
            pltpu.VMEM((64, 128), F32),
            pltpu.VMEM((256, 128), F32),
            pltpu.VMEM((4, 64, 128), F32),
            pltpu.VMEM((128, 128), F32),
            pltpu.VMEM((16, 3, 4, 128), F32),
            pltpu.VMEM((16, 3, 4, 128), F32),
            pltpu.VMEM((8, 3, 4, 128), F32),
            pltpu.VMEM((4, 16, 3, 4, 128), F32),
            pltpu.VMEM((768, 128), F32),
            dma((4,)), dma((3,)), dma((3,)), dma((3, 3)), dma((3, 3)),
            dma((10, 16)), dma((10, 16)), dma((5, 4)), dma((5, 4)),
            dma((8,)), dma((8,)), dma, dma, dma((9,)), dma((5,)),
        ],
        compiler_params=pltpu.CompilerParams(
            collective_id=0, has_side_effects=True, vmem_limit_bytes=48 * 2**20
        ),
    )(pair[0], crop_mask, weights, probe_signs)
    return out[None], curv


def solution(mesh):
    placed = (P("crop", "axial", None, None), P("crop", None), P(), P())
    return jax.shard_map(
        shards,
        mesh=mesh,
        in_specs=placed,
        out_specs=(P("crop", "axial", None, None), P()),
        check_vma=False,
    )
```

```python
import jax
import jax.numpy as jnp
from jax import lax
from jax.experimental import pallas as pl
from jax.experimental.pallas import tpu as pltpu
from jax.sharding import PartitionSpec as P

MESH = pl.DeviceIdType.MESH
F32 = jnp.float32
BF16 = jnp.bfloat16
EPS = 1e-05
TOTAL = 8 * 256 * 256
NT = (((1,), (1,)), ((), ()))
NN = (((1,), (0,)), ((), ()))
TN = (((0,), (0,)), ((), ()))


def dot(a, b, dims):
    return lax.dot_general(a, b, dims, preferred_element_type=F32)


def mean0(value):
    return jnp.mean(value, axis=0, keepdims=True)


BLOCK_OF = (6, 2, 1, 5, 0, 4, 3, 7)
PLACE_OF = (
    (2, 3, 0, 1), (0, 1, 3, 2), (1, 3, 2, 0), (2, 1, 0, 3),
    (3, 2, 0, 1), (0, 1, 3, 2), (1, 2, 3, 0), (3, 0, 1, 2),
)


def table(index, values):
    found = 0
    for k, value in enumerate(values):
        found = found + jnp.where(index == k, value, 0)
    return found


def loop(lo, hi, body):
    def step(i, carry):
        body(i)
        return carry

    lax.fori_loop(lo, hi, step, 0)


def kernel(
    pair_ref, cmask_ref, w_any, s_any,
    out_ref, curv_ref,
    pv, cm, w_ref, s_ref,
    wt, vt, wq, pg, mk, zn, fac, tmp,
    sf, rf, xs, xr, zs, zr, outs, xb4, xbr, xbs, rx, as_, ar,
    hsum, hs, hr, gi, us, ur, vb, wb, ft,
    in_s, mv_s, mv_r, ag_s, ag_r, xs_s, xs_r, q_s, q_r, v_s, v_r, o_s, o_r, lx_s, lq_s,
):
    crop = lax.axis_index("crop")
    axial = lax.axis_index("axial")
    xy = lax.div(axial, 4)
    hi = lax.rem(axial, 4)
    half = lax.div(crop, 4)
    q = lax.rem(crop, 4)
    v = 2 * hi + half

    def dev(c, a):
        return {"crop": c, "axial": a}

    def xy_dev(p):
        return dev(crop, 4 * p + hi)

    def q_dev(p):
        return dev(4 * half + p, axial)

    def v_dev(p):
        return dev(4 * lax.rem(p, 2) + q, 4 * xy + lax.div(p, 2))

    dst = table(
        4 * crop + hi, [4 * BLOCK_OF[c] + PLACE_OF[c][k] for c in range(8) for k in range(4)]
    )
    home = {4 * BLOCK_OF[c] + PLACE_OF[c][k]: 4 * c + k for c in range(8) for k in range(4)}
    homes = [home[k] for k in range(32)]
    src = table(4 * v + q, homes)
    slots = [table(v, [homes[4 * b + p] % 4 for b in range(8)]) for p in range(4)]

    def slot(p):
        return table(p, slots)

    dst_v, dst_q = lax.div(dst, 4), lax.rem(dst, 4)
    dst_c = 4 * lax.rem(dst_v, 2) + dst_q
    dst_a = 4 * xy + lax.div(dst_v, 2)
    src_c = lax.div(src, 4)
    src_a = 4 * xy + lax.rem(src, 4)
    moved = dst != 4 * v + q
    stays = jnp.logical_not(moved)

    def rcopy(src, dst, ssem, rsem, to):
        return pltpu.make_async_remote_copy(
            src_ref=src, dst_ref=dst, send_sem=ssem, recv_sem=rsem,
            device_id=to, device_id_type=MESH,
        )

    barrier = pltpu.get_barrier_semaphore()

    def greet(to):
        pl.semaphore_signal(barrier, inc=1, device_id=to, device_id_type=MESH)

    loop(1, 16, lambda d: greet(xy_dev(lax.rem(xy + d, 16))))
    loop(1, 8, lambda d: greet(v_dev(lax.rem(v + d, 8))))
    loop(1, 4, lambda d: greet(q_dev(lax.rem(q + d, 4))))

    @pl.when(moved)
    def _():
        greet(dev(dst_c, dst_a))
        greet(dev(src_c, src_a))

    loads = [
        pltpu.make_async_copy(a, b, in_s.at[k])
        for k, (a, b) in enumerate(
            ((w_any, w_ref), (s_any, s_ref), (cmask_ref, cm), (pair_ref, pv))
        )
    ]
    for load in loads:
        load.start()
    loads[0].wait()
    loads[1].wait()
    for t in range(6):
        cols = slice(128 * t, 128 * t + 128)
        wt[cols, :] = w_ref[:, cols].astype(F32).T.astype(BF16)
        probe = (2 * s_ref[:, cols] - 1).astype(F32) * (1.0 / jnp.sqrt(F32(128)))
        vt[cols, :] = probe.T.astype(BF16)
    for t in range(4):
        rows = pl.ds(pl.multiple_of(128 * t + 32 * q, 32), 32)
        wq[32 * t : 32 * t + 32, :] = wt[rows, :]
        wq[128 + 32 * t : 160 + 32 * t, :] = vt[rows, :]
    loads[2].wait()
    loads[3].wait()

    @pl.when(moved)
    def _():
        pl.semaphore_wait(barrier, 27)

    @pl.when(stays)
    def _():
        pl.semaphore_wait(barrier, 25)

    def put(k, lo, val):
        tmp[pl.ds(2048 * k + lo, 32, stride=16), :] = val

    def get(k, lo):
        return tmp[pl.ds(2048 * k + lo, 32, stride=16), :]

    def flat(k, i):
        return pl.ds(pl.multiple_of(2048 * k + 128 * i, 128), 128)

    def spread(k, src):
        def body(i):
            val = src[k, lax.div(i, 4), pl.ds(8 * lax.rem(i, 4), 8)].astype(F32)
            tmp[flat(k, i), :] = val.reshape(128, 128)

        loop(0, 8, body)

    own = slot(q)

    def lanes_of(k):
        return slice(128 * k, 128 * k + 128)

    def mv_pair(k):
        return rcopy(
            pv.at[:, lanes_of(k)], pg.at[pl.ds(4 * hi, 4), lanes_of(k)],
            mv_s.at[k], mv_r.at[k], dev(dst_c, dst_a),
        )

    def mv_mask():
        return rcopy(cm, mk, mv_s.at[2], mv_r.at[2], dev(dst_c, dst_a))

    def own_pair(k):
        return pltpu.make_async_copy(
            pv.at[:, lanes_of(k)], pg.at[pl.ds(4 * own, 4), lanes_of(k)], mv_r.at[k]
        )

    def own_mask():
        return pltpu.make_async_copy(cm, mk, mv_r.at[2])

    @pl.when(moved)
    def _():
        mv_mask().start()
        mv_pair(0).start()
        mv_pair(1).start()

    @pl.when(stays)
    def _():
        own_mask().start()
        own_pair(0).start()
        own_pair(1).start()

    q1 = q + 1 - 2 * lax.rem(q, 2)
    q2 = lax.rem(q + 2, 4)
    q3 = lax.rem(q1 + 2, 4)

    def block(k, p):
        return pg.at[pl.ds(4 * slot(p), 4), lanes_of(k)]

    def near(k):
        return rcopy(block(k, q), block(k, q), ag_s.at[k, 0], ag_r.at[k, 0], q_dev(q1))

    def far(k):
        return rcopy(block(k, q), block(k, q), ag_s.at[k, 1], ag_r.at[k, 1], q_dev(q2))

    def pass_on(k):
        return rcopy(block(k, q2), block(k, q2), ag_s.at[k, 2], ag_r.at[k, 2], q_dev(q1))

    def arrived(k):
        @pl.when(moved)
        def _():
            if k == 0:
                mv_mask().wait()
            mv_pair(k).wait()

        @pl.when(stays)
        def _():
            if k == 0:
                own_mask().wait()
            own_pair(k).wait()

    iota = lax.broadcasted_iota(jnp.int32, (1, 256), 1)

    def project(k, r):
        rows = pg[r, lanes_of(k), :].astype(F32)
        centered = rows - jnp.mean(rows, axis=1, keepdims=True)
        var = jnp.mean(centered * centered, axis=1, keepdims=True)
        znr = (centered * lax.rsqrt(var + EPS)).astype(BF16)
        zn[r, lanes_of(k), :] = znr
        proj = dot(wq[...], znr, NT)
        m = mk[...].astype(F32)
        mi = jnp.sum(jnp.where(iota == 16 * xy + r, m, 0.0), axis=1, keepdims=True)
        mrow = m[:, lanes_of(k)] * mi
        for side in range(2):
            lo = 64 * side
            p, g = proj[lo : lo + 32], proj[lo + 32 : lo + 64]
            tp, tg = proj[128 + lo : 160 + lo], proj[160 + lo : 192 + lo]
            s = jax.nn.sigmoid(g)
            fp = s * mrow
            fg = p * (fp * (1.0 - s))
            fac[k, r, lo : lo + 32, :] = fp
            fac[k, r, lo + 32 : lo + 64, :] = fg
            put(k, 512 * side + r, fp * p)
            put(k, 1024 + 512 * side + r, fg * tg + fp * tp)

    def project4(k, p):
        for i in range(4):
            project(k, 4 * p + i)

    def xy_start(n, src, dst):
        pltpu.make_async_copy(src(xy), dst(xy), lx_s.at[n]).start()

        def send(d):
            p = lax.rem(xy + d, 16)
            rcopy(src(p), dst(xy), xs_s.at[n, p], xs_r.at[n, xy], xy_dev(p)).start()

        loop(1, 16, send)

    def xy_wait(n, src, dst):
        pltpu.make_async_copy(src(xy), dst(xy), lx_s.at[n]).wait()

        def done(d):
            p = lax.rem(xy + d, 16)
            both = rcopy(src(p), dst(p), xs_s.at[n, p], xs_r.at[n, p], xy_dev(p))
            both.wait_send()
            both.wait_recv()

        loop(1, 16, done)

    def q_start(n, src, dst):
        pltpu.make_async_copy(src(q), dst(q), lq_s.at[n]).start()

        def send(d):
            p = lax.rem(q + d, 4)
            rcopy(src(p), dst(q), q_s.at[n, p], q_r.at[n, q], q_dev(p)).start()

        loop(1, 4, send)

    def q_wait(n, src, dst):
        pltpu.make_async_copy(src(q), dst(q), lq_s.at[n]).wait()

        def done(d):
            p = lax.rem(q + d, 4)
            both = rcopy(src(p), dst(p), q_s.at[n, p], q_r.at[n, p], q_dev(p))
            both.wait_send()
            both.wait_recv()

        loop(1, 4, done)

    def rows_of(p, n):
        return pl.ds(pl.multiple_of(n * p, n), n)

    def ab(k):
        return (
            k,
            lambda p: sf.at[k, :, pl.ds(2 * p, 2)],
            lambda p: rf.at[k, :, :, rows_of(p, 16), :],
        )

    for k in range(2):
        arrived(k)
        far(k).start()
        near(k).start()
        project4(k, slot(q))
        near(k).wait_recv()
        project4(k, slot(q1))
        far(k).wait_recv()
        pass_on(k).start()
        project4(k, slot(q2))
        pass_on(k).wait_recv()
        project4(k, slot(q3))

        def pack(i):
            val = tmp[flat(k, i), :].reshape(8, 16, 128)
            sf[k, lax.div(i, 4), pl.ds(8 * lax.rem(i, 4), 8)] = val.astype(BF16)

        loop(0, 16, pack)
        xy_start(*ab(k))
    for k in range(2):
        near(k).wait_send()
        far(k).wait_send()
        pass_on(k).wait_send()
    for k in range(2):
        xy_wait(*ab(k))

    def xx(k):
        return (
            2 + k,
            lambda p: xs.at[k, :, :, rows_of(p, 16), :],
            lambda p: xr.at[k, :, pl.ds(2 * p, 2)],
        )

    def both(ref, *at):
        return jnp.concatenate([ref[(0, *at)], ref[(1, *at)]], axis=1)

    for k in range(2):
        for c in range(2):
            a, b, ta, tb = [both(rf, n, c) for n in range(4)]
            b, tb = b[lanes_of(k)], tb[lanes_of(k)]
            x = dot(a, b, NT)
            tx = dot(jnp.concatenate([ta, a], axis=1), jnp.concatenate([b, tb], axis=1), NT)
            xs[k, 0, c] = x.astype(BF16)
            xs[k, 1, c] = tx.astype(BF16)
        xy_start(*xx(k))

    def zz(k):
        return (
            k,
            lambda p: zs.at[k, :, pl.ds(4 * slot(p), 4)],
            lambda p: zr.at[k, :, :, rows_of(p, 32), :],
        )

    for k in range(2):
        xy_wait(*xx(k))
        spread(k, xr)

        def turn(r):
            zs[k, 0, r] = get(k, r).astype(BF16)
            zs[k, 1, r] = get(k, 512 + r).astype(BF16)

        loop(0, 16, turn)
        q_start(*zz(k))

    hs[...] = jnp.zeros_like(hs)

    def head(k, r):
        znr = zn[4 * own + r, lanes_of(k), :]
        x = zr[k, 0, r].astype(F32)
        tx = zr[k, 1, r].astype(F32)
        c = x - mean0(x)
        rs = lax.rsqrt(mean0(c * c) + EPS)
        xnb = (c * rs).astype(BF16)
        tc = tx - mean0(tx)
        slope = -0.5 * (rs * rs * rs)
        drs = slope * mean0(2.0 * c * tc)
        dxnb = (tc * rs + c * drs).astype(BF16)
        g = dot(wt[512:640, :], znr, NT)
        dg = dot(vt[512:640, :], znr, NT)
        w_out = wt[640:768, :]
        out = dot(w_out, xnb, NN)
        dout = dot(w_out, dxnb, NN) + dot(vt[640:768, :], xnb, NN)
        s = jax.nn.sigmoid(g)
        sp = s * (1.0 - s)
        y = s * out
        ybar = (sp * dg * out + s * dout) * (1.0 / TOTAL)
        gbar = (ybar * out * sp).astype(BF16)
        obar = (ybar * s).astype(BF16)
        xnbar = dot(w_ref[:, 640:768], obar, NN).astype(BF16).astype(F32)
        rsbar = jnp.sum(xnbar * c, axis=0, keepdims=True)
        cbar = xnbar * rs + c * (rsbar * slope * (2.0 / 128))
        xb4[k, r] = (cbar - mean0(cbar)).astype(BF16)
        row = pg[4 * own + r, lanes_of(k), :].astype(F32)
        outs[r, lanes_of(k), :] = (row + y.T).astype(BF16)
        return dot(gbar, znr, NN), dot(obar, xnb, NT)

    def heads(k, i):
        first, second = head(k, 2 * i), head(k, 2 * i + 1)
        hs[0:128, :] += first[0] + second[0]
        hs[128:256, :] += first[1] + second[1]

    def xb(k):
        return (
            2 + k,
            lambda p: xb4.at[k, :, rows_of(p, 32), :],
            lambda p: xbr.at[k, pl.ds(4 * slot(p), 4)],
        )

    five = (4, lambda p: hs.at[rows_of(p, 64), :], lambda p: hr.at[p])
    for k in range(2):
        q_wait(*zz(k))
        loop(0, 2, lambda i: heads(k, i))
        q_start(*xb(k))

    def back():
        return rcopy(outs, out_ref, o_s, o_r, dev(src_c, src_a))

    def keep():
        return pltpu.make_async_copy(outs, out_ref, o_s)

    def rr(k):
        return (
            4 + k,
            lambda p: xbs.at[k, pl.ds(2 * p, 2)],
            lambda p: rx.at[k, :, rows_of(p, 16), :],
        )

    for k in range(2):
        q_wait(*xb(k))
        loop(0, 16, lambda r: put(k, r, xbr[k, r].astype(F32)))

        def pack_back(i):
            val = tmp[flat(k, i), :].reshape(8, 16, 128)
            xbs[k, pl.ds(8 * i, 8)] = val.astype(BF16)

        loop(0, 4, pack_back)
        xy_start(*rr(k))

    q_start(*five)

    for k in range(2):
        xy_wait(*rr(k))

    def aa(k):
        return (
            6 + k,
            lambda p: as_.at[k, :, :, rows_of(p, 16), :],
            lambda p: ar.at[k, :, pl.ds(2 * p, 2)],
        )

    for c in range(2):
        xbar = both(rx, c)
        abar = dot(xbar, both(rf, 1, c), NN).astype(BF16)
        bbar = dot(xbar, both(rf, 0, c), TN).astype(BF16)
        for k in range(2):
            as_[k, 0, c] = abar[:, lanes_of(k)]
            as_[k, 1, c] = bbar[:, lanes_of(k)]
    for k in range(2):
        xy_start(*aa(k))

    @pl.when(moved)
    def _():
        back().start()

    @pl.when(stays)
    def _():
        keep().start()

    gi[...] = jnp.zeros_like(gi)
    q_wait(*five)
    hsum[...] = hr[0] + hr[1] + hr[2] + hr[3]
    for k in range(2):
        xy_wait(*aa(k))
        spread(k, ar)

        def grad(r):
            ra = get(k, r)
            rb = get(k, 512 + r)
            d = (fac[k, r] * jnp.concatenate([ra, ra, rb, rb], axis=0)).astype(BF16)
            return dot(d, zn[r, lanes_of(k), :], NN)

        def grads(i):
            gi[...] += (grad(4 * i) + grad(4 * i + 1)) + (grad(4 * i + 2) + grad(4 * i + 3))

        loop(0, 4, grads)

    for p in range(16):
        us[p, 0] = gi[8 * p : 8 * p + 4, :]
        us[p, 1] = gi[8 * p + 4 : 8 * p + 8, :]
        us[p, 2] = hsum[4 * p : 4 * p + 4, :]
    eight = (8, lambda p: us.at[p], lambda p: ur.at[p])
    xy_start(*eight)
    xy_wait(*eight)
    total = ur[0]
    for p in range(1, 16):
        total = total + ur[p]
    vb[v] = total

    def v_copy(d, slot):
        p = lax.rem(v + d, 8)
        mine = v if slot else p
        return rcopy(vb.at[v], vb.at[mine], v_s.at[p], v_r.at[mine], v_dev(p))

    loop(1, 8, lambda d: v_copy(d, True).start())

    def v_done(d):
        both = v_copy(d, False)
        both.wait_send()
        both.wait_recv()

    loop(1, 8, v_done)
    total = vb[0]
    for p in range(1, 8):
        total = total + vb[p]
    core, row = lax.rem(q, 2), lax.div(q, 2)
    wb[core, row, xy] = total

    def swap():
        here = wb.at[core, row, xy]
        return rcopy(here, here, ag_s.at[2, 0], ag_r.at[2, 0], q_dev(q2))

    swap().start()
    swap().wait()

    def gather(d, mine):
        p = lax.rem(xy + d, 16)
        slot = xy if mine else p
        return rcopy(
            wb.at[core, :, xy], wb.at[core, :, slot], xs_s.at[9, p], xs_r.at[9, slot], xy_dev(p)
        )

    loop(1, 16, lambda d: gather(d, True).start())

    def gathered(d):
        both = gather(d, False)
        both.wait_send()
        both.wait_recv()

    loop(1, 16, gathered)

    share = rcopy(wb.at[core], wb.at[core], ag_s.at[2, 1], ag_r.at[2, 1], q_dev(q1))
    share.start()
    share.wait()

    for p in range(4):
        for k in range(16):
            lo = 128 * (k // 4) + 32 * p + 8 * (k % 4)
            ft[lo : lo + 4, :] = wb[p % 2, p // 2, k, 0]
            ft[lo + 4 : lo + 8, :] = wb[p % 2, p // 2, k, 1]
            lo = 512 + 64 * p + 4 * k
            ft[lo : lo + 4, :] = wb[p % 2, p // 2, k, 2]
    for t in range(6):
        cols = slice(128 * t, 128 * t + 128)
        curv_ref[:, cols] = ft[cols, :].T

    @pl.when(moved)
    def _():
        back().wait()

    @pl.when(stays)
    def _():
        keep().wait()


def shards(pair, crop_mask, weights, probe_signs):
    vmem = pl.BlockSpec(memory_space=pltpu.VMEM)
    dma = pltpu.SemaphoreType.DMA
    out, curv = pl.pallas_call(
        kernel,
        out_shape=(
            jax.ShapeDtypeStruct((4, 256, 128), BF16),
            jax.ShapeDtypeStruct((128, 768), F32),
        ),
        in_specs=[pl.BlockSpec(memory_space=pltpu.HBM)] * 4,
        out_specs=(pl.BlockSpec(memory_space=pl.ANY), vmem),
        scratch_shapes=[
            pltpu.VMEM((4, 256, 128), BF16),
            pltpu.VMEM((1, 256), jnp.int32),
            pltpu.VMEM((128, 768), BF16),
            pltpu.VMEM((128, 768), jnp.int32),
            pltpu.VMEM((768, 128), BF16),
            pltpu.VMEM((768, 128), BF16),
            pltpu.VMEM((256, 128), BF16),
            pltpu.VMEM((16, 256, 128), BF16),
            pltpu.VMEM((1, 256), jnp.int32),
            pltpu.VMEM((16, 256, 128), BF16),
            pltpu.VMEM((2, 16, 128, 128), F32),
            pltpu.VMEM((4096, 128), F32),
            pltpu.VMEM((2, 4, 32, 16, 128), BF16),
            pltpu.VMEM((2, 4, 2, 256, 128), BF16),
            pltpu.VMEM((2, 2, 2, 256, 128), BF16),
            pltpu.VMEM((2, 2, 32, 16, 128), BF16),
            pltpu.VMEM((2, 2, 16, 32, 128), BF16),
            pltpu.VMEM((2, 2, 4, 128, 128), BF16),
            pltpu.VMEM((4, 256, 128), BF16),
            pltpu.VMEM((2, 4, 128, 128), BF16),
            pltpu.VMEM((2, 16, 32, 128), BF16),
            pltpu.VMEM((2, 32, 16, 128), BF16),
            pltpu.VMEM((2, 2, 256, 128), BF16),
            pltpu.VMEM((2, 2, 2, 256, 128), BF16),
            pltpu.VMEM((2, 2, 32, 16, 128), BF16),
            pltpu.VMEM((64, 128), F32),
            pltpu.VMEM((256, 128), F32),
            pltpu.VMEM((4, 64, 128), F32),
            pltpu.VMEM((128, 128), F32),
            pltpu.VMEM((16, 3, 4, 128), F32),
            pltpu.VMEM((16, 3, 4, 128), F32),
            pltpu.VMEM((8, 3, 4, 128), F32),
            pltpu.VMEM((2, 2, 16, 3, 4, 128), F32),
            pltpu.VMEM((768, 128), F32),
            dma((4,)), dma((3,)), dma((3,)), dma((3, 3)), dma((3, 3)),
            dma((10, 16)), dma((10, 16)), dma((5, 4)), dma((5, 4)),
            dma((8,)), dma((8,)), dma, dma, dma((9,)), dma((5,)),
        ],
        compiler_params=pltpu.CompilerParams(
            collective_id=0, has_side_effects=True, vmem_limit_bytes=48 * 2**20
        ),
    )(pair[0], crop_mask, weights, probe_signs)
    return out[None], curv


def solution(mesh):
    placed = (P("crop", "axial", None, None), P("crop", None), P(), P())
    return jax.shard_map(
        shards,
        mesh=mesh,
        in_specs=placed,
        out_specs=(P("crop", "axial", None, None), P()),
        check_vma=False,
    )
```

```python
import jax
import jax.numpy as jnp
from jax import lax
from jax.experimental import pallas as pl
from jax.experimental.pallas import tpu as pltpu
from jax.sharding import PartitionSpec as P

MESH = pl.DeviceIdType.MESH
F32 = jnp.float32
BF16 = jnp.bfloat16
EPS = 1e-05
TOTAL = 8 * 256 * 256
NT = (((1,), (1,)), ((), ()))
NN = (((1,), (0,)), ((), ()))
TN = (((0,), (0,)), ((), ()))


def dot(a, b, dims):
    return lax.dot_general(a, b, dims, preferred_element_type=F32)


def mean0(value):
    return jnp.mean(value, axis=0, keepdims=True)


BLOCK_OF = (7, 3, 5, 1, 4, 0, 6, 2)
PLACE_OF = (
    (3, 2, 0, 1), (1, 0, 3, 2), (2, 1, 0, 3), (0, 2, 3, 1),
    (1, 0, 2, 3), (3, 2, 0, 1), (3, 1, 0, 2), (0, 3, 2, 1),
)


def table(index, values):
    found = 0
    for k, value in enumerate(values):
        found = found + jnp.where(index == k, value, 0)
    return found


def loop(lo, hi, body):
    def step(i, carry):
        body(i)
        return carry

    lax.fori_loop(lo, hi, step, 0)


def kernel(
    pair_ref, cmask_ref, w_any, s_any,
    out_ref, curv_ref,
    pv, cm, w_ref, s_ref,
    wt, vt, wq, pg, mk, zn, fac, tmp,
    sf, rf, xs, xr, zs, zr, outs, xb4, xbr, xbs, rx, as_, ar,
    hsum, hs, hr, gi, us, ur, vb, wb, ft,
    in_s, mv_s, mv_r, ag_s, ag_r, xs_s, xs_r, q_s, q_r, v_s, v_r, o_s, o_r, lx_s, lq_s,
):
    crop = lax.axis_index("crop")
    axial = lax.axis_index("axial")
    xy = lax.div(axial, 4)
    hi = lax.rem(axial, 4)
    half = lax.div(crop, 4)
    q = lax.rem(crop, 4)
    v = 2 * hi + half

    def dev(c, a):
        return {"crop": c, "axial": a}

    def xy_dev(p):
        return dev(crop, 4 * p + hi)

    def q_dev(p):
        return dev(4 * half + p, axial)

    def v_dev(p):
        return dev(4 * lax.rem(p, 2) + q, 4 * xy + lax.div(p, 2))

    dst = table(
        4 * crop + hi, [4 * BLOCK_OF[c] + PLACE_OF[c][k] for c in range(8) for k in range(4)]
    )
    home = {4 * BLOCK_OF[c] + PLACE_OF[c][k]: 4 * c + k for c in range(8) for k in range(4)}
    homes = [home[k] for k in range(32)]
    src = table(4 * v + q, homes)
    slots = [table(v, [homes[4 * b + p] % 4 for b in range(8)]) for p in range(4)]

    def slot(p):
        return table(p, slots)

    dst_v, dst_q = lax.div(dst, 4), lax.rem(dst, 4)
    dst_c = 4 * lax.rem(dst_v, 2) + dst_q
    dst_a = 4 * xy + lax.div(dst_v, 2)
    src_c = lax.div(src, 4)
    src_a = 4 * xy + lax.rem(src, 4)
    moved = dst != 4 * v + q
    stays = jnp.logical_not(moved)

    def rcopy(src, dst, ssem, rsem, to):
        return pltpu.make_async_remote_copy(
            src_ref=src, dst_ref=dst, send_sem=ssem, recv_sem=rsem,
            device_id=to, device_id_type=MESH,
        )

    barrier = pltpu.get_barrier_semaphore()

    def greet(to):
        pl.semaphore_signal(barrier, inc=1, device_id=to, device_id_type=MESH)

    loop(1, 16, lambda d: greet(xy_dev(lax.rem(xy + d, 16))))
    loop(1, 8, lambda d: greet(v_dev(lax.rem(v + d, 8))))
    loop(1, 4, lambda d: greet(q_dev(lax.rem(q + d, 4))))

    @pl.when(moved)
    def _():
        greet(dev(dst_c, dst_a))
        greet(dev(src_c, src_a))

    loads = [
        pltpu.make_async_copy(a, b, in_s.at[k])
        for k, (a, b) in enumerate(
            ((w_any, w_ref), (s_any, s_ref), (cmask_ref, cm), (pair_ref, pv))
        )
    ]
    for load in loads:
        load.start()
    loads[0].wait()
    loads[1].wait()
    for t in range(6):
        cols = slice(128 * t, 128 * t + 128)
        wt[cols, :] = w_ref[:, cols].astype(F32).T.astype(BF16)
        probe = (2 * s_ref[:, cols] - 1).astype(F32) * (1.0 / jnp.sqrt(F32(128)))
        vt[cols, :] = probe.T.astype(BF16)
    for t in range(4):
        rows = pl.ds(pl.multiple_of(128 * t + 32 * q, 32), 32)
        wq[32 * t : 32 * t + 32, :] = wt[rows, :]
        wq[128 + 32 * t : 160 + 32 * t, :] = vt[rows, :]
    loads[2].wait()
    loads[3].wait()

    @pl.when(moved)
    def _():
        pl.semaphore_wait(barrier, 27)

    @pl.when(stays)
    def _():
        pl.semaphore_wait(barrier, 25)

    def put(k, lo, val):
        tmp[pl.ds(2048 * k + lo, 32, stride=16), :] = val

    def get(k, lo):
        return tmp[pl.ds(2048 * k + lo, 32, stride=16), :]

    def flat(k, i):
        return pl.ds(pl.multiple_of(2048 * k + 128 * i, 128), 128)

    def spread(k, src):
        def body(i):
            val = src[k, lax.div(i, 4), pl.ds(8 * lax.rem(i, 4), 8)].astype(F32)
            tmp[flat(k, i), :] = val.reshape(128, 128)

        loop(0, 8, body)

    own = slot(q)

    def lanes_of(k):
        return slice(128 * k, 128 * k + 128)

    def mv_pair(k):
        return rcopy(
            pv.at[:, lanes_of(k)], pg.at[pl.ds(4 * hi, 4), lanes_of(k)],
            mv_s.at[k], mv_r.at[k], dev(dst_c, dst_a),
        )

    def mv_mask():
        return rcopy(cm, mk, mv_s.at[2], mv_r.at[2], dev(dst_c, dst_a))

    def own_pair(k):
        return pltpu.make_async_copy(
            pv.at[:, lanes_of(k)], pg.at[pl.ds(4 * own, 4), lanes_of(k)], mv_r.at[k]
        )

    def own_mask():
        return pltpu.make_async_copy(cm, mk, mv_r.at[2])

    @pl.when(moved)
    def _():
        mv_mask().start()
        mv_pair(0).start()

    @pl.when(stays)
    def _():
        own_mask().start()
        own_pair(0).start()
        own_pair(1).start()

    q1 = q + 1 - 2 * lax.rem(q, 2)
    q2 = lax.rem(q + 2, 4)
    q3 = lax.rem(q1 + 2, 4)

    def block(k, p):
        return pg.at[pl.ds(4 * slot(p), 4), lanes_of(k)]

    def near(k):
        return rcopy(block(k, q), block(k, q), ag_s.at[k, 0], ag_r.at[k, 0], q_dev(q1))

    def far(k):
        return rcopy(block(k, q), block(k, q), ag_s.at[k, 1], ag_r.at[k, 1], q_dev(q2))

    def pass_on(k):
        return rcopy(block(k, q2), block(k, q2), ag_s.at[k, 2], ag_r.at[k, 2], q_dev(q1))

    def arrived(k):
        @pl.when(moved)
        def _():
            if k == 0:
                mv_mask().wait()
            mv_pair(k).wait()

        @pl.when(stays)
        def _():
            if k == 0:
                own_mask().wait()
            own_pair(k).wait()

    iota = lax.broadcasted_iota(jnp.int32, (1, 256), 1)

    def project(k, r):
        rows = pg[r, lanes_of(k), :].astype(F32)
        centered = rows - jnp.mean(rows, axis=1, keepdims=True)
        var = jnp.mean(centered * centered, axis=1, keepdims=True)
        znr = (centered * lax.rsqrt(var + EPS)).astype(BF16)
        zn[r, lanes_of(k), :] = znr
        proj = dot(wq[...], znr, NT)
        m = mk[...].astype(F32)
        mi = jnp.sum(jnp.where(iota == 16 * xy + r, m, 0.0), axis=1, keepdims=True)
        mrow = m[:, lanes_of(k)] * mi
        for side in range(2):
            lo = 64 * side
            p, g = proj[lo : lo + 32], proj[lo + 32 : lo + 64]
            tp, tg = proj[128 + lo : 160 + lo], proj[160 + lo : 192 + lo]
            s = jax.nn.sigmoid(g)
            fp = s * mrow
            fg = p * (fp * (1.0 - s))
            fac[k, r, lo : lo + 32, :] = fp
            fac[k, r, lo + 32 : lo + 64, :] = fg
            put(k, 512 * side + r, fp * p)
            put(k, 1024 + 512 * side + r, fg * tg + fp * tp)

    def project4(k, p):
        for i in range(4):
            project(k, 4 * p + i)

    def xy_start(n, src, dst):
        pltpu.make_async_copy(src(xy), dst(xy), lx_s.at[n]).start()

        def send(d):
            p = lax.rem(xy + d, 16)
            rcopy(src(p), dst(xy), xs_s.at[n, p], xs_r.at[n, xy], xy_dev(p)).start()

        loop(1, 16, send)

    def xy_wait(n, src, dst):
        pltpu.make_async_copy(src(xy), dst(xy), lx_s.at[n]).wait()

        def done(d):
            p = lax.rem(xy + d, 16)
            both = rcopy(src(p), dst(p), xs_s.at[n, p], xs_r.at[n, p], xy_dev(p))
            both.wait_send()
            both.wait_recv()

        loop(1, 16, done)

    def q_start(n, src, dst):
        pltpu.make_async_copy(src(q), dst(q), lq_s.at[n]).start()

        def send(d):
            p = lax.rem(q + d, 4)
            rcopy(src(p), dst(q), q_s.at[n, p], q_r.at[n, q], q_dev(p)).start()

        loop(1, 4, send)

    def q_wait(n, src, dst):
        pltpu.make_async_copy(src(q), dst(q), lq_s.at[n]).wait()

        def done(d):
            p = lax.rem(q + d, 4)
            both = rcopy(src(p), dst(p), q_s.at[n, p], q_r.at[n, p], q_dev(p))
            both.wait_send()
            both.wait_recv()

        loop(1, 4, done)

    def rows_of(p, n):
        return pl.ds(pl.multiple_of(n * p, n), n)

    def ab(k):
        return (
            k,
            lambda p: sf.at[k, :, pl.ds(2 * p, 2)],
            lambda p: rf.at[k, :, :, rows_of(p, 16), :],
        )

    for k in range(2):
        arrived(k)
        far(k).start()
        near(k).start()
        if k == 0:
            @pl.when(moved)
            def _():
                mv_pair(1).start()
        project4(k, slot(q))
        near(k).wait_recv()
        project4(k, slot(q1))
        far(k).wait_recv()
        pass_on(k).start()
        project4(k, slot(q2))
        pass_on(k).wait_recv()
        project4(k, slot(q3))

        def pack(i):
            val = tmp[flat(k, i), :].reshape(8, 16, 128)
            sf[k, lax.div(i, 4), pl.ds(8 * lax.rem(i, 4), 8)] = val.astype(BF16)

        loop(0, 16, pack)
        xy_start(*ab(k))
    for k in range(2):
        near(k).wait_send()
        far(k).wait_send()
        pass_on(k).wait_send()
    for k in range(2):
        xy_wait(*ab(k))

    def xx(k):
        return (
            2 + k,
            lambda p: xs.at[k, :, :, rows_of(p, 16), :],
            lambda p: xr.at[k, :, pl.ds(2 * p, 2)],
        )

    def both(ref, *at):
        return jnp.concatenate([ref[(0, *at)], ref[(1, *at)]], axis=1)

    for k in range(2):
        for c in range(2):
            a, b, ta, tb = [both(rf, n, c) for n in range(4)]
            b, tb = b[lanes_of(k)], tb[lanes_of(k)]
            x = dot(a, b, NT)
            tx = dot(jnp.concatenate([ta, a], axis=1), jnp.concatenate([b, tb], axis=1), NT)
            xs[k, 0, c] = x.astype(BF16)
            xs[k, 1, c] = tx.astype(BF16)
        xy_start(*xx(k))

    def zz(k):
        return (
            k,
            lambda p: zs.at[k, :, pl.ds(4 * slot(p), 4)],
            lambda p: zr.at[k, :, :, rows_of(p, 32), :],
        )

    for k in range(2):
        xy_wait(*xx(k))
        spread(k, xr)

        def turn(r):
            zs[k, 0, r] = get(k, r).astype(BF16)
            zs[k, 1, r] = get(k, 512 + r).astype(BF16)

        loop(0, 16, turn)
        q_start(*zz(k))

    hs[...] = jnp.zeros_like(hs)

    def head(k, r):
        znr = zn[4 * own + r, lanes_of(k), :]
        x = zr[k, 0, r].astype(F32)
        tx = zr[k, 1, r].astype(F32)
        c = x - mean0(x)
        rs = lax.rsqrt(mean0(c * c) + EPS)
        xnb = (c * rs).astype(BF16)
        tc = tx - mean0(tx)
        slope = -0.5 * (rs * rs * rs)
        drs = slope * mean0(2.0 * c * tc)
        dxnb = (tc * rs + c * drs).astype(BF16)
        g = dot(wt[512:640, :], znr, NT)
        dg = dot(vt[512:640, :], znr, NT)
        w_out = wt[640:768, :]
        out = dot(w_out, xnb, NN)
        dout = dot(w_out, dxnb, NN) + dot(vt[640:768, :], xnb, NN)
        s = jax.nn.sigmoid(g)
        sp = s * (1.0 - s)
        y = s * out
        ybar = (sp * dg * out + s * dout) * (1.0 / TOTAL)
        gbar = (ybar * out * sp).astype(BF16)
        obar = (ybar * s).astype(BF16)
        xnbar = dot(w_ref[:, 640:768], obar, NN).astype(BF16).astype(F32)
        rsbar = jnp.sum(xnbar * c, axis=0, keepdims=True)
        cbar = xnbar * rs + c * (rsbar * slope * (2.0 / 128))
        xb4[k, r] = (cbar - mean0(cbar)).astype(BF16)
        row = pg[4 * own + r, lanes_of(k), :].astype(F32)
        outs[r, lanes_of(k), :] = (row + y.T).astype(BF16)
        return dot(gbar, znr, NN), dot(obar, xnb, NT)

    def heads(k, i):
        first, second = head(k, 2 * i), head(k, 2 * i + 1)
        hs[0:128, :] += first[0] + second[0]
        hs[128:256, :] += first[1] + second[1]

    def xb(k):
        return (
            2 + k,
            lambda p: xb4.at[k, :, rows_of(p, 32), :],
            lambda p: xbr.at[k, pl.ds(4 * slot(p), 4)],
        )

    five = (4, lambda p: hs.at[rows_of(p, 64), :], lambda p: hr.at[p])
    for k in range(2):
        q_wait(*zz(k))
        loop(0, 2, lambda i: heads(k, i))
        q_start(*xb(k))

    def back():
        return rcopy(outs, out_ref, o_s, o_r, dev(src_c, src_a))

    def keep():
        return pltpu.make_async_copy(outs, out_ref, o_s)

    def rr(k):
        return (
            4 + k,
            lambda p: xbs.at[k, pl.ds(2 * p, 2)],
            lambda p: rx.at[k, :, rows_of(p, 16), :],
        )

    for k in range(2):
        q_wait(*xb(k))
        loop(0, 16, lambda r: put(k, r, xbr[k, r].astype(F32)))

        def pack_back(i):
            val = tmp[flat(k, i), :].reshape(8, 16, 128)
            xbs[k, pl.ds(8 * i, 8)] = val.astype(BF16)

        loop(0, 4, pack_back)
        xy_start(*rr(k))

    q_start(*five)

    for k in range(2):
        xy_wait(*rr(k))

    def aa(k):
        return (
            6 + k,
            lambda p: as_.at[k, :, :, rows_of(p, 16), :],
            lambda p: ar.at[k, :, pl.ds(2 * p, 2)],
        )

    for c in range(2):
        xbar = both(rx, c)
        abar = dot(xbar, both(rf, 1, c), NN).astype(BF16)
        bbar = dot(xbar, both(rf, 0, c), TN).astype(BF16)
        for k in range(2):
            as_[k, 0, c] = abar[:, lanes_of(k)]
            as_[k, 1, c] = bbar[:, lanes_of(k)]
    for k in range(2):
        xy_start(*aa(k))

    @pl.when(moved)
    def _():
        back().start()

    @pl.when(stays)
    def _():
        keep().start()

    gi[...] = jnp.zeros_like(gi)
    q_wait(*five)
    hsum[...] = hr[0] + hr[1] + hr[2] + hr[3]
    for k in range(2):
        xy_wait(*aa(k))
        spread(k, ar)

        def grad(r):
            ra = get(k, r)
            rb = get(k, 512 + r)
            d = (fac[k, r] * jnp.concatenate([ra, ra, rb, rb], axis=0)).astype(BF16)
            return dot(d, zn[r, lanes_of(k), :], NN)

        def grads(i):
            gi[...] += (grad(4 * i) + grad(4 * i + 1)) + (grad(4 * i + 2) + grad(4 * i + 3))

        loop(0, 4, grads)

    for p in range(16):
        us[p, 0] = gi[8 * p : 8 * p + 4, :]
        us[p, 1] = gi[8 * p + 4 : 8 * p + 8, :]
        us[p, 2] = hsum[4 * p : 4 * p + 4, :]
    eight = (8, lambda p: us.at[p], lambda p: ur.at[p])
    xy_start(*eight)
    xy_wait(*eight)
    total = ur[0]
    for p in range(1, 16):
        total = total + ur[p]
    vb[v] = total

    def v_copy(d, slot):
        p = lax.rem(v + d, 8)
        mine = v if slot else p
        return rcopy(vb.at[v], vb.at[mine], v_s.at[p], v_r.at[mine], v_dev(p))

    loop(1, 8, lambda d: v_copy(d, True).start())

    def v_done(d):
        both = v_copy(d, False)
        both.wait_send()
        both.wait_recv()

    loop(1, 8, v_done)
    total = vb[0]
    for p in range(1, 8):
        total = total + vb[p]
    core, row = lax.rem(q, 2), lax.div(q, 2)
    wb[core, row, xy] = total

    def swap():
        here = wb.at[core, row, xy]
        return rcopy(here, here, ag_s.at[2, 0], ag_r.at[2, 0], q_dev(q2))

    swap().start()
    swap().wait()

    def gather(d, mine):
        p = lax.rem(xy + d, 16)
        slot = xy if mine else p
        return rcopy(
            wb.at[core, :, xy], wb.at[core, :, slot], xs_s.at[9, p], xs_r.at[9, slot], xy_dev(p)
        )

    loop(1, 16, lambda d: gather(d, True).start())

    def gathered(d):
        both = gather(d, False)
        both.wait_send()
        both.wait_recv()

    loop(1, 16, gathered)

    share = rcopy(wb.at[core], wb.at[core], ag_s.at[2, 1], ag_r.at[2, 1], q_dev(q1))
    share.start()
    share.wait()

    for p in range(4):
        for k in range(16):
            lo = 128 * (k // 4) + 32 * p + 8 * (k % 4)
            ft[lo : lo + 4, :] = wb[p % 2, p // 2, k, 0]
            ft[lo + 4 : lo + 8, :] = wb[p % 2, p // 2, k, 1]
            lo = 512 + 64 * p + 4 * k
            ft[lo : lo + 4, :] = wb[p % 2, p // 2, k, 2]
    for t in range(6):
        cols = slice(128 * t, 128 * t + 128)
        curv_ref[:, cols] = ft[cols, :].T

    @pl.when(moved)
    def _():
        back().wait()

    @pl.when(stays)
    def _():
        keep().wait()


def shards(pair, crop_mask, weights, probe_signs):
    vmem = pl.BlockSpec(memory_space=pltpu.VMEM)
    dma = pltpu.SemaphoreType.DMA
    out, curv = pl.pallas_call(
        kernel,
        out_shape=(
            jax.ShapeDtypeStruct((4, 256, 128), BF16),
            jax.ShapeDtypeStruct((128, 768), F32),
        ),
        in_specs=[pl.BlockSpec(memory_space=pltpu.HBM)] * 4,
        out_specs=(pl.BlockSpec(memory_space=pl.ANY), vmem),
        scratch_shapes=[
            pltpu.VMEM((4, 256, 128), BF16),
            pltpu.VMEM((1, 256), jnp.int32),
            pltpu.VMEM((128, 768), BF16),
            pltpu.VMEM((128, 768), jnp.int32),
            pltpu.VMEM((768, 128), BF16),
            pltpu.VMEM((768, 128), BF16),
            pltpu.VMEM((256, 128), BF16),
            pltpu.VMEM((16, 256, 128), BF16),
            pltpu.VMEM((1, 256), jnp.int32),
            pltpu.VMEM((16, 256, 128), BF16),
            pltpu.VMEM((2, 16, 128, 128), F32),
            pltpu.VMEM((4096, 128), F32),
            pltpu.VMEM((2, 4, 32, 16, 128), BF16),
            pltpu.VMEM((2, 4, 2, 256, 128), BF16),
            pltpu.VMEM((2, 2, 2, 256, 128), BF16),
            pltpu.VMEM((2, 2, 32, 16, 128), BF16),
            pltpu.VMEM((2, 2, 16, 32, 128), BF16),
            pltpu.VMEM((2, 2, 4, 128, 128), BF16),
            pltpu.VMEM((4, 256, 128), BF16),
            pltpu.VMEM((2, 4, 128, 128), BF16),
            pltpu.VMEM((2, 16, 32, 128), BF16),
            pltpu.VMEM((2, 32, 16, 128), BF16),
            pltpu.VMEM((2, 2, 256, 128), BF16),
            pltpu.VMEM((2, 2, 2, 256, 128), BF16),
            pltpu.VMEM((2, 2, 32, 16, 128), BF16),
            pltpu.VMEM((64, 128), F32),
            pltpu.VMEM((256, 128), F32),
            pltpu.VMEM((4, 64, 128), F32),
            pltpu.VMEM((128, 128), F32),
            pltpu.VMEM((16, 3, 4, 128), F32),
            pltpu.VMEM((16, 3, 4, 128), F32),
            pltpu.VMEM((8, 3, 4, 128), F32),
            pltpu.VMEM((2, 2, 16, 3, 4, 128), F32),
            pltpu.VMEM((768, 128), F32),
            dma((4,)), dma((3,)), dma((3,)), dma((3, 3)), dma((3, 3)),
            dma((10, 16)), dma((10, 16)), dma((5, 4)), dma((5, 4)),
            dma((8,)), dma((8,)), dma, dma, dma((9,)), dma((5,)),
        ],
        compiler_params=pltpu.CompilerParams(
            collective_id=0, has_side_effects=True, vmem_limit_bytes=67043328
        ),
    )(pair[0], crop_mask, weights, probe_signs)
    return out[None], curv


def solution(mesh):
    placed = (P("crop", "axial", None, None), P("crop", None), P(), P())
    return jax.shard_map(
        shards,
        mesh=mesh,
        in_specs=placed,
        out_specs=(P("crop", "axial", None, None), P()),
        check_vma=False,
    )
```

```python
import jax
import jax.numpy as jnp
from jax import lax
from jax.experimental import pallas as pl
from jax.experimental.pallas import tpu as pltpu
from jax.sharding import PartitionSpec as P

MESH = pl.DeviceIdType.MESH
F32 = jnp.float32
BF16 = jnp.bfloat16
EPS = 1e-05
TOTAL = 8 * 256 * 256
NT = (((1,), (1,)), ((), ()))
NN = (((1,), (0,)), ((), ()))
TN = (((0,), (0,)), ((), ()))


def dot(a, b, dims):
    return lax.dot_general(a, b, dims, preferred_element_type=F32)


def mean0(value):
    return jnp.mean(value, axis=0, keepdims=True)


BLOCK_OF = (7, 3, 5, 1, 4, 0, 6, 2)
PLACE_OF = (
    (3, 2, 0, 1), (1, 0, 3, 2), (2, 1, 0, 3), (0, 2, 3, 1),
    (1, 0, 2, 3), (3, 2, 0, 1), (3, 1, 0, 2), (0, 3, 2, 1),
)


def table(index, values):
    found = 0
    for k, value in enumerate(values):
        found = found + jnp.where(index == k, value, 0)
    return found


def loop(lo, hi, body):
    def step(i, carry):
        body(i)
        return carry

    lax.fori_loop(lo, hi, step, 0)


def kernel(
    pair_ref, cmask_ref, w_any, s_any,
    out_ref, curv_ref,
    pv, cm, w_ref, s_ref,
    wt, vt, wq, pg, mk, zn, fac, tmp,
    sf, rf, xs, xr, zs, zr, outs, xb4, xbr, xbs, rx, as_, ar,
    hsum, hs, hr, gi, us, ur, vb, wb, ft,
    in_s, mv_s, mv_r, ag_s, ag_r, xs_s, xs_r, q_s, q_r, v_s, v_r, o_s, o_r, lx_s, lq_s,
):
    crop = lax.axis_index("crop")
    axial = lax.axis_index("axial")
    xy = lax.div(axial, 4)
    hi = lax.rem(axial, 4)
    half = lax.div(crop, 4)
    q = lax.rem(crop, 4)
    v = 2 * hi + half

    def dev(c, a):
        return {"crop": c, "axial": a}

    def xy_dev(p):
        return dev(crop, 4 * p + hi)

    def q_dev(p):
        return dev(4 * half + p, axial)

    def v_dev(p):
        return dev(4 * lax.rem(p, 2) + q, 4 * xy + lax.div(p, 2))

    dst = table(
        4 * crop + hi, [4 * BLOCK_OF[c] + PLACE_OF[c][k] for c in range(8) for k in range(4)]
    )
    home = {4 * BLOCK_OF[c] + PLACE_OF[c][k]: 4 * c + k for c in range(8) for k in range(4)}
    homes = [home[k] for k in range(32)]
    src = table(4 * v + q, homes)
    slots = [table(v, [homes[4 * b + p] % 4 for b in range(8)]) for p in range(4)]

    def slot(p):
        return table(p, slots)

    dst_v, dst_q = lax.div(dst, 4), lax.rem(dst, 4)
    dst_c = 4 * lax.rem(dst_v, 2) + dst_q
    dst_a = 4 * xy + lax.div(dst_v, 2)
    src_c = lax.div(src, 4)
    src_a = 4 * xy + lax.rem(src, 4)
    moved = dst != 4 * v + q
    stays = jnp.logical_not(moved)

    def rcopy(src, dst, ssem, rsem, to):
        return pltpu.make_async_remote_copy(
            src_ref=src, dst_ref=dst, send_sem=ssem, recv_sem=rsem,
            device_id=to, device_id_type=MESH,
        )

    barrier = pltpu.get_barrier_semaphore()

    def greet(to):
        pl.semaphore_signal(barrier, inc=1, device_id=to, device_id_type=MESH)

    loop(1, 16, lambda d: greet(xy_dev(lax.rem(xy + d, 16))))
    loop(1, 8, lambda d: greet(v_dev(lax.rem(v + d, 8))))
    loop(1, 4, lambda d: greet(q_dev(lax.rem(q + d, 4))))

    @pl.when(moved)
    def _():
        greet(dev(dst_c, dst_a))
        greet(dev(src_c, src_a))

    loads = [
        pltpu.make_async_copy(a, b, in_s.at[k])
        for k, (a, b) in enumerate(
            ((w_any, w_ref), (s_any, s_ref), (cmask_ref, cm), (pair_ref, pv))
        )
    ]
    for load in loads:
        load.start()
    loads[0].wait()
    loads[1].wait()
    for t in range(6):
        cols = slice(128 * t, 128 * t + 128)
        wt[cols, :] = w_ref[:, cols].astype(F32).T.astype(BF16)
        probe = (2 * s_ref[:, cols] - 1).astype(F32) * (1.0 / jnp.sqrt(F32(128)))
        vt[cols, :] = probe.T.astype(BF16)
    for t in range(4):
        rows = pl.ds(pl.multiple_of(128 * t + 32 * q, 32), 32)
        wq[32 * t : 32 * t + 32, :] = wt[rows, :]
        wq[128 + 32 * t : 160 + 32 * t, :] = vt[rows, :]
    loads[2].wait()
    loads[3].wait()

    @pl.when(moved)
    def _():
        pl.semaphore_wait(barrier, 27)

    @pl.when(stays)
    def _():
        pl.semaphore_wait(barrier, 25)

    def put(k, lo, val):
        tmp[pl.ds(2048 * k + lo, 32, stride=16), :] = val

    def get(k, lo):
        return tmp[pl.ds(2048 * k + lo, 32, stride=16), :]

    def flat(k, i):
        return pl.ds(pl.multiple_of(2048 * k + 128 * i, 128), 128)

    def spread(k, src):
        def body(i):
            val = src[k, lax.div(i, 4), pl.ds(8 * lax.rem(i, 4), 8)].astype(F32)
            tmp[flat(k, i), :] = val.reshape(128, 128)

        loop(0, 8, body)

    own = slot(q)

    def lanes_of(k):
        return slice(128 * k, 128 * k + 128)

    def piece(p, i):
        return pl.ds(4 * p + 2 * (i % 2), 2), lanes_of(i // 2)

    def mv_pair(i):
        return rcopy(
            pv.at[piece(0, i)], pg.at[piece(hi, i)], mv_s.at[i], mv_r.at[i], dev(dst_c, dst_a)
        )

    def mv_mask():
        return rcopy(cm, mk, mv_s.at[4], mv_r.at[4], dev(dst_c, dst_a))

    def own_pair(i):
        return pltpu.make_async_copy(pv.at[piece(0, i)], pg.at[piece(own, i)], mv_r.at[i])

    def own_mask():
        return pltpu.make_async_copy(cm, mk, mv_r.at[4])

    def launch(i):
        @pl.when(moved)
        def _():
            if i == 0:
                mv_mask().start()
            mv_pair(i).start()

        @pl.when(stays)
        def _():
            if i == 0:
                own_mask().start()
            own_pair(i).start()

    launch(0)
    launch(1)

    q1 = q + 1 - 2 * lax.rem(q, 2)
    q2 = lax.rem(q + 2, 4)
    q3 = lax.rem(q1 + 2, 4)

    def carry(p, i, n, m, to):
        here = pg.at[piece(slot(p), i)]
        return rcopy(here, here, ag_s.at[n, m], ag_r.at[n, m], q_dev(to))

    def near(i):
        return carry(q, i, 0, i // 2, q1)

    def far(i):
        return carry(q, i, 1, i, q2)

    def pass_on(i):
        return carry(q2, i, 2, i // 2, q1)

    def all_rows(p, k, n, to):
        here = pg.at[pl.ds(4 * slot(p), 4), lanes_of(k)]
        return rcopy(here, here, ag_s.at[n, k], ag_r.at[n, k], q_dev(to))

    def arrived(i):
        @pl.when(moved)
        def _():
            if i == 0:
                mv_mask().wait()
            mv_pair(i).wait()

        @pl.when(stays)
        def _():
            if i == 0:
                own_mask().wait()
            own_pair(i).wait()

        far(i).start()
        near(i).start()
        if i < 2:
            launch(i + 2)

    iota = lax.broadcasted_iota(jnp.int32, (1, 256), 1)

    def project(k, r):
        rows = pg[r, lanes_of(k), :].astype(F32)
        centered = rows - jnp.mean(rows, axis=1, keepdims=True)
        var = jnp.mean(centered * centered, axis=1, keepdims=True)
        znr = (centered * lax.rsqrt(var + EPS)).astype(BF16)
        zn[r, lanes_of(k), :] = znr
        proj = dot(wq[...], znr, NT)
        m = mk[...].astype(F32)
        mi = jnp.sum(jnp.where(iota == 16 * xy + r, m, 0.0), axis=1, keepdims=True)
        mrow = m[:, lanes_of(k)] * mi
        for side in range(2):
            lo = 64 * side
            p, g = proj[lo : lo + 32], proj[lo + 32 : lo + 64]
            tp, tg = proj[128 + lo : 160 + lo], proj[160 + lo : 192 + lo]
            s = jax.nn.sigmoid(g)
            fp = s * mrow
            fg = p * (fp * (1.0 - s))
            fac[k, r, lo : lo + 32, :] = fp
            fac[k, r, lo + 32 : lo + 64, :] = fg
            put(k, 512 * side + r, fp * p)
            put(k, 1024 + 512 * side + r, fg * tg + fp * tp)

    def project4(k, p):
        for i in range(4):
            project(k, 4 * p + i)

    def xy_start(n, src, dst, most):
        pltpu.make_async_copy(src(xy), dst(xy), lx_s.at[n % 2]).start()

        def send(d):
            p = lax.rem(xy + d, 16)
            rcopy(src(p), dst(xy), xs_s.at[n], xs_r.at[n], xy_dev(p)).start()

        loop(1, 16, send)

    def xy_wait(n, src, dst, most):
        pltpu.make_async_copy(src(xy), dst(xy), lx_s.at[n % 2]).wait()
        rcopy(most, most, xs_s.at[n], xs_r.at[n], xy_dev(lax.rem(xy + 1, 16))).wait()

    def q_start(n, src, dst, most):
        pltpu.make_async_copy(src(q), dst(q), lq_s.at[n % 2]).start()

        def send(d):
            p = lax.rem(q + d, 4)
            rcopy(src(p), dst(q), q_s.at[n], q_r.at[n], q_dev(p)).start()

        loop(1, 4, send)

    def q_wait(n, src, dst, most):
        pltpu.make_async_copy(src(q), dst(q), lq_s.at[n % 2]).wait()
        rcopy(most, most, q_s.at[n], q_r.at[n], q_dev(q1)).wait()

    def rows_of(p, n):
        return pl.ds(pl.multiple_of(n * p, n), n)

    def ab(k):
        return (
            k,
            lambda p: sf.at[k, :, pl.ds(2 * p, 2)],
            lambda p: rf.at[k, :, :, rows_of(p, 16), :],
            rf.at[k, :, :, 0:240, :],
        )

    def pack(k):
        def body(i):
            val = tmp[flat(k, i), :].reshape(8, 16, 128)
            sf[k, lax.div(i, 4), pl.ds(8 * lax.rem(i, 4), 8)] = val.astype(BF16)

        loop(0, 16, body)
        xy_start(*ab(k))

    arrived(0)
    arrived(1)
    for k in range(2):
        project4(k, slot(q))
        for i in (2 * k, 2 * k + 1):
            far(i).wait_recv()
            pass_on(i).start()
        project4(k, slot(q2))
        all_rows(q, k, 0, q1).wait_recv()
        project4(k, slot(q1))
        if k == 0:
            arrived(2)
        all_rows(q2, k, 2, q1).wait_recv()
        project4(k, slot(q3))
        pack(k)
        if k == 0:
            arrived(3)
    for k in range(2):
        all_rows(q, k, 0, q1).wait_send()
        all_rows(q2, k, 2, q1).wait_send()
    for i in range(4):
        far(i).wait_send()
    for k in range(2):
        xy_wait(*ab(k))

    def xx(k):
        return (
            2 + k,
            lambda p: xs.at[k, :, :, rows_of(p, 16), :],
            lambda p: xr.at[k, :, pl.ds(2 * p, 2)],
            xr.at[k, :, 0:30],
        )

    def both(ref, *at):
        return jnp.concatenate([ref[(0, *at)], ref[(1, *at)]], axis=1)

    for k in range(2):
        for c in range(2):
            a, b, ta, tb = [both(rf, n, c) for n in range(4)]
            b, tb = b[lanes_of(k)], tb[lanes_of(k)]
            x = dot(a, b, NT)
            tx = dot(jnp.concatenate([ta, a], axis=1), jnp.concatenate([b, tb], axis=1), NT)
            xs[k, 0, c] = x.astype(BF16)
            xs[k, 1, c] = tx.astype(BF16)
        xy_start(*xx(k))

    def zz(k):
        return (
            k,
            lambda p: zs.at[k, :, pl.ds(4 * slot(p), 4)],
            lambda p: zr.at[k, :, :, rows_of(p, 32), :],
            zr.at[k, :, :, 0:96, :],
        )

    for k in range(2):
        xy_wait(*xx(k))
        spread(k, xr)

        def turn(r):
            zs[k, 0, r] = get(k, r).astype(BF16)
            zs[k, 1, r] = get(k, 512 + r).astype(BF16)

        loop(0, 16, turn)
        q_start(*zz(k))

    hs[...] = jnp.zeros_like(hs)

    def head(k, r):
        znr = zn[4 * own + r, lanes_of(k), :]
        x = zr[k, 0, r].astype(F32)
        tx = zr[k, 1, r].astype(F32)
        c = x - mean0(x)
        rs = lax.rsqrt(mean0(c * c) + EPS)
        xnb = (c * rs).astype(BF16)
        tc = tx - mean0(tx)
        slope = -0.5 * (rs * rs * rs)
        drs = slope * mean0(2.0 * c * tc)
        dxnb = (tc * rs + c * drs).astype(BF16)
        g = dot(wt[512:640, :], znr, NT)
        dg = dot(vt[512:640, :], znr, NT)
        w_out = wt[640:768, :]
        out = dot(w_out, xnb, NN)
        dout = dot(w_out, dxnb, NN) + dot(vt[640:768, :], xnb, NN)
        s = jax.nn.sigmoid(g)
        sp = s * (1.0 - s)
        y = s * out
        ybar = (sp * dg * out + s * dout) * (1.0 / TOTAL)
        gbar = (ybar * out * sp).astype(BF16)
        obar = (ybar * s).astype(BF16)
        xnbar = dot(w_ref[:, 640:768], obar, NN).astype(BF16).astype(F32)
        rsbar = jnp.sum(xnbar * c, axis=0, keepdims=True)
        cbar = xnbar * rs + c * (rsbar * slope * (2.0 / 128))
        xb4[k, r] = (cbar - mean0(cbar)).astype(BF16)
        row = pg[4 * own + r, lanes_of(k), :].astype(F32)
        outs[r, lanes_of(k), :] = (row + y.T).astype(BF16)
        return dot(gbar, znr, NN), dot(obar, xnb, NT)

    def heads(k, i):
        first, second = head(k, 2 * i), head(k, 2 * i + 1)
        hs[0:128, :] += first[0] + second[0]
        hs[128:256, :] += first[1] + second[1]

    def xb(k):
        return (
            2 + k,
            lambda p: xb4.at[k, :, rows_of(p, 32), :],
            lambda p: xbr.at[k, pl.ds(4 * slot(p), 4)],
            xbr.at[k, 0:12],
        )

    five = (4, lambda p: hs.at[rows_of(p, 64), :], lambda p: hr.at[p], hr.at[0:3])
    for k in range(2):
        q_wait(*zz(k))
        loop(0, 2, lambda i: heads(k, i))
        q_start(*xb(k))

    def back():
        return rcopy(outs, out_ref, o_s, o_r, dev(src_c, src_a))

    def keep():
        return pltpu.make_async_copy(outs, out_ref, o_s)

    def rr(k):
        return (
            4 + k,
            lambda p: xbs.at[k, pl.ds(2 * p, 2)],
            lambda p: rx.at[k, :, rows_of(p, 16), :],
            rx.at[k, :, 0:240, :],
        )

    for k in range(2):
        q_wait(*xb(k))
        loop(0, 16, lambda r: put(k, r, xbr[k, r].astype(F32)))

        def pack_back(i):
            val = tmp[flat(k, i), :].reshape(8, 16, 128)
            xbs[k, pl.ds(8 * i, 8)] = val.astype(BF16)

        loop(0, 4, pack_back)
        xy_start(*rr(k))

    q_start(*five)

    for k in range(2):
        xy_wait(*rr(k))

    def aa(k):
        return (
            6 + k,
            lambda p: as_.at[k, :, :, rows_of(p, 16), :],
            lambda p: ar.at[k, :, pl.ds(2 * p, 2)],
            ar.at[k, :, 0:30],
        )

    for c in range(2):
        xbar = both(rx, c)
        abar = dot(xbar, both(rf, 1, c), NN).astype(BF16)
        bbar = dot(xbar, both(rf, 0, c), TN).astype(BF16)
        for k in range(2):
            as_[k, 0, c] = abar[:, lanes_of(k)]
            as_[k, 1, c] = bbar[:, lanes_of(k)]
    for k in range(2):
        xy_start(*aa(k))

    @pl.when(moved)
    def _():
        back().start()

    @pl.when(stays)
    def _():
        keep().start()

    gi[...] = jnp.zeros_like(gi)
    q_wait(*five)
    hsum[...] = hr[0] + hr[1] + hr[2] + hr[3]
    for k in range(2):
        xy_wait(*aa(k))
        spread(k, ar)

        def grad(r):
            ra = get(k, r)
            rb = get(k, 512 + r)
            d = (fac[k, r] * jnp.concatenate([ra, ra, rb, rb], axis=0)).astype(BF16)
            return dot(d, zn[r, lanes_of(k), :], NN)

        def grads(i):
            gi[...] += (grad(4 * i) + grad(4 * i + 1)) + (grad(4 * i + 2) + grad(4 * i + 3))

        loop(0, 4, grads)

    for p in range(16):
        us[p, 0] = gi[8 * p : 8 * p + 4, :]
        us[p, 1] = gi[8 * p + 4 : 8 * p + 8, :]
        us[p, 2] = hsum[4 * p : 4 * p + 4, :]
    eight = (8, lambda p: us.at[p], lambda p: ur.at[p], ur.at[0:15])
    xy_start(*eight)
    xy_wait(*eight)
    total = ur[0]
    for p in range(1, 16):
        total = total + ur[p]
    vb[v] = total

    def v_send(d):
        p = lax.rem(v + d, 8)
        rcopy(vb.at[v], vb.at[v], v_s, v_r, v_dev(p)).start()

    loop(1, 8, v_send)
    rcopy(vb.at[0:7], vb.at[0:7], v_s, v_r, v_dev(lax.rem(v + 1, 8))).wait()
    total = vb[0]
    for p in range(1, 8):
        total = total + vb[p]
    core, row = lax.rem(q, 2), lax.div(q, 2)
    wb[core, row, xy] = total

    def swap():
        here = wb.at[core, row, xy]
        return rcopy(here, here, ag_s.at[0, 2], ag_r.at[0, 2], q_dev(q2))

    swap().start()
    swap().wait()

    def gather(d):
        p = lax.rem(xy + d, 16)
        here = wb.at[core, :, xy]
        rcopy(here, here, xs_s.at[9], xs_r.at[9], xy_dev(p)).start()

    loop(1, 16, gather)
    most = wb.at[core, :, 0:15]
    rcopy(most, most, xs_s.at[9], xs_r.at[9], xy_dev(lax.rem(xy + 1, 16))).wait()

    share = rcopy(wb.at[core], wb.at[core], ag_s.at[0, 3], ag_r.at[0, 3], q_dev(q1))
    share.start()
    share.wait()

    for p in range(4):
        for k in range(16):
            lo = 128 * (k // 4) + 32 * p + 8 * (k % 4)
            ft[lo : lo + 4, :] = wb[p % 2, p // 2, k, 0]
            ft[lo + 4 : lo + 8, :] = wb[p % 2, p // 2, k, 1]
            lo = 512 + 64 * p + 4 * k
            ft[lo : lo + 4, :] = wb[p % 2, p // 2, k, 2]
    for t in range(6):
        cols = slice(128 * t, 128 * t + 128)
        curv_ref[:, cols] = ft[cols, :].T

    @pl.when(moved)
    def _():
        back().wait()

    @pl.when(stays)
    def _():
        keep().wait()

def shards(pair, crop_mask, weights, probe_signs):
    dma = pltpu.SemaphoreType.DMA
    out, curv = pl.pallas_call(
        kernel,
        out_shape=(
            pltpu.VMEM((4, 256, 128), BF16),
            pltpu.VMEM((128, 768), F32),
        ),
        in_specs=[pl.BlockSpec(memory_space=pltpu.HBM)] * 4,
        out_specs=(pl.BlockSpec(memory_space=pltpu.VMEM),) * 2,
        scratch_shapes=[
            pltpu.VMEM((4, 256, 128), BF16),
            pltpu.VMEM((1, 256), jnp.int32),
            pltpu.VMEM((128, 768), BF16),
            pltpu.VMEM((128, 768), jnp.int32),
            pltpu.VMEM((768, 128), BF16),
            pltpu.VMEM((768, 128), BF16),
            pltpu.VMEM((256, 128), BF16),
            pltpu.VMEM((16, 256, 128), BF16),
            pltpu.VMEM((1, 256), jnp.int32),
            pltpu.VMEM((16, 256, 128), BF16),
            pltpu.VMEM((2, 16, 128, 128), F32),
            pltpu.VMEM((4096, 128), F32),
            pltpu.VMEM((2, 4, 32, 16, 128), BF16),
            pltpu.VMEM((2, 4, 2, 256, 128), BF16),
            pltpu.VMEM((2, 2, 2, 256, 128), BF16),
            pltpu.VMEM((2, 2, 32, 16, 128), BF16),
            pltpu.VMEM((2, 2, 16, 32, 128), BF16),
            pltpu.VMEM((2, 2, 4, 128, 128), BF16),
            pltpu.VMEM((4, 256, 128), BF16),
            pltpu.VMEM((2, 4, 128, 128), BF16),
            pltpu.VMEM((2, 16, 32, 128), BF16),
            pltpu.VMEM((2, 32, 16, 128), BF16),
            pltpu.VMEM((2, 2, 256, 128), BF16),
            pltpu.VMEM((2, 2, 2, 256, 128), BF16),
            pltpu.VMEM((2, 2, 32, 16, 128), BF16),
            pltpu.VMEM((64, 128), F32),
            pltpu.VMEM((256, 128), F32),
            pltpu.VMEM((4, 64, 128), F32),
            pltpu.VMEM((128, 128), F32),
            pltpu.VMEM((16, 3, 4, 128), F32),
            pltpu.VMEM((16, 3, 4, 128), F32),
            pltpu.VMEM((8, 3, 4, 128), F32),
            pltpu.VMEM((2, 2, 16, 3, 4, 128), F32),
            pltpu.VMEM((768, 128), F32),
            dma((4,)), dma((5,)), dma((5,)), dma((3, 4)), dma((3, 4)),
            dma((10,)), dma((10,)), dma((5,)), dma((5,)),
            dma, dma, dma, dma, dma((2,)), dma((2,)),
        ],
        compiler_params=pltpu.CompilerParams(
            collective_id=0, has_side_effects=True, vmem_limit_bytes=58 * 2**20
        ),
    )(pair[0], crop_mask, weights, probe_signs)
    return out[None], curv


def solution(mesh):
    placed = (P("crop", "axial", None, None), P("crop", None), P(), P())
    return jax.shard_map(
        shards,
        mesh=mesh,
        in_specs=placed,
        out_specs=(P("crop", "axial", None, None), P()),
        check_vma=False,
    )
```

```python
import jax
import jax.numpy as jnp
from jax import lax
from jax.experimental import pallas as pl
from jax.experimental.pallas import tpu as pltpu
from jax.sharding import PartitionSpec as P

MESH = pl.DeviceIdType.MESH
F32 = jnp.float32
BF16 = jnp.bfloat16
EPS = 1e-05
TOTAL = 8 * 256 * 256
NT = (((1,), (1,)), ((), ()))
NN = (((1,), (0,)), ((), ()))
TN = (((0,), (0,)), ((), ()))


def dot(a, b, dims):
    return lax.dot_general(a, b, dims, preferred_element_type=F32)


def mean0(value):
    return jnp.mean(value, axis=0, keepdims=True)


BLOCK_OF = (7, 3, 5, 1, 4, 0, 6, 2)
PLACE_OF = (
    (3, 2, 0, 1), (1, 0, 3, 2), (2, 1, 0, 3), (0, 2, 3, 1),
    (1, 0, 2, 3), (3, 2, 0, 1), (3, 1, 0, 2), (0, 3, 2, 1),
)


SHIFTS = (
    (2, 2), (2, 1), (1, 2), (2, 3), (3, 2), (1, 1), (3, 3), (1, 3), (3, 1),
    (2, 0), (0, 2), (1, 0), (0, 1), (3, 0), (0, 3),
)


def table(index, values):
    found = 0
    for k, value in enumerate(values):
        found = found + jnp.where(index == k, value, 0)
    return found


def loop(lo, hi, body):
    def step(i, carry):
        body(i)
        return carry

    lax.fori_loop(lo, hi, step, 0)


def kernel(
    pair_ref, cmask_ref, w_any, s_any,
    out_ref, curv_ref,
    pv, cm, w_ref, s_ref,
    wt, vt, wq, pg, mk, zn, fac, tmp,
    sf, rf, xs, xr, zs, zr, outs, xb4, xbr, xbs, rx, as_, ar,
    hsum, hs, hr, gi, us, ur, vb, wb, ft,
    in_s, mv_s, mv_r, ag_s, ag_r, xs_s, xs_r, q_s, q_r, v_s, v_r, o_s, o_r, lx_s, lq_s,
):
    crop = lax.axis_index("crop")
    axial = lax.axis_index("axial")
    xy = lax.div(axial, 4)
    hi = lax.rem(axial, 4)
    half = lax.div(crop, 4)
    q = lax.rem(crop, 4)
    v = 2 * hi + half

    def dev(c, a):
        return {"crop": c, "axial": a}

    def xy_dev(p):
        return dev(crop, 4 * p + hi)

    def q_dev(p):
        return dev(4 * half + p, axial)

    def v_dev(p):
        return dev(4 * lax.rem(p, 2) + q, 4 * xy + lax.div(p, 2))

    dst = table(
        4 * crop + hi, [4 * BLOCK_OF[c] + PLACE_OF[c][k] for c in range(8) for k in range(4)]
    )
    home = {4 * BLOCK_OF[c] + PLACE_OF[c][k]: 4 * c + k for c in range(8) for k in range(4)}
    homes = [home[k] for k in range(32)]
    src = table(4 * v + q, homes)
    slots = [table(v, [homes[4 * b + p] % 4 for b in range(8)]) for p in range(4)]

    def slot(p):
        return table(p, slots)

    dst_v, dst_q = lax.div(dst, 4), lax.rem(dst, 4)
    dst_c = 4 * lax.rem(dst_v, 2) + dst_q
    dst_a = 4 * xy + lax.div(dst_v, 2)
    src_c = lax.div(src, 4)
    src_a = 4 * xy + lax.rem(src, 4)
    moved = dst != 4 * v + q
    stays = jnp.logical_not(moved)

    def rcopy(src, dst, ssem, rsem, to):
        return pltpu.make_async_remote_copy(
            src_ref=src, dst_ref=dst, send_sem=ssem, recv_sem=rsem,
            device_id=to, device_id_type=MESH,
        )

    barrier = pltpu.get_barrier_semaphore()

    def greet(to):
        pl.semaphore_signal(barrier, inc=1, device_id=to, device_id_type=MESH)

    loop(1, 16, lambda d: greet(xy_dev(lax.rem(xy + d, 16))))
    loop(1, 8, lambda d: greet(v_dev(lax.rem(v + d, 8))))
    loop(1, 4, lambda d: greet(q_dev(lax.rem(q + d, 4))))

    @pl.when(moved)
    def _():
        greet(dev(dst_c, dst_a))
        greet(dev(src_c, src_a))

    loads = [
        pltpu.make_async_copy(a, b, in_s.at[k])
        for k, (a, b) in enumerate(
            ((w_any, w_ref), (s_any, s_ref), (cmask_ref, cm), (pair_ref, pv))
        )
    ]
    for load in loads:
        load.start()
    loads[0].wait()
    loads[1].wait()
    for t in range(6):
        cols = slice(128 * t, 128 * t + 128)
        wt[cols, :] = w_ref[:, cols].astype(F32).T.astype(BF16)
        probe = (2 * s_ref[:, cols] - 1).astype(F32) * (1.0 / jnp.sqrt(F32(128)))
        vt[cols, :] = probe.T.astype(BF16)
    for t in range(4):
        rows = pl.ds(pl.multiple_of(128 * t + 32 * q, 32), 32)
        wq[32 * t : 32 * t + 32, :] = wt[rows, :]
        wq[128 + 32 * t : 160 + 32 * t, :] = vt[rows, :]
    loads[2].wait()
    loads[3].wait()

    @pl.when(moved)
    def _():
        pl.semaphore_wait(barrier, 27)

    @pl.when(stays)
    def _():
        pl.semaphore_wait(barrier, 25)

    def put(k, lo, val):
        tmp[pl.ds(2048 * k + lo, 32, stride=16), :] = val

    def get(k, lo):
        return tmp[pl.ds(2048 * k + lo, 32, stride=16), :]

    def flat(k, i):
        return pl.ds(pl.multiple_of(2048 * k + 128 * i, 128), 128)

    def spread(k, src):
        def body(i):
            val = src[k, lax.div(i, 4), pl.ds(8 * lax.rem(i, 4), 8)].astype(F32)
            tmp[flat(k, i), :] = val.reshape(128, 128)

        loop(0, 8, body)

    own = slot(q)

    def lanes_of(k):
        return slice(128 * k, 128 * k + 128)

    def piece(p, i):
        return pl.ds(4 * p + 2 * (i % 2), 2), lanes_of(i // 2)

    def mv_pair(i):
        return rcopy(
            pv.at[piece(0, i)], pg.at[piece(hi, i)], mv_s.at[i], mv_r.at[i], dev(dst_c, dst_a)
        )

    def mv_mask():
        return rcopy(cm, mk, mv_s.at[4], mv_r.at[4], dev(dst_c, dst_a))

    def own_pair(i):
        return pltpu.make_async_copy(pv.at[piece(0, i)], pg.at[piece(own, i)], mv_r.at[i])

    def own_mask():
        return pltpu.make_async_copy(cm, mk, mv_r.at[4])

    def launch(i):
        @pl.when(moved)
        def _():
            if i == 0:
                mv_mask().start()
            mv_pair(i).start()

        @pl.when(stays)
        def _():
            if i == 0:
                own_mask().start()
            own_pair(i).start()

    launch(0)
    launch(1)

    q1 = q + 1 - 2 * lax.rem(q, 2)
    q2 = lax.rem(q + 2, 4)
    q3 = lax.rem(q1 + 2, 4)

    def carry(p, i, n, m, to):
        here = pg.at[piece(slot(p), i)]
        return rcopy(here, here, ag_s.at[n, m], ag_r.at[n, m], q_dev(to))

    def near(i):
        return carry(q, i, 0, i // 2, q1)

    def far(i):
        return carry(q, i, 1, i, q2)

    def pass_on(i):
        return carry(q2, i, 2, i // 2, q1)

    def all_rows(p, k, n, to):
        here = pg.at[pl.ds(4 * slot(p), 4), lanes_of(k)]
        return rcopy(here, here, ag_s.at[n, k], ag_r.at[n, k], q_dev(to))

    def arrived(i):
        @pl.when(moved)
        def _():
            if i == 0:
                mv_mask().wait()
            mv_pair(i).wait()

        @pl.when(stays)
        def _():
            if i == 0:
                own_mask().wait()
            own_pair(i).wait()

        far(i).start()
        near(i).start()
        if i < 2:
            launch(i + 2)

    iota = lax.broadcasted_iota(jnp.int32, (1, 256), 1)

    def project(k, r):
        rows = pg[r, lanes_of(k), :].astype(F32)
        centered = rows - jnp.mean(rows, axis=1, keepdims=True)
        var = jnp.mean(centered * centered, axis=1, keepdims=True)
        znr = (centered * lax.rsqrt(var + EPS)).astype(BF16)
        zn[r, lanes_of(k), :] = znr
        proj = dot(wq[...], znr, NT)
        m = mk[...].astype(F32)
        mi = jnp.sum(jnp.where(iota == 16 * xy + r, m, 0.0), axis=1, keepdims=True)
        mrow = m[:, lanes_of(k)] * mi
        for side in range(2):
            lo = 64 * side
            p, g = proj[lo : lo + 32], proj[lo + 32 : lo + 64]
            tp, tg = proj[128 + lo : 160 + lo], proj[160 + lo : 192 + lo]
            s = jax.nn.sigmoid(g)
            fp = s * mrow
            fg = p * (fp * (1.0 - s))
            fac[k, r, lo : lo + 32, :] = fp
            fac[k, r, lo + 32 : lo + 64, :] = fg
            put(k, 512 * side + r, fp * p)
            put(k, 1024 + 512 * side + r, fg * tg + fp * tp)

    def project4(k, p):
        for i in range(4):
            project(k, 4 * p + i)

    peers = [
        4 * lax.rem(lax.div(xy, 4) + dx, 4) + lax.rem(lax.rem(xy, 4) + dy, 4)
        for dx, dy in SHIFTS
    ]

    def xy_start(n, src, dst, most):
        pltpu.make_async_copy(src(xy), dst(xy), lx_s.at[n % 2]).start()

        for p in peers:
            rcopy(src(p), dst(xy), xs_s.at[n], xs_r.at[n], xy_dev(p)).start()

    def xy_wait(n, src, dst, most):
        pltpu.make_async_copy(src(xy), dst(xy), lx_s.at[n % 2]).wait()
        rcopy(most, most, xs_s.at[n], xs_r.at[n], xy_dev(lax.rem(xy + 1, 16))).wait()

    def q_start(n, src, dst, most):
        pltpu.make_async_copy(src(q), dst(q), lq_s.at[n % 2]).start()

        for p in (q2, q3, q1):
            rcopy(src(p), dst(q), q_s.at[n], q_r.at[n], q_dev(p)).start()

    def q_wait(n, src, dst, most):
        pltpu.make_async_copy(src(q), dst(q), lq_s.at[n % 2]).wait()
        rcopy(most, most, q_s.at[n], q_r.at[n], q_dev(q1)).wait()

    def rows_of(p, n):
        return pl.ds(pl.multiple_of(n * p, n), n)

    def ab(k):
        return (
            k,
            lambda p: sf.at[k, :, pl.ds(2 * p, 2)],
            lambda p: rf.at[k, :, :, rows_of(p, 16), :],
            rf.at[k, :, :, 0:240, :],
        )

    def pack(k):
        def body(i):
            val = tmp[flat(k, i), :].reshape(8, 16, 128)
            sf[k, lax.div(i, 4), pl.ds(8 * lax.rem(i, 4), 8)] = val.astype(BF16)

        loop(0, 16, body)
        xy_start(*ab(k))

    arrived(0)
    arrived(1)
    for k in range(2):
        project4(k, slot(q))
        for i in (2 * k, 2 * k + 1):
            far(i).wait_recv()
            pass_on(i).start()
        project4(k, slot(q2))
        all_rows(q, k, 0, q1).wait_recv()
        project4(k, slot(q1))
        if k == 0:
            arrived(2)
        all_rows(q2, k, 2, q1).wait_recv()
        project4(k, slot(q3))
        pack(k)
        if k == 0:
            arrived(3)
    for k in range(2):
        all_rows(q, k, 0, q1).wait_send()
        all_rows(q2, k, 2, q1).wait_send()
    for i in range(4):
        far(i).wait_send()
    for k in range(2):
        xy_wait(*ab(k))

    def xx(k):
        return (
            2 + k,
            lambda p: xs.at[k, :, :, rows_of(p, 16), :],
            lambda p: xr.at[k, :, pl.ds(2 * p, 2)],
            xr.at[k, :, 0:30],
        )

    def both(ref, *at):
        return jnp.concatenate([ref[(0, *at)], ref[(1, *at)]], axis=1)

    for k in range(2):
        for c in range(2):
            a, b, ta, tb = [both(rf, n, c) for n in range(4)]
            b, tb = b[lanes_of(k)], tb[lanes_of(k)]
            x = dot(a, b, NT)
            tx = dot(jnp.concatenate([ta, a], axis=1), jnp.concatenate([b, tb], axis=1), NT)
            xs[k, 0, c] = x.astype(BF16)
            xs[k, 1, c] = tx.astype(BF16)
        xy_start(*xx(k))

    def zz(k):
        return (
            k,
            lambda p: zs.at[k, :, pl.ds(4 * slot(p), 4)],
            lambda p: zr.at[k, :, :, rows_of(p, 32), :],
            zr.at[k, :, :, 0:96, :],
        )

    for k in range(2):
        xy_wait(*xx(k))
        spread(k, xr)

        def turn(r):
            zs[k, 0, r] = get(k, r).astype(BF16)
            zs[k, 1, r] = get(k, 512 + r).astype(BF16)

        loop(0, 16, turn)
        q_start(*zz(k))

    hs[...] = jnp.zeros_like(hs)

    def head(k, r):
        znr = zn[4 * own + r, lanes_of(k), :]
        x = zr[k, 0, r].astype(F32)
        tx = zr[k, 1, r].astype(F32)
        c = x - mean0(x)
        rs = lax.rsqrt(mean0(c * c) + EPS)
        xnb = (c * rs).astype(BF16)
        tc = tx - mean0(tx)
        slope = -0.5 * (rs * rs * rs)
        drs = slope * mean0(2.0 * c * tc)
        dxnb = (tc * rs + c * drs).astype(BF16)
        g = dot(wt[512:640, :], znr, NT)
        dg = dot(vt[512:640, :], znr, NT)
        w_out = wt[640:768, :]
        out = dot(w_out, xnb, NN)
        dout = dot(w_out, dxnb, NN) + dot(vt[640:768, :], xnb, NN)
        s = jax.nn.sigmoid(g)
        sp = s * (1.0 - s)
        y = s * out
        ybar = (sp * dg * out + s * dout) * (1.0 / TOTAL)
        gbar = (ybar * out * sp).astype(BF16)
        obar = (ybar * s).astype(BF16)
        xnbar = dot(w_ref[:, 640:768], obar, NN).astype(BF16).astype(F32)
        rsbar = jnp.sum(xnbar * c, axis=0, keepdims=True)
        cbar = xnbar * rs + c * (rsbar * slope * (2.0 / 128))
        xb4[k, r] = (cbar - mean0(cbar)).astype(BF16)
        row = pg[4 * own + r, lanes_of(k), :].astype(F32)
        outs[r, lanes_of(k), :] = (row + y.T).astype(BF16)
        return dot(gbar, znr, NN), dot(obar, xnb, NT)

    def heads(k, i):
        first, second = head(k, 2 * i), head(k, 2 * i + 1)
        hs[0:128, :] += first[0] + second[0]
        hs[128:256, :] += first[1] + second[1]

    def xb(k):
        return (
            2 + k,
            lambda p: xb4.at[k, :, rows_of(p, 32), :],
            lambda p: xbr.at[k, pl.ds(4 * slot(p), 4)],
            xbr.at[k, 0:12],
        )

    five = (4, lambda p: hs.at[rows_of(p, 64), :], lambda p: hr.at[p], hr.at[0:3])
    for k in range(2):
        q_wait(*zz(k))
        loop(0, 2, lambda i: heads(k, i))
        q_start(*xb(k))

    def back():
        return rcopy(outs, out_ref, o_s, o_r, dev(src_c, src_a))

    def keep():
        return pltpu.make_async_copy(outs, out_ref, o_s)

    def rr(k):
        return (
            4 + k,
            lambda p: xbs.at[k, pl.ds(2 * p, 2)],
            lambda p: rx.at[k, :, rows_of(p, 16), :],
            rx.at[k, :, 0:240, :],
        )

    for k in range(2):
        q_wait(*xb(k))
        loop(0, 16, lambda r: put(k, r, xbr[k, r].astype(F32)))

        def pack_back(i):
            val = tmp[flat(k, i), :].reshape(8, 16, 128)
            xbs[k, pl.ds(8 * i, 8)] = val.astype(BF16)

        loop(0, 4, pack_back)
        xy_start(*rr(k))

    q_start(*five)

    for k in range(2):
        xy_wait(*rr(k))

    def aa(k):
        return (
            6 + k,
            lambda p: as_.at[k, :, :, rows_of(p, 16), :],
            lambda p: ar.at[k, :, pl.ds(2 * p, 2)],
            ar.at[k, :, 0:30],
        )

    for c in range(2):
        xbar = both(rx, c)
        abar = dot(xbar, both(rf, 1, c), NN).astype(BF16)
        bbar = dot(xbar, both(rf, 0, c), TN).astype(BF16)
        for k in range(2):
            as_[k, 0, c] = abar[:, lanes_of(k)]
            as_[k, 1, c] = bbar[:, lanes_of(k)]
    for k in range(2):
        xy_start(*aa(k))

    @pl.when(moved)
    def _():
        back().start()

    @pl.when(stays)
    def _():
        keep().start()

    gi[...] = jnp.zeros_like(gi)
    q_wait(*five)
    hsum[...] = hr[0] + hr[1] + hr[2] + hr[3]
    for k in range(2):
        xy_wait(*aa(k))
        spread(k, ar)

        def grad(r):
            ra = get(k, r)
            rb = get(k, 512 + r)
            d = (fac[k, r] * jnp.concatenate([ra, ra, rb, rb], axis=0)).astype(BF16)
            return dot(d, zn[r, lanes_of(k), :], NN)

        def grads(i):
            gi[...] += (grad(4 * i) + grad(4 * i + 1)) + (grad(4 * i + 2) + grad(4 * i + 3))

        loop(0, 4, grads)

    for p in range(16):
        us[p, 0] = gi[8 * p : 8 * p + 4, :]
        us[p, 1] = gi[8 * p + 4 : 8 * p + 8, :]
        us[p, 2] = hsum[4 * p : 4 * p + 4, :]
    eight = (8, lambda p: us.at[p], lambda p: ur.at[p], ur.at[0:15])
    xy_start(*eight)
    xy_wait(*eight)
    total = ur[0]
    for p in range(1, 16):
        total = total + ur[p]
    vb[v] = total

    for d in (4, 3, 5, 2, 6, 1, 7):
        rcopy(vb.at[v], vb.at[v], v_s, v_r, v_dev(lax.rem(v + d, 8))).start()
    rcopy(vb.at[0:7], vb.at[0:7], v_s, v_r, v_dev(lax.rem(v + 1, 8))).wait()
    total = vb[0]
    for p in range(1, 8):
        total = total + vb[p]
    core, row = lax.rem(q, 2), lax.div(q, 2)
    wb[core, row, xy] = total

    def swap():
        here = wb.at[core, row, xy]
        return rcopy(here, here, ag_s.at[0, 2], ag_r.at[0, 2], q_dev(q2))

    swap().start()
    swap().wait()

    here = wb.at[core, :, xy]
    for p in peers:
        rcopy(here, here, xs_s.at[9], xs_r.at[9], xy_dev(p)).start()
    most = wb.at[core, :, 0:15]
    rcopy(most, most, xs_s.at[9], xs_r.at[9], xy_dev(lax.rem(xy + 1, 16))).wait()

    share = rcopy(wb.at[core], wb.at[core], ag_s.at[0, 3], ag_r.at[0, 3], q_dev(q1))
    share.start()
    share.wait()

    for p in range(4):
        for k in range(16):
            lo = 128 * (k // 4) + 32 * p + 8 * (k % 4)
            ft[lo : lo + 4, :] = wb[p % 2, p // 2, k, 0]
            ft[lo + 4 : lo + 8, :] = wb[p % 2, p // 2, k, 1]
            lo = 512 + 64 * p + 4 * k
            ft[lo : lo + 4, :] = wb[p % 2, p // 2, k, 2]
    for t in range(6):
        cols = slice(128 * t, 128 * t + 128)
        curv_ref[:, cols] = ft[cols, :].T

    @pl.when(moved)
    def _():
        back().wait()

    @pl.when(stays)
    def _():
        keep().wait()

def shards(pair, crop_mask, weights, probe_signs):
    dma = pltpu.SemaphoreType.DMA
    out, curv = pl.pallas_call(
        kernel,
        out_shape=(
            pltpu.VMEM((4, 256, 128), BF16),
            pltpu.VMEM((128, 768), F32),
        ),
        in_specs=[pl.BlockSpec(memory_space=pltpu.HBM)] * 4,
        out_specs=(pl.BlockSpec(memory_space=pltpu.VMEM),) * 2,
        scratch_shapes=[
            pltpu.VMEM((4, 256, 128), BF16),
            pltpu.VMEM((1, 256), jnp.int32),
            pltpu.VMEM((128, 768), BF16),
            pltpu.VMEM((128, 768), jnp.int32),
            pltpu.VMEM((768, 128), BF16),
            pltpu.VMEM((768, 128), BF16),
            pltpu.VMEM((256, 128), BF16),
            pltpu.VMEM((16, 256, 128), BF16),
            pltpu.VMEM((1, 256), jnp.int32),
            pltpu.VMEM((16, 256, 128), BF16),
            pltpu.VMEM((2, 16, 128, 128), F32),
            pltpu.VMEM((4096, 128), F32),
            pltpu.VMEM((2, 4, 32, 16, 128), BF16),
            pltpu.VMEM((2, 4, 2, 256, 128), BF16),
            pltpu.VMEM((2, 2, 2, 256, 128), BF16),
            pltpu.VMEM((2, 2, 32, 16, 128), BF16),
            pltpu.VMEM((2, 2, 16, 32, 128), BF16),
            pltpu.VMEM((2, 2, 4, 128, 128), BF16),
            pltpu.VMEM((4, 256, 128), BF16),
            pltpu.VMEM((2, 4, 128, 128), BF16),
            pltpu.VMEM((2, 16, 32, 128), BF16),
            pltpu.VMEM((2, 32, 16, 128), BF16),
            pltpu.VMEM((2, 2, 256, 128), BF16),
            pltpu.VMEM((2, 2, 2, 256, 128), BF16),
            pltpu.VMEM((2, 2, 32, 16, 128), BF16),
            pltpu.VMEM((64, 128), F32),
            pltpu.VMEM((256, 128), F32),
            pltpu.VMEM((4, 64, 128), F32),
            pltpu.VMEM((128, 128), F32),
            pltpu.VMEM((16, 3, 4, 128), F32),
            pltpu.VMEM((16, 3, 4, 128), F32),
            pltpu.VMEM((8, 3, 4, 128), F32),
            pltpu.VMEM((2, 2, 16, 3, 4, 128), F32),
            pltpu.VMEM((768, 128), F32),
            dma((4,)), dma((5,)), dma((5,)), dma((3, 4)), dma((3, 4)),
            dma((10,)), dma((10,)), dma((5,)), dma((5,)),
            dma, dma, dma, dma, dma((2,)), dma((2,)),
        ],
        compiler_params=pltpu.CompilerParams(
            collective_id=0, has_side_effects=True, vmem_limit_bytes=58 * 2**20
        ),
    )(pair[0], crop_mask, weights, probe_signs)
    return out[None], curv


def solution(mesh):
    placed = (P("crop", "axial", None, None), P("crop", None), P(), P())
    return jax.shard_map(
        shards,
        mesh=mesh,
        in_specs=placed,
        out_specs=(P("crop", "axial", None, None), P()),
        check_vma=False,
    )
```

```python
import jax
import jax.numpy as jnp
from jax import lax
from jax.experimental import pallas as pl
from jax.experimental.pallas import tpu as pltpu
from jax.sharding import PartitionSpec as P

MESH = pl.DeviceIdType.MESH
F32 = jnp.float32
BF16 = jnp.bfloat16
EPS = 1e-05
TOTAL = 8 * 256 * 256
NT = (((1,), (1,)), ((), ()))
NN = (((1,), (0,)), ((), ()))
TN = (((0,), (0,)), ((), ()))


def dot(a, b, dims):
    return lax.dot_general(a, b, dims, preferred_element_type=F32)


def mean0(value):
    return jnp.mean(value, axis=0, keepdims=True)


BLOCK_OF = (7, 3, 5, 1, 4, 0, 6, 2)
PLACE_OF = (
    (3, 2, 0, 1), (1, 0, 3, 2), (2, 1, 0, 3), (0, 2, 3, 1),
    (1, 0, 2, 3), (3, 2, 0, 1), (3, 1, 0, 2), (0, 3, 2, 1),
)


SHIFTS = (
    (2, 2), (2, 1), (1, 2), (2, 3), (3, 2), (1, 1), (3, 3), (1, 3), (3, 1),
    (2, 0), (0, 2), (1, 0), (0, 1), (3, 0), (0, 3),
)


def table(index, values):
    found = 0
    for k, value in enumerate(values):
        found = found + jnp.where(index == k, value, 0)
    return found


def loop(lo, hi, body):
    def step(i, carry):
        body(i)
        return carry

    lax.fori_loop(lo, hi, step, 0)


def kernel(
    pair_ref, cmask_ref, w_any, s_any,
    out_ref, curv_ref,
    pv, cm, w_ref, s_ref,
    wt, vt, wq, pg, mk, zn, fac, tmp,
    sf, rf, xs, xr, zs, zr, outs, xb4, xbr, xbs, rx, as_, ar,
    hsum, hs, hr, gi, us, ur, vb, wb, ft,
    in_s, mv_s, mv_r, ag_s, ag_r, xs_s, xs_r, q_s, q_r, v_s, v_r, o_s, o_r, lx_s, lq_s,
):
    crop = lax.axis_index("crop")
    axial = lax.axis_index("axial")
    xy = lax.div(axial, 4)
    hi = lax.rem(axial, 4)
    half = lax.div(crop, 4)
    q = lax.rem(crop, 4)
    v = 2 * hi + half

    def dev(c, a):
        return {"crop": c, "axial": a}

    def xy_dev(p):
        return dev(crop, 4 * p + hi)

    def q_dev(p):
        return dev(4 * half + p, axial)

    def v_dev(p):
        return dev(4 * lax.rem(p, 2) + q, 4 * xy + lax.div(p, 2))

    dst = table(
        4 * crop + hi, [4 * BLOCK_OF[c] + PLACE_OF[c][k] for c in range(8) for k in range(4)]
    )
    home = {4 * BLOCK_OF[c] + PLACE_OF[c][k]: 4 * c + k for c in range(8) for k in range(4)}
    homes = [home[k] for k in range(32)]
    src = table(4 * v + q, homes)
    slots = [table(v, [homes[4 * b + p] % 4 for b in range(8)]) for p in range(4)]

    def slot(p):
        return table(p, slots)

    dst_v, dst_q = lax.div(dst, 4), lax.rem(dst, 4)
    dst_c = 4 * lax.rem(dst_v, 2) + dst_q
    dst_a = 4 * xy + lax.div(dst_v, 2)
    src_c = lax.div(src, 4)
    src_a = 4 * xy + lax.rem(src, 4)
    moved = dst != 4 * v + q
    stays = jnp.logical_not(moved)

    def rcopy(src, dst, ssem, rsem, to):
        return pltpu.make_async_remote_copy(
            src_ref=src, dst_ref=dst, send_sem=ssem, recv_sem=rsem,
            device_id=to, device_id_type=MESH,
        )

    barrier = pltpu.get_barrier_semaphore()

    def greet(to):
        pl.semaphore_signal(barrier, inc=1, device_id=to, device_id_type=MESH)

    loop(1, 16, lambda d: greet(xy_dev(lax.rem(xy + d, 16))))
    loop(1, 8, lambda d: greet(v_dev(lax.rem(v + d, 8))))
    loop(1, 4, lambda d: greet(q_dev(lax.rem(q + d, 4))))

    @pl.when(moved)
    def _():
        greet(dev(dst_c, dst_a))
        greet(dev(src_c, src_a))

    loads = [
        pltpu.make_async_copy(a, b, in_s.at[k])
        for k, (a, b) in enumerate(
            ((w_any, w_ref), (s_any, s_ref), (cmask_ref, cm), (pair_ref, pv))
        )
    ]
    for load in loads:
        load.start()
    loads[0].wait()
    loads[1].wait()
    for t in range(6):
        cols = slice(128 * t, 128 * t + 128)
        wt[cols, :] = w_ref[:, cols].astype(F32).T.astype(BF16)
        probe = (2 * s_ref[:, cols] - 1).astype(F32) * (1.0 / jnp.sqrt(F32(128)))
        vt[cols, :] = probe.T.astype(BF16)
    for t in range(4):
        rows = pl.ds(pl.multiple_of(128 * t + 32 * q, 32), 32)
        wq[32 * t : 32 * t + 32, :] = wt[rows, :]
        wq[128 + 32 * t : 160 + 32 * t, :] = vt[rows, :]
    loads[2].wait()
    loads[3].wait()

    @pl.when(moved)
    def _():
        pl.semaphore_wait(barrier, 27)

    @pl.when(stays)
    def _():
        pl.semaphore_wait(barrier, 25)

    def put(k, lo, val):
        tmp[pl.ds(2048 * k + lo, 32, stride=16), :] = val

    def get(k, lo):
        return tmp[pl.ds(2048 * k + lo, 32, stride=16), :]

    def flat(k, i):
        return pl.ds(pl.multiple_of(2048 * k + 128 * i, 128), 128)

    def spread(k, t, src):
        for i in range(4):
            val = src[k, t, 8 * i : 8 * i + 8].astype(F32)
            tmp[flat(k, 4 * t + i), :] = val.reshape(128, 128)

    own = slot(q)

    def lanes_of(k):
        return slice(128 * k, 128 * k + 128)

    def piece(p, i):
        return pl.ds(4 * p + 2 * (i % 2), 2), lanes_of(i // 2)

    def mv_pair(i):
        return rcopy(
            pv.at[piece(0, i)], pg.at[piece(hi, i)], mv_s.at[i], mv_r.at[i], dev(dst_c, dst_a)
        )

    def mv_mask():
        return rcopy(cm, mk, mv_s.at[4], mv_r.at[4], dev(dst_c, dst_a))

    def own_pair(i):
        return pltpu.make_async_copy(pv.at[piece(0, i)], pg.at[piece(own, i)], mv_r.at[i])

    def own_mask():
        return pltpu.make_async_copy(cm, mk, mv_r.at[4])

    def launch(i):
        @pl.when(moved)
        def _():
            if i == 0:
                mv_mask().start()
            mv_pair(i).start()

        @pl.when(stays)
        def _():
            if i == 0:
                own_mask().start()
            own_pair(i).start()

    launch(0)
    launch(1)

    q1 = q + 1 - 2 * lax.rem(q, 2)
    q2 = lax.rem(q + 2, 4)
    q3 = lax.rem(q1 + 2, 4)

    def carry(p, i, n, m, to):
        here = pg.at[piece(slot(p), i)]
        return rcopy(here, here, ag_s.at[n, m], ag_r.at[n, m], q_dev(to))

    def near(i):
        return carry(q, i, 0, i // 2, q1)

    def far(i):
        return carry(q, i, 1, i, q2)

    def pass_on(i):
        return carry(q2, i, 2, i // 2, q1)

    def all_rows(p, k, n, to):
        here = pg.at[pl.ds(4 * slot(p), 4), lanes_of(k)]
        return rcopy(here, here, ag_s.at[n, k], ag_r.at[n, k], q_dev(to))

    def arrived(i):
        @pl.when(moved)
        def _():
            if i == 0:
                mv_mask().wait()
            mv_pair(i).wait()

        @pl.when(stays)
        def _():
            if i == 0:
                own_mask().wait()
            own_pair(i).wait()

        far(i).start()
        near(i).start()
        if i < 2:
            launch(i + 2)

    iota = lax.broadcasted_iota(jnp.int32, (1, 256), 1)

    def project(k, r):
        rows = pg[r, lanes_of(k), :].astype(F32)
        centered = rows - jnp.mean(rows, axis=1, keepdims=True)
        var = jnp.mean(centered * centered, axis=1, keepdims=True)
        znr = (centered * lax.rsqrt(var + EPS)).astype(BF16)
        zn[r, lanes_of(k), :] = znr
        proj = dot(wq[...], znr, NT)
        m = mk[...].astype(F32)
        mi = jnp.sum(jnp.where(iota == 16 * xy + r, m, 0.0), axis=1, keepdims=True)
        mrow = m[:, lanes_of(k)] * mi
        for side in range(2):
            lo = 64 * side
            p, g = proj[lo : lo + 32], proj[lo + 32 : lo + 64]
            tp, tg = proj[128 + lo : 160 + lo], proj[160 + lo : 192 + lo]
            s = jax.nn.sigmoid(g)
            fp = s * mrow
            fg = p * (fp * (1.0 - s))
            fac[k, r, lo : lo + 32, :] = fp
            fac[k, r, lo + 32 : lo + 64, :] = fg
            put(k, 512 * side + r, fp * p)
            put(k, 1024 + 512 * side + r, fg * tg + fp * tp)

    def project4(k, p):
        for i in range(4):
            project(k, 4 * p + i)

    peers = [
        4 * lax.rem(lax.div(xy, 4) + dx, 4) + lax.rem(lax.rem(xy, 4) + dy, 4)
        for dx, dy in SHIFTS
    ]

    def xy_start(n, src, dst, most):
        pltpu.make_async_copy(src(xy), dst(xy), lx_s.at[n % 4]).start()

        for p in peers:
            rcopy(src(p), dst(xy), xs_s.at[n], xs_r.at[n], xy_dev(p)).start()

    def xy_wait(n, src, dst, most):
        pltpu.make_async_copy(src(xy), dst(xy), lx_s.at[n % 4]).wait()
        rcopy(most, most, xs_s.at[n], xs_r.at[n], xy_dev(lax.rem(xy + 1, 16))).wait()

    def q_start(n, src, dst, most):
        pltpu.make_async_copy(src(q), dst(q), lq_s.at[n]).start()

        for p in (q2, q3, q1):
            rcopy(src(p), dst(q), q_s.at[n], q_r.at[n], q_dev(p)).start()

    def q_wait(n, src, dst, most):
        pltpu.make_async_copy(src(q), dst(q), lq_s.at[n]).wait()
        rcopy(most, most, q_s.at[n], q_r.at[n], q_dev(q1)).wait()

    def rows_of(p, n):
        return pl.ds(pl.multiple_of(n * p, n), n)

    def ab(t, k):
        two = pl.ds(2 * t, 2)
        return (
            12 + 2 * t + k,
            lambda p: sf.at[k, two, pl.ds(2 * p, 2)],
            lambda p: rf.at[k, two, :, rows_of(p, 16), :],
            rf.at[k, two, :, 0:240, :],
        )

    def pack(k):
        def body(i):
            val = tmp[flat(k, i), :].reshape(8, 16, 128)
            sf[k, lax.div(i, 4), pl.ds(8 * lax.rem(i, 4), 8)] = val.astype(BF16)

        loop(0, 16, body)
        xy_start(*ab(0, k))
        xy_start(*ab(1, k))

    arrived(0)
    arrived(1)
    for k in range(2):
        project4(k, slot(q))
        for i in (2 * k, 2 * k + 1):
            far(i).wait_recv()
            pass_on(i).start()
        project4(k, slot(q2))
        all_rows(q, k, 0, q1).wait_recv()
        project4(k, slot(q1))
        if k == 0:
            arrived(2)
        all_rows(q2, k, 2, q1).wait_recv()
        project4(k, slot(q3))
        pack(k)
        if k == 0:
            arrived(3)
    for k in range(2):
        all_rows(q, k, 0, q1).wait_send()
        all_rows(q2, k, 2, q1).wait_send()
    for i in range(4):
        far(i).wait_send()
    def xx(t, k):
        return (
            2 * t + k,
            lambda p: xs.at[k, t, :, rows_of(p, 16), :],
            lambda p: xr.at[k, t, pl.ds(2 * p, 2)],
            xr.at[k, t, 0:30],
        )

    def both(ref, *at):
        return jnp.concatenate([ref[(0, *at)], ref[(1, *at)]], axis=1)

    for t in range(2):
        for k in range(2):
            xy_wait(*ab(t, k))
        for k in range(2):
            for c in range(2):
                a, b = both(rf, 0, c), both(rf, 1, c)[lanes_of(k)]
                if t == 1:
                    ta, tb = both(rf, 2, c), both(rf, 3, c)[lanes_of(k)]
                    a = jnp.concatenate([ta, a], axis=1)
                    b = jnp.concatenate([b, tb], axis=1)
                xs[k, t, c] = dot(a, b, NT).astype(BF16)
            xy_start(*xx(t, k))

    def zz(t, k):
        return (
            5 + 2 * t + k,
            lambda p: zs.at[k, t, pl.ds(4 * slot(p), 4)],
            lambda p: zr.at[k, t, :, rows_of(p, 32), :],
            zr.at[k, t, :, 0:96, :],
        )

    for t in range(2):
        for k in range(2):
            xy_wait(*xx(t, k))
            spread(k, t, xr)

            def turn(r):
                zs[k, t, r] = get(k, 512 * t + r).astype(BF16)

            loop(0, 16, turn)
            q_start(*zz(t, k))

    hs[...] = jnp.zeros_like(hs)

    def head(k, r):
        znr = zn[4 * own + r, lanes_of(k), :]
        x = zr[k, 0, r].astype(F32)
        tx = zr[k, 1, r].astype(F32)
        c = x - mean0(x)
        rs = lax.rsqrt(mean0(c * c) + EPS)
        xnb = (c * rs).astype(BF16)
        tc = tx - mean0(tx)
        slope = -0.5 * (rs * rs * rs)
        drs = slope * mean0(2.0 * c * tc)
        dxnb = (tc * rs + c * drs).astype(BF16)
        g = dot(wt[512:640, :], znr, NT)
        dg = dot(vt[512:640, :], znr, NT)
        w_out = wt[640:768, :]
        out = dot(w_out, xnb, NN)
        dout = dot(w_out, dxnb, NN) + dot(vt[640:768, :], xnb, NN)
        s = jax.nn.sigmoid(g)
        sp = s * (1.0 - s)
        y = s * out
        ybar = (sp * dg * out + s * dout) * (1.0 / TOTAL)
        gbar = (ybar * out * sp).astype(BF16)
        obar = (ybar * s).astype(BF16)
        xnbar = dot(w_ref[:, 640:768], obar, NN).astype(BF16).astype(F32)
        rsbar = jnp.sum(xnbar * c, axis=0, keepdims=True)
        cbar = xnbar * rs + c * (rsbar * slope * (2.0 / 128))
        xb4[k, r] = (cbar - mean0(cbar)).astype(BF16)
        row = pg[4 * own + r, lanes_of(k), :].astype(F32)
        outs[r, lanes_of(k), :] = (row + y.T).astype(BF16)
        return dot(gbar, znr, NN), dot(obar, xnb, NT)

    def heads(k, i):
        first, second = head(k, 2 * i), head(k, 2 * i + 1)
        hs[0:128, :] += first[0] + second[0]
        hs[128:256, :] += first[1] + second[1]

    def xb(k):
        return (
            2 + k,
            lambda p: xb4.at[k, :, rows_of(p, 32), :],
            lambda p: xbr.at[k, pl.ds(4 * slot(p), 4)],
            xbr.at[k, 0:12],
        )

    five = (4, lambda p: hs.at[rows_of(p, 64), :], lambda p: hr.at[p], hr.at[0:3])
    for k in range(2):
        q_wait(*zz(0, k))
        q_wait(*zz(1, k))
        loop(0, 2, lambda i: heads(k, i))
        q_start(*xb(k))

    def back():
        return rcopy(outs, out_ref, o_s, o_r, dev(src_c, src_a))

    def keep():
        return pltpu.make_async_copy(outs, out_ref, o_s)

    def rr(k):
        return (
            4 + k,
            lambda p: xbs.at[k, pl.ds(2 * p, 2)],
            lambda p: rx.at[k, :, rows_of(p, 16), :],
            rx.at[k, :, 0:240, :],
        )

    for k in range(2):
        q_wait(*xb(k))
        loop(0, 16, lambda r: put(k, r, xbr[k, r].astype(F32)))

        def pack_back(i):
            val = tmp[flat(k, i), :].reshape(8, 16, 128)
            xbs[k, pl.ds(8 * i, 8)] = val.astype(BF16)

        loop(0, 4, pack_back)
        xy_start(*rr(k))

    q_start(*five)

    for k in range(2):
        xy_wait(*rr(k))

    def aa(k):
        return (
            6 + k,
            lambda p: as_.at[k, :, :, rows_of(p, 16), :],
            lambda p: ar.at[k, :, pl.ds(2 * p, 2)],
            ar.at[k, :, 0:30],
        )

    for c in range(2):
        xbar = both(rx, c)
        abar = dot(xbar, both(rf, 1, c), NN).astype(BF16)
        bbar = dot(xbar, both(rf, 0, c), TN).astype(BF16)
        for k in range(2):
            as_[k, 0, c] = abar[:, lanes_of(k)]
            as_[k, 1, c] = bbar[:, lanes_of(k)]
    for k in range(2):
        xy_start(*aa(k))

    @pl.when(moved)
    def _():
        back().start()

    @pl.when(stays)
    def _():
        keep().start()

    gi[...] = jnp.zeros_like(gi)
    q_wait(*five)
    hsum[...] = hr[0] + hr[1] + hr[2] + hr[3]
    for k in range(2):
        xy_wait(*aa(k))
        spread(k, 0, ar)
        spread(k, 1, ar)

        def grad(r):
            ra = get(k, r)
            rb = get(k, 512 + r)
            d = (fac[k, r] * jnp.concatenate([ra, ra, rb, rb], axis=0)).astype(BF16)
            return dot(d, zn[r, lanes_of(k), :], NN)

        def grads(i):
            gi[...] += (grad(4 * i) + grad(4 * i + 1)) + (grad(4 * i + 2) + grad(4 * i + 3))

        loop(0, 4, grads)

    for p in range(16):
        us[p, 0] = gi[8 * p : 8 * p + 4, :]
        us[p, 1] = gi[8 * p + 4 : 8 * p + 8, :]
        us[p, 2] = hsum[4 * p : 4 * p + 4, :]
    eight = (8, lambda p: us.at[p], lambda p: ur.at[p], ur.at[0:15])
    xy_start(*eight)
    xy_wait(*eight)
    total = ur[0]
    for p in range(1, 16):
        total = total + ur[p]
    vb[v] = total

    for d in (4, 3, 5, 2, 6, 1, 7):
        rcopy(vb.at[v], vb.at[v], v_s, v_r, v_dev(lax.rem(v + d, 8))).start()
    rcopy(vb.at[0:7], vb.at[0:7], v_s, v_r, v_dev(lax.rem(v + 1, 8))).wait()
    total = vb[0]
    for p in range(1, 8):
        total = total + vb[p]
    wb[xy, q] = total.astype(BF16)

    for p in (q2, q3, q1):
        here = wb.at[xy, q]
        rcopy(here, here, q_s.at[0], q_r.at[0], q_dev(p)).start()
    most = wb.at[0, 0:3]
    rcopy(most, most, q_s.at[0], q_r.at[0], q_dev(q1)).wait()
    here = wb.at[xy]
    for p in peers:
        rcopy(here, here, xs_s.at[9], xs_r.at[9], xy_dev(p)).start()
    most = wb.at[0:15]
    rcopy(most, most, xs_s.at[9], xs_r.at[9], xy_dev(peers[0])).wait()

    for p in range(4):
        for k in range(16):
            lo = 128 * (k // 4) + 32 * p + 8 * (k % 4)
            ft[lo : lo + 4, :] = wb[k, p, 0].astype(F32)
            ft[lo + 4 : lo + 8, :] = wb[k, p, 1].astype(F32)
            lo = 512 + 64 * p + 4 * k
            ft[lo : lo + 4, :] = wb[k, p, 2].astype(F32)
    for t in range(6):
        cols = slice(128 * t, 128 * t + 128)
        curv_ref[:, cols] = ft[cols, :].T

    @pl.when(moved)
    def _():
        back().wait()

    @pl.when(stays)
    def _():
        keep().wait()

def shards(pair, crop_mask, weights, probe_signs):
    dma = pltpu.SemaphoreType.DMA
    out, curv = pl.pallas_call(
        kernel,
        out_shape=(
            pltpu.VMEM((4, 256, 128), BF16),
            pltpu.VMEM((128, 768), F32),
        ),
        in_specs=[pl.BlockSpec(memory_space=pltpu.HBM)] * 4,
        out_specs=(pl.BlockSpec(memory_space=pltpu.VMEM),) * 2,
        scratch_shapes=[
            pltpu.VMEM((4, 256, 128), BF16),
            pltpu.VMEM((1, 256), jnp.int32),
            pltpu.VMEM((128, 768), BF16),
            pltpu.VMEM((128, 768), jnp.int32),
            pltpu.VMEM((768, 128), BF16),
            pltpu.VMEM((768, 128), BF16),
            pltpu.VMEM((256, 128), BF16),
            pltpu.VMEM((16, 256, 128), BF16),
            pltpu.VMEM((1, 256), jnp.int32),
            pltpu.VMEM((16, 256, 128), BF16),
            pltpu.VMEM((2, 16, 128, 128), F32),
            pltpu.VMEM((4096, 128), F32),
            pltpu.VMEM((2, 4, 32, 16, 128), BF16),
            pltpu.VMEM((2, 4, 2, 256, 128), BF16),
            pltpu.VMEM((2, 2, 2, 256, 128), BF16),
            pltpu.VMEM((2, 2, 32, 16, 128), BF16),
            pltpu.VMEM((2, 2, 16, 32, 128), BF16),
            pltpu.VMEM((2, 2, 4, 128, 128), BF16),
            pltpu.VMEM((4, 256, 128), BF16),
            pltpu.VMEM((2, 4, 128, 128), BF16),
            pltpu.VMEM((2, 16, 32, 128), BF16),
            pltpu.VMEM((2, 32, 16, 128), BF16),
            pltpu.VMEM((2, 2, 256, 128), BF16),
            pltpu.VMEM((2, 2, 2, 256, 128), BF16),
            pltpu.VMEM((2, 2, 32, 16, 128), BF16),
            pltpu.VMEM((64, 128), F32),
            pltpu.VMEM((256, 128), F32),
            pltpu.VMEM((4, 64, 128), F32),
            pltpu.VMEM((128, 128), F32),
            pltpu.VMEM((16, 3, 4, 128), F32),
            pltpu.VMEM((16, 3, 4, 128), F32),
            pltpu.VMEM((8, 3, 4, 128), F32),
            pltpu.VMEM((16, 4, 3, 4, 128), BF16),
            pltpu.VMEM((768, 128), F32),
            dma((4,)), dma((5,)), dma((5,)), dma((3, 4)), dma((3, 4)),
            dma((16,)), dma((16,)), dma((9,)), dma((9,)),
            dma, dma, dma, dma, dma((4,)), dma((9,)),
        ],
        compiler_params=pltpu.CompilerParams(
            collective_id=0, has_side_effects=True, vmem_limit_bytes=58 * 2**20
        ),
    )(pair[0], crop_mask, weights, probe_signs)
    return out[None], curv


def solution(mesh):
    placed = (P("crop", "axial", None, None), P("crop", None), P(), P())
    return jax.shard_map(
        shards,
        mesh=mesh,
        in_specs=placed,
        out_specs=(P("crop", "axial", None, None), P()),
        check_vma=False,
    )
```

```python
import jax
import jax.numpy as jnp
from jax import lax
from jax.experimental import pallas as pl
from jax.experimental.pallas import tpu as pltpu
from jax.sharding import PartitionSpec as P

MESH = pl.DeviceIdType.MESH
F32 = jnp.float32
BF16 = jnp.bfloat16
EPS = 1e-05
TOTAL = 8 * 256 * 256
NT = (((1,), (1,)), ((), ()))
NN = (((1,), (0,)), ((), ()))
TN = (((0,), (0,)), ((), ()))


def dot(a, b, dims):
    return lax.dot_general(a, b, dims, preferred_element_type=F32)


def mean0(value):
    return jnp.mean(value, axis=0, keepdims=True)


BLOCK_OF = (7, 3, 5, 1, 4, 0, 6, 2)
PLACE_OF = (
    (3, 2, 0, 1), (1, 0, 3, 2), (2, 1, 0, 3), (0, 2, 3, 1),
    (1, 0, 2, 3), (3, 2, 0, 1), (3, 1, 0, 2), (0, 3, 2, 1),
)


SHIFTS = (
    (2, 2), (2, 1), (1, 2), (2, 3), (3, 2), (1, 1), (3, 3), (1, 3), (3, 1),
    (2, 0), (0, 2), (1, 0), (0, 1), (3, 0), (0, 3),
)


def table(index, values):
    found = 0
    for k, value in enumerate(values):
        found = found + jnp.where(index == k, value, 0)
    return found


def loop(lo, hi, body):
    def step(i, carry):
        body(i)
        return carry

    lax.fori_loop(lo, hi, step, 0)


def kernel(
    pair_ref, cmask_ref, w_any, s_any,
    out_ref, curv_ref,
    pv, cm, w_ref, s_ref,
    wt, vt, wq, pg, mk, zn, fac, tmp,
    sf, rf, xs, xr, zs, zr, outs, xb4, xbr, xbs, rx, as_, ar,
    hsum, hs, hr, gi, us, ur, vb, wb, ft,
    in_s, mv_s, mv_r, ag_s, ag_r, xs_s, xs_r, q_s, q_r, v_s, v_r, o_s, o_r, lx_s, lq_s,
):
    crop = lax.axis_index("crop")
    axial = lax.axis_index("axial")
    xy = lax.div(axial, 4)
    hi = lax.rem(axial, 4)
    half = lax.div(crop, 4)
    q = lax.rem(crop, 4)
    v = 2 * hi + half

    def dev(c, a):
        return {"crop": c, "axial": a}

    def xy_dev(p):
        return dev(crop, 4 * p + hi)

    def q_dev(p):
        return dev(4 * half + p, axial)

    def v_dev(p):
        return dev(4 * lax.rem(p, 2) + q, 4 * xy + lax.div(p, 2))

    dst = table(
        4 * crop + hi, [4 * BLOCK_OF[c] + PLACE_OF[c][k] for c in range(8) for k in range(4)]
    )
    home = {4 * BLOCK_OF[c] + PLACE_OF[c][k]: 4 * c + k for c in range(8) for k in range(4)}
    homes = [home[k] for k in range(32)]
    src = table(4 * v + q, homes)
    slots = [table(v, [homes[4 * b + p] % 4 for b in range(8)]) for p in range(4)]

    def slot(p):
        return table(p, slots)

    dst_v, dst_q = lax.div(dst, 4), lax.rem(dst, 4)
    dst_c = 4 * lax.rem(dst_v, 2) + dst_q
    dst_a = 4 * xy + lax.div(dst_v, 2)
    src_c = lax.div(src, 4)
    src_a = 4 * xy + lax.rem(src, 4)
    moved = dst != 4 * v + q
    stays = jnp.logical_not(moved)

    def rcopy(src, dst, ssem, rsem, to):
        return pltpu.make_async_remote_copy(
            src_ref=src, dst_ref=dst, send_sem=ssem, recv_sem=rsem,
            device_id=to, device_id_type=MESH,
        )

    peers = [
        4 * lax.rem(lax.div(xy, 4) + dx, 4) + lax.rem(lax.rem(xy, 4) + dy, 4)
        for dx, dy in SHIFTS
    ]

    barrier = pltpu.get_barrier_semaphore()

    def greet(to):
        pl.semaphore_signal(barrier, inc=1, device_id=to, device_id_type=MESH)

    @pl.when(moved)
    def _():
        greet(dev(dst_c, dst_a))
        greet(dev(src_c, src_a))

    for d in (4, 3, 5, 2, 6, 1, 7):
        greet(v_dev(lax.rem(v + d, 8)))
    for p in peers:
        greet(xy_dev(p))
    for d in (2, 3, 1):
        greet(q_dev(lax.rem(q + d, 4)))

    loads = [
        pltpu.make_async_copy(a, b, in_s.at[k])
        for k, (a, b) in enumerate(
            ((w_any, w_ref), (s_any, s_ref), (cmask_ref, cm), (pair_ref, pv))
        )
    ]
    for load in loads:
        load.start()
    loads[2].wait()
    loads[3].wait()

    @pl.when(moved)
    def _():
        pl.semaphore_wait(barrier, 27)

    @pl.when(stays)
    def _():
        pl.semaphore_wait(barrier, 25)

    def put(k, lo, val):
        tmp[pl.ds(2048 * k + lo, 32, stride=16), :] = val

    def get(k, lo):
        return tmp[pl.ds(2048 * k + lo, 32, stride=16), :]

    def flat(k, i):
        return pl.ds(pl.multiple_of(2048 * k + 128 * i, 128), 128)

    def spread(k, t, src):
        for i in range(4):
            val = src[k, t, 8 * i : 8 * i + 8].astype(F32)
            tmp[flat(k, 4 * t + i), :] = val.reshape(128, 128)

    own = slot(q)

    def lanes_of(k):
        return slice(128 * k, 128 * k + 128)

    def piece(p, i):
        return pl.ds(4 * p + 2 * (i % 2), 2), lanes_of(i // 2)

    def mv_pair(i):
        return rcopy(
            pv.at[piece(0, i)], pg.at[piece(hi, i)], mv_s.at[i], mv_r.at[i], dev(dst_c, dst_a)
        )

    def mv_mask():
        return rcopy(cm, mk, mv_s.at[4], mv_r.at[4], dev(dst_c, dst_a))

    def own_pair(i):
        return pltpu.make_async_copy(pv.at[piece(0, i)], pg.at[piece(own, i)], mv_r.at[i])

    def own_mask():
        return pltpu.make_async_copy(cm, mk, mv_r.at[4])

    def launch(i):
        @pl.when(moved)
        def _():
            if i == 0:
                mv_mask().start()
            mv_pair(i).start()

        @pl.when(stays)
        def _():
            if i == 0:
                own_mask().start()
            own_pair(i).start()

    launch(0)
    launch(1)
    launch(2)

    loads[0].wait()
    loads[1].wait()
    for t in range(6):
        cols = slice(128 * t, 128 * t + 128)
        wt[cols, :] = w_ref[:, cols].astype(F32).T.astype(BF16)
        probe = (2 * s_ref[:, cols] - 1).astype(F32) * (1.0 / jnp.sqrt(F32(128)))
        vt[cols, :] = probe.T.astype(BF16)
    for t in range(4):
        rows = pl.ds(pl.multiple_of(128 * t + 32 * q, 32), 32)
        wq[32 * t : 32 * t + 32, :] = wt[rows, :]
        wq[128 + 32 * t : 160 + 32 * t, :] = vt[rows, :]

    q1 = q + 1 - 2 * lax.rem(q, 2)
    q2 = lax.rem(q + 2, 4)
    q3 = lax.rem(q1 + 2, 4)

    def carry(p, i, n, m, to):
        here = pg.at[piece(slot(p), i)]
        return rcopy(here, here, ag_s.at[n, m], ag_r.at[n, m], q_dev(to))

    def near(i):
        return carry(q, i, 0, i // 2, q1)

    def far(i):
        return carry(q, i, 1, i, q2)

    def pass_on(i):
        return carry(q2, i, 2, i // 2, q1)

    def all_rows(p, k, n, to):
        here = pg.at[pl.ds(4 * slot(p), 4), lanes_of(k)]
        return rcopy(here, here, ag_s.at[n, k], ag_r.at[n, k], q_dev(to))

    def arrived(i):
        @pl.when(moved)
        def _():
            if i == 0:
                mv_mask().wait()
            mv_pair(i).wait()

        @pl.when(stays)
        def _():
            if i == 0:
                own_mask().wait()
            own_pair(i).wait()

        far(i).start()
        near(i).start()
        if i == 0:
            launch(3)

    iota = lax.broadcasted_iota(jnp.int32, (1, 256), 1)

    def project(k, r):
        rows = pg[r, lanes_of(k), :].astype(F32)
        centered = rows - jnp.mean(rows, axis=1, keepdims=True)
        var = jnp.mean(centered * centered, axis=1, keepdims=True)
        znr = (centered * lax.rsqrt(var + EPS)).astype(BF16)
        zn[r, lanes_of(k), :] = znr
        proj = dot(wq[...], znr, NT)
        m = mk[...].astype(F32)
        mi = jnp.sum(jnp.where(iota == 16 * xy + r, m, 0.0), axis=1, keepdims=True)
        mrow = m[:, lanes_of(k)] * mi
        for side in range(2):
            lo = 64 * side
            p, g = proj[lo : lo + 32], proj[lo + 32 : lo + 64]
            tp, tg = proj[128 + lo : 160 + lo], proj[160 + lo : 192 + lo]
            s = jax.nn.sigmoid(g)
            fp = s * mrow
            fg = p * (fp * (1.0 - s))
            fac[k, r, lo : lo + 32, :] = fp
            fac[k, r, lo + 32 : lo + 64, :] = fg
            put(k, 512 * side + r, fp * p)
            put(k, 1024 + 512 * side + r, fg * tg + fp * tp)

    def project4(k, p):
        for i in range(4):
            project(k, 4 * p + i)

    def xy_start(n, src, dst, most):
        pltpu.make_async_copy(src(xy), dst(xy), lx_s.at[n % 4]).start()

        for p in peers:
            rcopy(src(p), dst(xy), xs_s.at[n], xs_r.at[n], xy_dev(p)).start()

    def xy_wait(n, src, dst, most):
        pltpu.make_async_copy(src(xy), dst(xy), lx_s.at[n % 4]).wait()
        rcopy(most, most, xs_s.at[n], xs_r.at[n], xy_dev(lax.rem(xy + 1, 16))).wait()

    def q_start(n, src, dst, most):
        pltpu.make_async_copy(src(q), dst(q), lq_s.at[n]).start()

        for p in (q2, q3, q1):
            rcopy(src(p), dst(q), q_s.at[n], q_r.at[n], q_dev(p)).start()

    def q_wait(n, src, dst, most):
        pltpu.make_async_copy(src(q), dst(q), lq_s.at[n]).wait()
        rcopy(most, most, q_s.at[n], q_r.at[n], q_dev(q1)).wait()

    def rows_of(p, n):
        return pl.ds(pl.multiple_of(n * p, n), n)

    def ab(t, k):
        two = pl.ds(2 * t, 2)
        return (
            12 + 2 * t + k,
            lambda p: sf.at[k, two, pl.ds(2 * p, 2)],
            lambda p: rf.at[k, two, :, rows_of(p, 16), :],
            rf.at[k, two, :, 0:240, :],
        )

    def pack(k):
        def body(i):
            val = tmp[flat(k, i), :].reshape(8, 16, 128)
            sf[k, lax.div(i, 4), pl.ds(8 * lax.rem(i, 4), 8)] = val.astype(BF16)

        loop(0, 16, body)
        xy_start(*ab(0, k))
        xy_start(*ab(1, k))

    arrived(0)
    arrived(1)
    for k in range(2):
        project4(k, slot(q))
        for i in (2 * k, 2 * k + 1):
            far(i).wait_recv()
            pass_on(i).start()
        project4(k, slot(q2))
        all_rows(q, k, 0, q1).wait_recv()
        project4(k, slot(q1))
        if k == 0:
            arrived(2)
        all_rows(q2, k, 2, q1).wait_recv()
        project4(k, slot(q3))
        pack(k)
        if k == 0:
            arrived(3)
    for k in range(2):
        all_rows(q, k, 0, q1).wait_send()
        all_rows(q2, k, 2, q1).wait_send()
    for i in range(4):
        far(i).wait_send()
    def xx(t, k):
        return (
            2 * t + k,
            lambda p: xs.at[k, t, :, rows_of(p, 16), :],
            lambda p: xr.at[k, t, pl.ds(2 * p, 2)],
            xr.at[k, t, 0:30],
        )

    def both(ref, *at):
        return jnp.concatenate([ref[(0, *at)], ref[(1, *at)]], axis=1)

    for t in range(2):
        for k in range(2):
            xy_wait(*ab(t, k))
        for k in range(2):
            for c in range(2):
                a, b = both(rf, 0, c), both(rf, 1, c)[lanes_of(k)]
                if t == 1:
                    ta, tb = both(rf, 2, c), both(rf, 3, c)[lanes_of(k)]
                    a = jnp.concatenate([ta, a], axis=1)
                    b = jnp.concatenate([b, tb], axis=1)
                xs[k, t, c] = dot(a, b, NT).astype(BF16)
            xy_start(*xx(t, k))

    def zz(t, k):
        return (
            5 + 2 * t + k,
            lambda p: zs.at[k, t, pl.ds(4 * slot(p), 4)],
            lambda p: zr.at[k, t, :, rows_of(p, 32), :],
            zr.at[k, t, :, 0:96, :],
        )

    for t in range(2):
        for k in range(2):
            xy_wait(*xx(t, k))
            spread(k, t, xr)

            def turn(r):
                zs[k, t, r] = get(k, 512 * t + r).astype(BF16)

            loop(0, 16, turn)
            q_start(*zz(t, k))

    hs[...] = jnp.zeros_like(hs)

    def heads(k):
        zn4 = zn[pl.ds(4 * own, 4), lanes_of(k), :].reshape(512, 128)
        x = jnp.concatenate([zr[k, 0, r] for r in range(4)], axis=1).astype(F32)
        tx = jnp.concatenate([zr[k, 1, r] for r in range(4)], axis=1).astype(F32)
        c = x - mean0(x)
        rs = lax.rsqrt(mean0(c * c) + EPS)
        xnb = (c * rs).astype(BF16)
        tc = tx - mean0(tx)
        slope = -0.5 * (rs * rs * rs)
        drs = slope * mean0(2.0 * c * tc)
        dxnb = (tc * rs + c * drs).astype(BF16)
        gates = dot(jnp.concatenate([wt[512:640, :], vt[512:640, :]], axis=0), zn4, NT)
        w_out = wt[640:768, :]
        outs2 = dot(jnp.concatenate([w_out, vt[640:768, :]], axis=0), xnb, NN)
        out = outs2[:128]
        dout = dot(w_out, dxnb, NN) + outs2[128:]
        s = jax.nn.sigmoid(gates[:128])
        sp = s * (1.0 - s)
        y = s * out
        ybar = (sp * gates[128:] * out + s * dout) * (1.0 / TOTAL)
        gbar = (ybar * out * sp).astype(BF16)
        obar = (ybar * s).astype(BF16)
        xnbar = dot(w_ref[:, 640:768], obar, NN).astype(BF16).astype(F32)
        rsbar = jnp.sum(xnbar * c, axis=0, keepdims=True)
        cbar = xnbar * rs + c * (rsbar * slope * (2.0 / 128))
        xbar = (cbar - mean0(cbar)).astype(BF16)
        for r in range(4):
            xb4[k, r] = xbar[:, lanes_of(r)]
        return y, gbar, obar, xnb, zn4

    def rest(k, y, gbar, obar, xnb, zn4):
        hs[0:128, :] += dot(gbar, zn4, NN)
        hs[128:256, :] += dot(obar, xnb, NT)
        for r in range(4):
            row = pg[4 * own + r, lanes_of(k), :].astype(F32)
            outs[r, lanes_of(k), :] = (row + y[:, lanes_of(r)].T).astype(BF16)

    def xb(k):
        return (
            2 + k,
            lambda p: xb4.at[k, :, rows_of(p, 32), :],
            lambda p: xbr.at[k, pl.ds(4 * slot(p), 4)],
            xbr.at[k, 0:12],
        )

    five = (4, lambda p: hs.at[rows_of(p, 64), :], lambda p: hr.at[p], hr.at[0:3])
    for k in range(2):
        q_wait(*zz(0, k))
        q_wait(*zz(1, k))
        kept = heads(k)
        q_start(*xb(k))
        rest(k, *kept)

    def back():
        return rcopy(outs, out_ref, o_s, o_r, dev(src_c, src_a))

    def keep():
        return pltpu.make_async_copy(outs, out_ref, o_s)

    def rr(k):
        return (
            4 + k,
            lambda p: xbs.at[k, pl.ds(2 * p, 2)],
            lambda p: rx.at[k, :, rows_of(p, 16), :],
            rx.at[k, :, 0:240, :],
        )

    for k in range(2):
        q_wait(*xb(k))
        loop(0, 16, lambda r: put(k, r, xbr[k, r].astype(F32)))

        def pack_back(i):
            val = tmp[flat(k, i), :].reshape(8, 16, 128)
            xbs[k, pl.ds(8 * i, 8)] = val.astype(BF16)

        loop(0, 4, pack_back)
        xy_start(*rr(k))

    q_start(*five)

    for k in range(2):
        xy_wait(*rr(k))

    def aa(t, k):
        return (
            6 + 10 * t + k,
            lambda p: as_.at[k, t, :, rows_of(p, 16), :],
            lambda p: ar.at[k, t, pl.ds(2 * p, 2)],
            ar.at[k, t, 0:30],
        )

    for t in range(2):
        for c in range(2):
            bar = dot(both(rx, c), both(rf, 1 - t, c), TN if t else NN).astype(BF16)
            for k in range(2):
                as_[k, t, c] = bar[:, lanes_of(k)]
        for k in range(2):
            xy_start(*aa(t, k))

    @pl.when(moved)
    def _():
        back().start()

    @pl.when(stays)
    def _():
        keep().start()

    gi[...] = jnp.zeros_like(gi)
    q_wait(*five)
    hsum[...] = hr[0] + hr[1] + hr[2] + hr[3]
    def grad(t, k, r):
        bar = get(k, 512 * t + r)
        d = fac[k, r, 64 * t : 64 * t + 64, :] * jnp.concatenate([bar, bar], axis=0)
        return dot(d.astype(BF16), zn[r, lanes_of(k), :], NN)

    for t in range(2):
        for k in range(2):
            xy_wait(*aa(t, k))
            spread(k, t, ar)

            def grads(i):
                parts = [grad(t, k, 8 * i + n) for n in range(8)]
                while len(parts) > 1:
                    parts = [x + y for x, y in zip(parts[::2], parts[1::2])]
                gi[64 * t : 64 * t + 64, :] += parts[0]

            loop(0, 2, grads)

    for p in range(16):
        us[p, 0] = gi[8 * p : 8 * p + 4, :]
        us[p, 1] = gi[8 * p + 4 : 8 * p + 8, :]
        us[p, 2] = hsum[4 * p : 4 * p + 4, :]
    eight = (8, lambda p: us.at[p], lambda p: ur.at[p], ur.at[0:15])
    xy_start(*eight)
    xy_wait(*eight)
    total = ur[0]
    for p in range(1, 16):
        total = total + ur[p]
    vb[v] = total

    for d in (4, 3, 5, 2, 6, 1, 7):
        rcopy(vb.at[v], vb.at[v], v_s, v_r, v_dev(lax.rem(v + d, 8))).start()
    rcopy(vb.at[0:7], vb.at[0:7], v_s, v_r, v_dev(lax.rem(v + 1, 8))).wait()
    total = vb[0]
    for p in range(1, 8):
        total = total + vb[p]
    wb[xy, q] = total.astype(BF16)

    for p in (q2, q3, q1):
        here = wb.at[xy, q]
        rcopy(here, here, q_s.at[0], q_r.at[0], q_dev(p)).start()
    most = wb.at[0, 0:3]
    rcopy(most, most, q_s.at[0], q_r.at[0], q_dev(q1)).wait()
    here = wb.at[xy]
    for p in peers:
        rcopy(here, here, xs_s.at[9], xs_r.at[9], xy_dev(p)).start()
    most = wb.at[0:15]
    rcopy(most, most, xs_s.at[9], xs_r.at[9], xy_dev(peers[0])).wait()

    for p in range(4):
        for k in range(16):
            lo = 128 * (k // 4) + 32 * p + 8 * (k % 4)
            ft[lo : lo + 4, :] = wb[k, p, 0].astype(F32)
            ft[lo + 4 : lo + 8, :] = wb[k, p, 1].astype(F32)
            lo = 512 + 64 * p + 4 * k
            ft[lo : lo + 4, :] = wb[k, p, 2].astype(F32)
    for t in range(6):
        cols = slice(128 * t, 128 * t + 128)
        curv_ref[:, cols] = ft[cols, :].T

    @pl.when(moved)
    def _():
        back().wait()

    @pl.when(stays)
    def _():
        keep().wait()

def shards(pair, crop_mask, weights, probe_signs):
    dma = pltpu.SemaphoreType.DMA
    out, curv = pl.pallas_call(
        kernel,
        out_shape=(
            pltpu.VMEM((4, 256, 128), BF16),
            pltpu.VMEM((128, 768), F32),
        ),
        in_specs=[pl.BlockSpec(memory_space=pltpu.HBM)] * 4,
        out_specs=(pl.BlockSpec(memory_space=pltpu.VMEM),) * 2,
        scratch_shapes=[
            pltpu.VMEM((4, 256, 128), BF16),
            pltpu.VMEM((1, 256), jnp.int32),
            pltpu.VMEM((128, 768), BF16),
            pltpu.VMEM((128, 768), jnp.int32),
            pltpu.VMEM((768, 128), BF16),
            pltpu.VMEM((768, 128), BF16),
            pltpu.VMEM((256, 128), BF16),
            pltpu.VMEM((16, 256, 128), BF16),
            pltpu.VMEM((1, 256), jnp.int32),
            pltpu.VMEM((16, 256, 128), BF16),
            pltpu.VMEM((2, 16, 128, 128), F32),
            pltpu.VMEM((4096, 128), F32),
            pltpu.VMEM((2, 4, 32, 16, 128), BF16),
            pltpu.VMEM((2, 4, 2, 256, 128), BF16),
            pltpu.VMEM((2, 2, 2, 256, 128), BF16),
            pltpu.VMEM((2, 2, 32, 16, 128), BF16),
            pltpu.VMEM((2, 2, 16, 32, 128), BF16),
            pltpu.VMEM((2, 2, 4, 128, 128), BF16),
            pltpu.VMEM((4, 256, 128), BF16),
            pltpu.VMEM((2, 4, 128, 128), BF16),
            pltpu.VMEM((2, 16, 32, 128), BF16),
            pltpu.VMEM((2, 32, 16, 128), BF16),
            pltpu.VMEM((2, 2, 256, 128), BF16),
            pltpu.VMEM((2, 2, 2, 256, 128), BF16),
            pltpu.VMEM((2, 2, 32, 16, 128), BF16),
            pltpu.VMEM((64, 128), F32),
            pltpu.VMEM((256, 128), F32),
            pltpu.VMEM((4, 64, 128), F32),
            pltpu.VMEM((128, 128), F32),
            pltpu.VMEM((16, 3, 4, 128), F32),
            pltpu.VMEM((16, 3, 4, 128), F32),
            pltpu.VMEM((8, 3, 4, 128), F32),
            pltpu.VMEM((16, 4, 3, 4, 128), BF16),
            pltpu.VMEM((768, 128), F32),
            dma((4,)), dma((5,)), dma((5,)), dma((3, 4)), dma((3, 4)),
            dma((18,)), dma((18,)), dma((9,)), dma((9,)),
            dma, dma, dma, dma, dma((4,)), dma((9,)),
        ],
        compiler_params=pltpu.CompilerParams(
            collective_id=0, has_side_effects=True, vmem_limit_bytes=58 * 2**20
        ),
    )(pair[0], crop_mask, weights, probe_signs)
    return out[None], curv


def solution(mesh):
    placed = (P("crop", "axial", None, None), P("crop", None), P(), P())
    return jax.shard_map(
        shards,
        mesh=mesh,
        in_specs=placed,
        out_specs=(P("crop", "axial", None, None), P()),
        check_vma=False,
    )
```

```python
import jax
import jax.numpy as jnp
from jax import lax
from jax.experimental import pallas as pl
from jax.experimental.pallas import tpu as pltpu
from jax.sharding import PartitionSpec as P

MESH = pl.DeviceIdType.MESH
F32 = jnp.float32
BF16 = jnp.bfloat16
EPS = 1e-05
TOTAL = 8 * 256 * 256
NT = (((1,), (1,)), ((), ()))
NN = (((1,), (0,)), ((), ()))
TN = (((0,), (0,)), ((), ()))


def dot(a, b, dims):
    return lax.dot_general(a, b, dims, preferred_element_type=F32)


def mean0(value):
    return jnp.mean(value, axis=0, keepdims=True)


BLOCK_OF = (7, 3, 5, 1, 4, 0, 6, 2)
PLACE_OF = (
    (3, 2, 0, 1), (1, 0, 3, 2), (2, 1, 0, 3), (0, 2, 3, 1),
    (1, 0, 2, 3), (3, 2, 0, 1), (3, 1, 0, 2), (0, 3, 2, 1),
)


SHIFTS = (
    (2, 2), (2, 1), (1, 2), (2, 3), (3, 2), (1, 1), (3, 3), (1, 3), (3, 1),
    (2, 0), (0, 2), (1, 0), (0, 1), (3, 0), (0, 3),
)


def table(index, values):
    found = 0
    for k, value in enumerate(values):
        found = found + jnp.where(index == k, value, 0)
    return found


def loop(lo, hi, body):
    def step(i, carry):
        body(i)
        return carry

    lax.fori_loop(lo, hi, step, 0)


def kernel(
    pair_ref, cmask_ref, w_any, s_any,
    out_ref, curv_ref,
    pv, cm, w_ref, s_ref,
    wt, vt, wq, pg, mk, zn, fac, tmp,
    sf, rf, xs, xr, zs, zr, outs, xb4, xbr, xbs, rx, as_, ar,
    hsum, hs, hr, gi, us, ur, vb, wb, ft,
    in_s, mv_s, mv_r, ag_s, ag_r, xs_s, xs_r, q_s, q_r, v_s, v_r, o_s, o_r, lx_s, lq_s,
):
    crop = lax.axis_index("crop")
    axial = lax.axis_index("axial")
    xy = lax.div(axial, 4)
    hi = lax.rem(axial, 4)
    half = lax.div(crop, 4)
    q = lax.rem(crop, 4)
    v = 2 * hi + half

    def dev(c, a):
        return {"crop": c, "axial": a}

    def xy_dev(p):
        return dev(crop, 4 * p + hi)

    def q_dev(p):
        return dev(4 * half + p, axial)

    def v_dev(p):
        return dev(4 * lax.rem(p, 2) + q, 4 * xy + lax.div(p, 2))

    dst = table(
        4 * crop + hi, [4 * BLOCK_OF[c] + PLACE_OF[c][k] for c in range(8) for k in range(4)]
    )
    home = {4 * BLOCK_OF[c] + PLACE_OF[c][k]: 4 * c + k for c in range(8) for k in range(4)}
    homes = [home[k] for k in range(32)]
    src = table(4 * v + q, homes)
    slots = [table(v, [homes[4 * b + p] % 4 for b in range(8)]) for p in range(4)]

    def slot(p):
        return table(p, slots)

    dst_v, dst_q = lax.div(dst, 4), lax.rem(dst, 4)
    dst_c = 4 * lax.rem(dst_v, 2) + dst_q
    dst_a = 4 * xy + lax.div(dst_v, 2)
    src_c = lax.div(src, 4)
    src_a = 4 * xy + lax.rem(src, 4)
    moved = dst != 4 * v + q
    stays = jnp.logical_not(moved)

    def rcopy(src, dst, ssem, rsem, to):
        return pltpu.make_async_remote_copy(
            src_ref=src, dst_ref=dst, send_sem=ssem, recv_sem=rsem,
            device_id=to, device_id_type=MESH,
        )

    peers = [
        4 * lax.rem(lax.div(xy, 4) + dx, 4) + lax.rem(lax.rem(xy, 4) + dy, 4)
        for dx, dy in SHIFTS
    ]

    barrier = pltpu.get_barrier_semaphore()

    def greet(to):
        pl.semaphore_signal(barrier, inc=1, device_id=to, device_id_type=MESH)

    @pl.when(moved)
    def _():
        greet(dev(dst_c, dst_a))
        greet(dev(src_c, src_a))

    for d in (4, 3, 5, 2, 6, 1, 7):
        greet(v_dev(lax.rem(v + d, 8)))
    for p in peers:
        greet(xy_dev(p))
    for d in (2, 3, 1):
        greet(q_dev(lax.rem(q + d, 4)))

    loads = [
        pltpu.make_async_copy(a, b, in_s.at[k])
        for k, (a, b) in enumerate(
            ((w_any, w_ref), (s_any, s_ref), (cmask_ref, cm), (pair_ref, pv))
        )
    ]
    for load in loads:
        load.start()
    loads[2].wait()
    loads[3].wait()

    @pl.when(moved)
    def _():
        pl.semaphore_wait(barrier, 27)

    @pl.when(stays)
    def _():
        pl.semaphore_wait(barrier, 25)

    def put(k, lo, val):
        tmp[pl.ds(2048 * k + lo, 32, stride=16), :] = val

    def get(k, lo):
        return tmp[pl.ds(2048 * k + lo, 32, stride=16), :]

    def flat(k, i):
        return pl.ds(pl.multiple_of(2048 * k + 128 * i, 128), 128)

    def spread(k, t, src):
        for i in range(4):
            val = src[k, t, 8 * i : 8 * i + 8].astype(F32)
            tmp[flat(k, 4 * t + i), :] = val.reshape(128, 128)

    own = slot(q)

    def lanes_of(k):
        return slice(128 * k, 128 * k + 128)

    def piece(p, i):
        return pl.ds(4 * p + 2 * (i % 2), 2), lanes_of(i // 2)

    def mv_pair(i):
        return rcopy(
            pv.at[piece(0, i)], pg.at[piece(hi, i)], mv_s.at[i], mv_r.at[i], dev(dst_c, dst_a)
        )

    def mv_mask():
        return rcopy(cm, mk.at[0], mv_s.at[4], mv_r.at[4], dev(dst_c, dst_a))

    def own_pair(i):
        return pltpu.make_async_copy(pv.at[piece(0, i)], pg.at[piece(own, i)], mv_r.at[i])

    def own_mask():
        return pltpu.make_async_copy(cm, mk.at[0], mv_r.at[4])

    def launch(i):
        @pl.when(moved)
        def _():
            if i == 0:
                mv_mask().start()
            mv_pair(i).start()

        @pl.when(stays)
        def _():
            if i == 0:
                own_mask().start()
            own_pair(i).start()

    launch(0)
    launch(1)
    launch(2)

    loads[0].wait()
    loads[1].wait()
    for t in range(6):
        cols = slice(128 * t, 128 * t + 128)
        wt[cols, :] = w_ref[:, cols].astype(F32).T.astype(BF16)
        probe = (2 * s_ref[:, cols] - 1).astype(F32) * (1.0 / jnp.sqrt(F32(128)))
        vt[cols, :] = probe.T.astype(BF16)
    for t in range(4):
        rows = pl.ds(pl.multiple_of(128 * t + 32 * q, 32), 32)
        wq[32 * t : 32 * t + 32, :] = wt[rows, :]
        wq[128 + 32 * t : 160 + 32 * t, :] = vt[rows, :]

    q1 = q + 1 - 2 * lax.rem(q, 2)
    q2 = lax.rem(q + 2, 4)
    q3 = lax.rem(q1 + 2, 4)

    def carry(p, i, n, m, to):
        here = pg.at[piece(slot(p), i)]
        return rcopy(here, here, ag_s.at[n, m], ag_r.at[n, m], q_dev(to))

    def near(i):
        return carry(q, i, 0, i // 2, q1)

    def far(i):
        return carry(q, i, 1, i, q2)

    def pass_on(i):
        return carry(q2, i, 2, i // 2, q1)

    def all_rows(p, k, n, to):
        here = pg.at[pl.ds(4 * slot(p), 4), lanes_of(k)]
        return rcopy(here, here, ag_s.at[n, k], ag_r.at[n, k], q_dev(to))

    def arrived(i):
        @pl.when(moved)
        def _():
            if i == 0:
                mv_mask().wait()
            mv_pair(i).wait()

        @pl.when(stays)
        def _():
            if i == 0:
                own_mask().wait()
            own_pair(i).wait()

        far(i).start()
        near(i).start()
        if i == 0:
            launch(3)

    iota = lax.broadcasted_iota(jnp.int32, (1, 256), 1)

    def project(k, r):
        rows = pg[r, lanes_of(k), :].astype(F32)
        centered = rows - jnp.mean(rows, axis=1, keepdims=True)
        var = jnp.mean(centered * centered, axis=1, keepdims=True)
        znr = (centered * lax.rsqrt(var + EPS)).astype(BF16)
        zn[r, lanes_of(k), :] = znr
        proj = dot(wq[...], znr, NT)
        m = mk[0].astype(F32)
        mi = jnp.sum(jnp.where(iota == 16 * xy + r, m, 0.0), axis=1, keepdims=True)
        mrow = m[:, lanes_of(k)] * mi
        for side in range(2):
            lo = 64 * side
            p, g = proj[lo : lo + 32], proj[lo + 32 : lo + 64]
            tp, tg = proj[128 + lo : 160 + lo], proj[160 + lo : 192 + lo]
            s = jax.nn.sigmoid(g)
            fp = s * mrow
            fg = p * (fp * (1.0 - s))
            fac[k, r, lo : lo + 32, :] = fp
            fac[k, r, lo + 32 : lo + 64, :] = fg
            put(k, 512 * side + r, fp * p)
            put(k, 1024 + 512 * side + r, fg * tg + fp * tp)

    def project4(k, p):
        for i in range(4):
            project(k, 4 * p + i)

    def xy_start(n, src, dst, most):
        pltpu.make_async_copy(src(xy), dst(xy), lx_s.at[n % 4]).start()

        for p in peers:
            rcopy(src(p), dst(xy), xs_s.at[n], xs_r.at[n], xy_dev(p)).start()

    def xy_wait(n, src, dst, most):
        pltpu.make_async_copy(src(xy), dst(xy), lx_s.at[n % 4]).wait()
        rcopy(most, most, xs_s.at[n], xs_r.at[n], xy_dev(lax.rem(xy + 1, 16))).wait()

    def q_start(n, src, dst, most):
        pltpu.make_async_copy(src(q), dst(q), lq_s.at[n]).start()

        for p in (q2, q3, q1):
            rcopy(src(p), dst(q), q_s.at[n], q_r.at[n], q_dev(p)).start()

    def q_wait(n, src, dst, most):
        pltpu.make_async_copy(src(q), dst(q), lq_s.at[n]).wait()
        rcopy(most, most, q_s.at[n], q_r.at[n], q_dev(q1)).wait()

    def rows_of(p, n):
        return pl.ds(pl.multiple_of(n * p, n), n)

    def ab(t, k):
        two = pl.ds(2 * t, 2)
        return (
            12 + 2 * t + k,
            lambda p: sf.at[k, two, pl.ds(2 * p, 2)],
            lambda p: rf.at[k, two, :, rows_of(p, 16), :],
            rf.at[k, two, :, 0:240, :],
        )

    def pack(k):
        def body(i):
            val = tmp[flat(k, i), :].reshape(8, 16, 128)
            sf[k, lax.div(i, 4), pl.ds(8 * lax.rem(i, 4), 8)] = val.astype(BF16)

        loop(0, 16, body)
        xy_start(*ab(0, k))
        xy_start(*ab(1, k))

    arrived(0)
    arrived(1)
    for k in range(2):
        project4(k, slot(q))
        for i in (2 * k, 2 * k + 1):
            far(i).wait_recv()
            pass_on(i).start()
        project4(k, slot(q2))
        all_rows(q, k, 0, q1).wait_recv()
        project4(k, slot(q1))
        if k == 0:
            arrived(2)
        all_rows(q2, k, 2, q1).wait_recv()
        project4(k, slot(q3))
        pack(k)
        if k == 0:
            arrived(3)
    for k in range(2):
        all_rows(q, k, 0, q1).wait_send()
        all_rows(q2, k, 2, q1).wait_send()
    for i in range(4):
        far(i).wait_send()
    def xx(t, k):
        return (
            2 * t + k,
            lambda p: xs.at[k, t, :, rows_of(p, 16), :],
            lambda p: xr.at[k, t, pl.ds(2 * p, 2)],
            xr.at[k, t, 0:30],
        )

    def both(ref, *at):
        return jnp.concatenate([ref[(0, *at)], ref[(1, *at)]], axis=1)

    for t in range(2):
        for k in range(2):
            xy_wait(*ab(t, k))
        for k in range(2):
            for c in range(2):
                a, b = both(rf, 0, c), both(rf, 1, c)[lanes_of(k)]
                if t == 1:
                    ta, tb = both(rf, 2, c), both(rf, 3, c)[lanes_of(k)]
                    a = jnp.concatenate([ta, a], axis=1)
                    b = jnp.concatenate([b, tb], axis=1)
                xs[k, t, c] = dot(a, b, NT).astype(BF16)
            xy_start(*xx(t, k))

    def zz(t, k):
        return (
            5 + 2 * t + k,
            lambda p: zs.at[k, t, pl.ds(4 * slot(p), 4)],
            lambda p: zr.at[k, t, :, rows_of(p, 32), :],
            zr.at[k, t, :, 0:96, :],
        )

    for t in range(2):
        for k in range(2):
            xy_wait(*xx(t, k))
            spread(k, t, xr)

            def turn(r):
                zs[k, t, r] = get(k, 512 * t + r).astype(BF16)

            loop(0, 16, turn)
            q_start(*zz(t, k))

    hs[...] = jnp.zeros_like(hs)

    def heads(k):
        zn4 = zn[pl.ds(4 * own, 4), lanes_of(k), :].reshape(512, 128)
        x = jnp.concatenate([zr[k, 0, r] for r in range(4)], axis=1).astype(F32)
        tx = jnp.concatenate([zr[k, 1, r] for r in range(4)], axis=1).astype(F32)
        c = x - mean0(x)
        rs = lax.rsqrt(mean0(c * c) + EPS)
        xnb = (c * rs).astype(BF16)
        tc = tx - mean0(tx)
        slope = -0.5 * (rs * rs * rs)
        drs = slope * mean0(2.0 * c * tc)
        dxnb = (tc * rs + c * drs).astype(BF16)
        gates = dot(jnp.concatenate([wt[512:640, :], vt[512:640, :]], axis=0), zn4, NT)
        w_out = wt[640:768, :]
        outs2 = dot(jnp.concatenate([w_out, vt[640:768, :]], axis=0), xnb, NN)
        out = outs2[:128]
        dout = dot(w_out, dxnb, NN) + outs2[128:]
        s = jax.nn.sigmoid(gates[:128])
        sp = s * (1.0 - s)
        y = s * out
        ybar = (sp * gates[128:] * out + s * dout) * (1.0 / TOTAL)
        gbar = (ybar * out * sp).astype(BF16)
        obar = (ybar * s).astype(BF16)
        xnbar = dot(w_ref[:, 640:768], obar, NN).astype(BF16).astype(F32)
        rsbar = jnp.sum(xnbar * c, axis=0, keepdims=True)
        cbar = xnbar * rs + c * (rsbar * slope * (2.0 / 128))
        xbar = (cbar - mean0(cbar)).astype(BF16)
        for r in range(4):
            xb4[k, r] = xbar[:, lanes_of(r)]
        return y, gbar, obar, xnb, zn4

    def rest(k, y, gbar, obar, xnb, zn4):
        hs[0:128, :] += dot(gbar, zn4, NN)
        hs[128:256, :] += dot(obar, xnb, NT)
        for r in range(4):
            row = pg[4 * own + r, lanes_of(k), :].astype(F32)
            outs[r, lanes_of(k), :] = (row + y[:, lanes_of(r)].T).astype(BF16)

    def xb(k):
        return (
            2 + k,
            lambda p: xb4.at[k, :, rows_of(p, 32), :],
            lambda p: xbr.at[k, pl.ds(4 * slot(p), 4)],
            xbr.at[k, 0:12],
        )

    five = (4, lambda p: hs.at[rows_of(p, 64), :], lambda p: hr.at[p], hr.at[0:3])
    for k in range(2):
        q_wait(*zz(0, k))
        q_wait(*zz(1, k))
        kept = heads(k)
        q_start(*xb(k))
        rest(k, *kept)

    def back():
        return rcopy(outs, out_ref, o_s, o_r, dev(src_c, src_a))

    def keep():
        return pltpu.make_async_copy(outs, out_ref, o_s)

    def rr(k):
        return (
            4 + k,
            lambda p: xbs.at[k, pl.ds(2 * p, 2)],
            lambda p: rx.at[k, :, rows_of(p, 16), :],
            rx.at[k, :, 0:240, :],
        )

    for k in range(2):
        q_wait(*xb(k))
        loop(0, 16, lambda r: put(k, r, xbr[k, r].astype(F32)))

        def pack_back(i):
            val = tmp[flat(k, i), :].reshape(8, 16, 128)
            xbs[k, pl.ds(8 * i, 8)] = val.astype(BF16)

        loop(0, 4, pack_back)
        xy_start(*rr(k))

    q_start(*five)

    for k in range(2):
        xy_wait(*rr(k))

    def aa(t, k):
        return (
            6 + 10 * t + k,
            lambda p: as_.at[k, t, :, rows_of(p, 16), :],
            lambda p: ar.at[k, t, pl.ds(2 * p, 2)],
            ar.at[k, t, 0:30],
        )

    for t in range(2):
        for c in range(2):
            bar = dot(both(rx, c), both(rf, 1 - t, c), TN if t else NN).astype(BF16)
            for k in range(2):
                as_[k, t, c] = bar[:, lanes_of(k)]
        for k in range(2):
            xy_start(*aa(t, k))

    @pl.when(moved)
    def _():
        back().start()

    @pl.when(stays)
    def _():
        keep().start()

    gi[...] = jnp.zeros_like(gi)
    q_wait(*five)
    hsum[...] = hr[0] + hr[1] + hr[2] + hr[3]
    def grad(t, k, r):
        bar = get(k, 512 * t + r)
        d = fac[k, r, 64 * t : 64 * t + 64, :] * jnp.concatenate([bar, bar], axis=0)
        return dot(d.astype(BF16), zn[r, lanes_of(k), :], NN)

    for t in range(2):
        for k in range(2):
            xy_wait(*aa(t, k))
            spread(k, t, ar)

            def grads(i):
                parts = [grad(t, k, 8 * i + n) for n in range(8)]
                while len(parts) > 1:
                    parts = [x + y for x, y in zip(parts[::2], parts[1::2])]
                gi[64 * t : 64 * t + 64, :] += parts[0]

            loop(0, 2, grads)

    for p in range(16):
        us[p, 0] = gi[8 * p : 8 * p + 4, :]
        us[p, 1] = gi[8 * p + 4 : 8 * p + 8, :]
        us[p, 2] = hsum[4 * p : 4 * p + 4, :]
    eight = (8, lambda p: us.at[p], lambda p: ur.at[p], ur.at[0:15])
    xy_start(*eight)
    xy_wait(*eight)
    total = ur[0]
    for p in range(1, 16):
        total = total + ur[p]
    vb[v] = total

    for d in (4, 3, 5, 2, 6, 1, 7):
        rcopy(vb.at[v], vb.at[v], v_s, v_r, v_dev(lax.rem(v + d, 8))).start()
    rcopy(vb.at[0:7], vb.at[0:7], v_s, v_r, v_dev(lax.rem(v + 1, 8))).wait()
    total = vb[0]
    for p in range(1, 8):
        total = total + vb[p]
    wb[xy, q] = total.astype(BF16)

    for p in (q2, q3, q1):
        here = wb.at[xy, q]
        rcopy(here, here, q_s.at[0], q_r.at[0], q_dev(p)).start()
    most = wb.at[0, 0:3]
    rcopy(most, most, q_s.at[0], q_r.at[0], q_dev(q1)).wait()
    here = wb.at[xy]
    for p in peers:
        rcopy(here, here, xs_s.at[9], xs_r.at[9], xy_dev(p)).start()
    most = wb.at[0:15]
    rcopy(most, most, xs_s.at[9], xs_r.at[9], xy_dev(peers[0])).wait()

    for p in range(4):
        for k in range(16):
            lo = 128 * (k // 4) + 32 * p + 8 * (k % 4)
            ft[lo : lo + 4, :] = wb[k, p, 0].astype(F32)
            ft[lo + 4 : lo + 8, :] = wb[k, p, 1].astype(F32)
            lo = 512 + 64 * p + 4 * k
            ft[lo : lo + 4, :] = wb[k, p, 2].astype(F32)
    for t in range(6):
        cols = slice(128 * t, 128 * t + 128)
        curv_ref[:, cols] = ft[cols, :].T

    @pl.when(moved)
    def _():
        back().wait()

    @pl.when(stays)
    def _():
        keep().wait()

def shards(pair, crop_mask, weights, probe_signs):
    dma = pltpu.SemaphoreType.DMA
    out, curv = pl.pallas_call(
        kernel,
        out_shape=(
            pltpu.VMEM((4, 256, 128), BF16),
            pltpu.VMEM((128, 768), F32),
        ),
        in_specs=[pl.BlockSpec(memory_space=pltpu.HBM)] * 4,
        out_specs=(pl.BlockSpec(memory_space=pltpu.VMEM),) * 2,
        scratch_shapes=[
            pltpu.VMEM((4, 256, 128), BF16),
            pltpu.VMEM((1, 256), jnp.int32),
            pltpu.VMEM((128, 768), BF16),
            pltpu.VMEM((128, 768), jnp.int32),
            pltpu.VMEM((768, 128), BF16),
            pltpu.VMEM((768, 128), BF16),
            pltpu.VMEM((256, 128), BF16),
            pltpu.VMEM((16, 256, 128), BF16),
            pltpu.VMEM((8, 1, 256), jnp.int32),
            pltpu.VMEM((16, 256, 128), BF16),
            pltpu.VMEM((2, 16, 128, 128), F32),
            pltpu.VMEM((4224, 128), F32),
            pltpu.VMEM((2, 4, 32, 16, 128), BF16),
            pltpu.VMEM((2, 4, 2, 256, 128), BF16),
            pltpu.VMEM((2, 2, 2, 256, 128), BF16),
            pltpu.VMEM((2, 2, 32, 16, 128), BF16),
            pltpu.VMEM((2, 2, 16, 32, 128), BF16),
            pltpu.VMEM((2, 2, 4, 128, 128), BF16),
            pltpu.VMEM((4, 256, 128), BF16),
            pltpu.VMEM((2, 4, 128, 128), BF16),
            pltpu.VMEM((2, 16, 32, 128), BF16),
            pltpu.VMEM((2, 32, 16, 128), BF16),
            pltpu.VMEM((2, 2, 256, 128), BF16),
            pltpu.VMEM((2, 2, 2, 256, 128), BF16),
            pltpu.VMEM((2, 2, 32, 16, 128), BF16),
            pltpu.VMEM((64, 128), F32),
            pltpu.VMEM((256, 128), F32),
            pltpu.VMEM((4, 64, 128), F32),
            pltpu.VMEM((128, 128), F32),
            pltpu.VMEM((17, 3, 4, 128), F32),
            pltpu.VMEM((17, 3, 4, 128), F32),
            pltpu.VMEM((9, 3, 4, 128), F32),
            pltpu.VMEM((17, 4, 3, 4, 128), BF16),
            pltpu.VMEM((768, 128), F32),
            dma((4,)), dma((5,)), dma((5,)), dma((3, 4)), dma((3, 4)),
            dma((18,)), dma((18,)), dma((9,)), dma((9,)),
            dma, dma, dma, dma, dma((4,)), dma((9,)),
        ],
        compiler_params=pltpu.CompilerParams(
            collective_id=0, has_side_effects=True, vmem_limit_bytes=58 * 2**20
        ),
    )(pair[0], crop_mask, weights, probe_signs)
    return out[None], curv


def solution(mesh):
    placed = (P("crop", "axial", None, None), P("crop", None), P(), P())
    return jax.shard_map(
        shards,
        mesh=mesh,
        in_specs=placed,
        out_specs=(P("crop", "axial", None, None), P()),
        check_vma=False,
    )
```
